32 devices in a mesh: dp: 1 (over z), ch: 4 (over y), wd: 8 (over x, core).
Axes of the slice: x: 4, y: 4, z: 1, core: 2. Of those that a mesh axis runs over, the one named last changes fastest.
The devices are a block of a 4x4x8 slice.
Arguments:
- resid_in: bfloat16 [4096, 4096], P('dp', 'wd')
- seg_pos: int32 [1, 4096], P('dp')
- gain_temporal: bfloat16 [4096], P('wd')
- w_x: bfloat16 [4096, 4096], P('wd', 'ch')
- bias_x: bfloat16 [4096], P('ch')
- w_y: bfloat16 [4096, 4096], P('wd', 'ch')
- bias_y: bfloat16 [4096], P('ch')
- conv_w: bfloat16 [4, 4096], P(None, 'ch')
- conv_bias: bfloat16 [4096], P('ch')
- lam_param: float32 [4096], P('ch')
- rgate_w: bfloat16 [16, 256, 256], P('ch')
- rgate_b: bfloat16 [4096], P('ch')
- igate_w: bfloat16 [16, 256, 256], P('ch')
- igate_b: bfloat16 [4096], P('ch')
- w_o: bfloat16 [4096, 4096], P('ch', 'wd')
- bias_o: bfloat16 [4096], P('wd')
- gain_mlp: bfloat16 [4096], P('wd')
- w_g: bfloat16 [4096, 12288], P('wd', 'ch')
- bias_g: bfloat16 [12288], P('ch')
- w_u: bfloat16 [4096, 12288], P('wd', 'ch')
- bias_u: bfloat16 [12288], P('ch')
- w_d: bfloat16 [12288, 4096], P('ch', 'wd')
- bias_d: bfloat16 [4096], P('wd')
Outputs:
- output: bfloat16 [4096, 4096], P('dp', 'wd')
All inputs are finite; a program needn't handle non-finite values.
Results may differ from the reference program's by a relative error of at most 0.0128771.
Values are sent between devices in bfloat16 or wider.
A program may use at most 768 MiB of HBM per device.

```python
import jax
import jax.numpy as jnp
from jax import lax

D = 4096
D_RNN = 4096
F = 12288
BLOCKS = 16
B = 1
T = 4096
CONV_WIDTH = 4
BLOCK_WIDTH = D_RNN // BLOCKS
EPS = 1e-6


def normal_draw(key, shape, scale):
    return (jax.random.normal(key, shape, jnp.float32) * scale).astype(jnp.bfloat16)


def doc_positions(key):
    cuts = jax.random.randint(key, (B, 4), 0, T)
    steps = jnp.arange(T, dtype=jnp.int32)
    starts = jnp.any(steps[None, :, None] == cuts[:, None, :], axis=2) | (steps == 0)[None, :]
    last_start = lax.cummax(jnp.where(starts, steps[None, :], 0), axis=1)
    return (steps[None, :] - last_start).astype(jnp.int32)


def setup_inputs(seed: int = 0, part: int = 0) -> dict:
    root = jax.random.key(seed)
    part_key = jax.random.fold_in(root, part)
    keys = jax.random.split(root, 24)
    col_ramp = 0.5 + 1.5 * jnp.arange(D, dtype=jnp.float32) / D
    noise = jax.random.normal(jax.random.fold_in(part_key, 0), (B * T, D), jnp.float32)
    decay_target = jax.random.uniform(keys[9], (D_RNN,), jnp.float32, 0.9, 0.999)
    sigma_lam = decay_target ** 0.125
    return {
        'resid_in': (noise * col_ramp).astype(jnp.bfloat16),
        'seg_pos': doc_positions(jax.random.fold_in(part_key, 1)),
        'gain_temporal': normal_draw(keys[0], (D,), 0.5),
        'w_x': normal_draw(keys[1], (D, D_RNN), D ** -0.5),
        'bias_x': normal_draw(keys[2], (D_RNN,), 0.5),
        'w_y': normal_draw(keys[3], (D, D_RNN), D ** -0.5),
        'bias_y': normal_draw(keys[4], (D_RNN,), 0.5),
        'conv_w': normal_draw(keys[5], (CONV_WIDTH, D_RNN), 0.5),
        'conv_bias': normal_draw(keys[6], (D_RNN,), 0.5),
        'lam_param': jnp.log(sigma_lam / (1.0 - sigma_lam)),
        'rgate_w': normal_draw(keys[7], (BLOCKS, BLOCK_WIDTH, BLOCK_WIDTH), BLOCK_WIDTH ** -0.5),
        'rgate_b': normal_draw(keys[8], (D_RNN,), 1.0),
        'igate_w': normal_draw(keys[10], (BLOCKS, BLOCK_WIDTH, BLOCK_WIDTH), BLOCK_WIDTH ** -0.5),
        'igate_b': normal_draw(keys[11], (D_RNN,), 1.0),
        'w_o': normal_draw(keys[12], (D_RNN, D), 1.5 * D_RNN ** -0.5),
        'bias_o': normal_draw(keys[13], (D,), 0.5),
        'gain_mlp': normal_draw(keys[14], (D,), 0.5),
        'w_g': normal_draw(keys[15], (D, F), D ** -0.5),
        'bias_g': normal_draw(keys[16], (F,), 0.5),
        'w_u': normal_draw(keys[17], (D, F), D ** -0.5),
        'bias_u': normal_draw(keys[18], (F,), 0.5),
        'w_d': normal_draw(keys[19], (F, D), 1.5 * F ** -0.5),
        'bias_d': normal_draw(keys[20], (D,), 0.5),
    }


def rms_scale(vals, gain):
    mean_sq = jnp.mean(vals * vals, axis=-1, keepdims=True)
    return (vals * lax.rsqrt(mean_sq + EPS) * (1.0 + gain.astype(jnp.float32))).astype(jnp.bfloat16)


def conv_mix(vals, positions, conv_w, conv_bias):
    vals32 = vals.astype(jnp.float32)
    taps = conv_w.astype(jnp.float32)
    total = conv_bias.astype(jnp.float32) + vals32 * taps[0]
    for shift in range(1, CONV_WIDTH):
        moved = jnp.pad(vals32[:-shift], ((shift, 0), (0, 0)))
        total = total + jnp.where((positions >= shift)[:, None], moved, 0.0) * taps[shift]
    return total.astype(jnp.bfloat16)


def combine(left, right):
    return left[0] * right[0], right[0] * left[1] + right[1]


def rg_lru(conv_out, positions, lam_param, rgate_w, rgate_b, igate_w, igate_b):
    grouped = conv_out.astype(jnp.float32).reshape(T, BLOCKS, BLOCK_WIDTH)
    rate = jax.nn.sigmoid(jnp.einsum('tbi,bij->tbj', grouped, rgate_w.astype(jnp.float32)).reshape(T, D_RNN) + rgate_b.astype(jnp.float32))
    inflow = jax.nn.sigmoid(jnp.einsum('tbi,bij->tbj', grouped, igate_w.astype(jnp.float32)).reshape(T, D_RNN) + igate_b.astype(jnp.float32))
    log_a = -8.0 * rate * jax.nn.softplus(-lam_param.astype(jnp.float32))
    reset = (positions == 0)[:, None]
    decay = jnp.where(reset, 0.0, jnp.exp(log_a))
    scale = jnp.where(reset, 1.0, jnp.sqrt(-jnp.expm1(2.0 * log_a)))
    drive = scale * inflow * conv_out.astype(jnp.float32)
    return lax.associative_scan(combine, (decay, drive), axis=0)[1]


def reference(resid_in, seg_pos, gain_temporal, w_x, bias_x, w_y, bias_y, conv_w, conv_bias, lam_param, rgate_w, rgate_b, igate_w, igate_b, w_o, bias_o, gain_mlp, w_g, bias_g, w_u, bias_u, w_d, bias_d):
    def one_sequence(pair):
        seq_x, positions = pair
        resid32 = seq_x.astype(jnp.float32)
        normed = rms_scale(resid32, gain_temporal)
        y_branch = jax.nn.gelu(jnp.dot(normed, w_y, preferred_element_type=jnp.float32) + bias_y.astype(jnp.float32), approximate=True).astype(jnp.bfloat16)
        u_branch = (jnp.dot(normed, w_x, preferred_element_type=jnp.float32) + bias_x.astype(jnp.float32)).astype(jnp.bfloat16)
        conv_out = conv_mix(u_branch, positions, conv_w, conv_bias)
        hidden = rg_lru(conv_out, positions, lam_param, rgate_w, rgate_b, igate_w, igate_b)
        mixed = (hidden * y_branch.astype(jnp.float32)).astype(jnp.bfloat16)
        resid = resid32 + jnp.dot(mixed, w_o, preferred_element_type=jnp.float32) + bias_o.astype(jnp.float32)
        normed2 = rms_scale(resid, gain_mlp)
        gate = jax.nn.gelu(jnp.dot(normed2, w_g, preferred_element_type=jnp.float32) + bias_g.astype(jnp.float32), approximate=True)
        upper = jnp.dot(normed2, w_u, preferred_element_type=jnp.float32) + bias_u.astype(jnp.float32)
        inner = (gate * upper).astype(jnp.bfloat16)
        return (resid + jnp.dot(inner, w_d, preferred_element_type=jnp.float32) + bias_d.astype(jnp.float32)).astype(jnp.bfloat16)
    per_seq = lax.map(one_sequence, (resid_in.reshape(B, T, D), seg_pos))
    return per_seq.reshape(B * T, D)
```

```python
import functools

import jax
import jax.numpy as jnp
from jax import lax
from jax.experimental import pallas as pl
from jax.experimental.pallas import tpu as pltpu
from jax.sharding import PartitionSpec as P

EPS = 1e-6
CORES = 2
SEGS = 8
PAD = 8


def rms_apply(vals, sum_sq, width, gain):
    return (vals * lax.rsqrt(sum_sq / width + EPS) * (1.0 + gain.astype(jnp.float32))).astype(jnp.bfloat16)


def neg_expm1(z):
    series = -z * (1.0 + z * (0.5 + z * (1.0 / 6.0 + z * (1.0 / 24.0))))
    return jnp.where(z > -0.03, series, 1.0 - jnp.exp(z))


def lru_kernel(u_ref, y_ref, pos_ref, taps_ref, cbias_ref, gate_w_ref, gate_b_ref, lam_ref, out_ref, u32, a_s, b_s):
    tokens, wide = u_ref.shape
    width = y_ref.shape[1]
    tile = tokens // SEGS
    pitch = tile + PAD
    taps = taps_ref[...].astype(jnp.float32)
    n_taps = taps_ref.shape[0]
    cbias = cbias_ref[...].astype(jnp.float32)
    gate_b = gate_b_ref[...].astype(jnp.float32)
    lam = -lam_ref[...]
    soft = -8.0 * (jnp.maximum(lam, 0.0) + jnp.log(1.0 + jnp.exp(-jnp.abs(lam))))
    u32[0:PAD, :] = jnp.zeros((PAD, wide), jnp.float32)

    def widen(i, carry):
        rows = pl.multiple_of(i * tile, tile)
        u32[pl.ds(rows + PAD, tile), :] = u_ref[pl.ds(rows, tile), :].astype(jnp.float32)
        return carry
    lax.fori_loop(0, SEGS, widen, 0)

    sub = tile // 4

    def gates(i, carry):
        rows = pl.multiple_of(i * sub, sub)
        window = u32[pl.ds(rows, sub + PAD), :]
        pos = pos_ref[pl.ds(rows, sub), :]
        total = cbias + window[PAD:] * taps[0:1]
        for k in range(1, n_taps):
            total = total + jnp.where(pos >= k, window[PAD - k:PAD - k + sub], 0.0) * taps[k:k + 1]
        conv = total.astype(jnp.bfloat16)
        pre = jnp.dot(conv, gate_w_ref[...], preferred_element_type=jnp.float32) + gate_b
        both = jax.nn.sigmoid(pre)
        log_a = both[:, :width] * soft
        reset = pos == 0
        decay = jnp.where(reset, 0.0, jnp.exp(log_a))
        scale = jnp.where(reset, 1.0, jnp.sqrt(neg_expm1(2.0 * log_a)))
        drive = scale * both[:, width:] * conv[:, :width].astype(jnp.float32)
        seg = i // 4
        at = pl.multiple_of(seg * pitch + (i - seg * 4) * sub, 8)
        a_s[pl.ds(at, sub), :] = decay
        b_s[pl.ds(at, sub), :] = drive
        return carry
    lax.fori_loop(0, SEGS * 4, gates, 0)

    def steps(i, carry):
        hid, acc = carry
        for j in range(8):
            t = i * 8 + j
            a = a_s[pl.ds(t, SEGS, stride=pitch), :]
            hid = a * hid + b_s[pl.ds(t, SEGS, stride=pitch), :]
            acc = a * acc
            b_s[pl.ds(t, SEGS, stride=pitch), :] = hid
            a_s[pl.ds(t, SEGS, stride=pitch), :] = acc
        return hid, acc
    hid, acc = lax.fori_loop(0, tile // 8, steps, (jnp.zeros((SEGS, width), jnp.float32), jnp.ones((SEGS, width), jnp.float32)))

    entry = jnp.zeros((1, width), jnp.float32)
    for seg in range(SEGS):
        for q in range(4):
            at = seg * pitch + q * sub
            hidden = b_s[at:at + sub, :] + a_s[at:at + sub, :] * entry
            rows = slice(seg * tile + q * sub, seg * tile + (q + 1) * sub)
            out_ref[rows, :] = (hidden * y_ref[rows, :].astype(jnp.float32)).astype(jnp.bfloat16)
        entry = hid[seg:seg + 1] + acc[seg:seg + 1] * entry


def lru(u_pair, y_rows, pos, taps, cbias, gate_w, gate_b, lam):
    tokens, wide = u_pair.shape
    width = y_rows.shape[1]
    rows = SEGS * (tokens // SEGS + PAD)
    return pl.pallas_call(
        lru_kernel,
        out_shape=jax.ShapeDtypeStruct((tokens, width), jnp.bfloat16),
        in_specs=[pl.BlockSpec(memory_space=pltpu.VMEM)] * 8,
        out_specs=pl.BlockSpec(memory_space=pltpu.VMEM),
        scratch_shapes=[pltpu.VMEM((tokens + PAD, wide), jnp.float32), pltpu.VMEM((rows, width), jnp.float32), pltpu.VMEM((rows, width), jnp.float32)],
        compiler_params=pltpu.CompilerParams(vmem_limit_bytes=48 << 20),
        name='lru',
    )(u_pair, y_rows, pos, taps, cbias, gate_w, gate_b, lam)


def gate_up_kernel(n_ref, w_ref, bias_ref, out_ref, acc):
    step = pl.program_id(2)
    half = out_ref.shape[1]
    part = jnp.dot(n_ref[0, 0], w_ref[0], preferred_element_type=jnp.float32)

    @pl.when(step == 0)
    def _():
        acc[...] = part

    @pl.when(step > 0)
    def _():
        acc[...] += part

    @pl.when(step == pl.num_programs(2) - 1)
    def _():
        bias = bias_ref[...].astype(jnp.float32)
        total = acc[...] + bias
        out_ref[...] = (jax.nn.gelu(total[:, :half], approximate=True) * total[:, half:]).astype(jnp.bfloat16)


def gate_up(normed, weight, bias):
    ch, wd, share, depth = normed.shape
    cols = weight.shape[2]
    tile = 512
    return pl.pallas_call(
        gate_up_kernel,
        grid=(ch, share // tile, wd),
        out_shape=jax.ShapeDtypeStruct((ch * share, cols // 2), jnp.bfloat16),
        in_specs=[pl.BlockSpec((1, 1, tile, depth), lambda c, t, i: (c, i, t, 0)),
                  pl.BlockSpec((1, depth, cols), lambda c, t, i: (i, 0, 0)),
                  pl.BlockSpec((1, cols), lambda c, t, i: (0, 0))],
        out_specs=pl.BlockSpec((tile, cols // 2), lambda c, t, i: (c * (share // tile) + t, 0)),
        scratch_shapes=[pltpu.VMEM((tile, cols), jnp.float32)],
        compiler_params=pltpu.CompilerParams(vmem_limit_bytes=40 << 20),
        name='gate_up',
    )(normed, weight, bias)


def down_kernel(h_ref, w_ref, out_ref, acc):
    step = pl.program_id(1)
    depth = h_ref.shape[2]
    part = jnp.dot(h_ref[0], w_ref[pl.ds(pl.multiple_of(step * depth, depth), depth), :], preferred_element_type=jnp.float32)

    @pl.when(step == 0)
    def _():
        acc[...] = part

    @pl.when(step > 0)
    def _():
        acc[...] += part

    @pl.when(step == pl.num_programs(1) - 1)
    def _():
        out_ref[...] = acc[...].astype(jnp.bfloat16)


def down(parts, weight):
    count, tokens, depth = parts.shape
    cols = weight.shape[1]
    tile = 1024
    return pl.pallas_call(
        down_kernel,
        grid=(tokens // tile, count),
        out_shape=jax.ShapeDtypeStruct((tokens, cols), jnp.bfloat16),
        in_specs=[pl.BlockSpec((1, tile, depth), lambda t, i: (i, t, 0)),
                  pl.BlockSpec(weight.shape, lambda t, i: (0, 0))],
        out_specs=pl.BlockSpec((tile, cols), lambda t, i: (t, 0)),
        scratch_shapes=[pltpu.VMEM((tile, cols), jnp.float32)],
        compiler_params=pltpu.CompilerParams(vmem_limit_bytes=40 << 20),
        name='down',
    )(parts, weight)


def solution(mesh):
    wd_count = mesh.shape['wd']
    ch_count = mesh.shape['ch']
    chips = wd_count // CORES
    row_spec = P('dp', 'wd')
    specs = (row_spec, P('dp', None), P('wd'), P('wd', 'ch'), P('ch'), P('wd', 'ch'), P('ch'), P(None, 'ch'), P('ch'), P('ch'), P('ch', None, None), P('ch'), P('ch', None, None), P('ch'), P('ch', 'wd'), P('wd'), P('wd'), P('wd', 'ch'), P('ch'), P('wd', 'ch'), P('ch'), P('ch', 'wd'), P('wd'))
    swap = [(i, i + 1 - 2 * (i % CORES)) for i in range(wd_count)]
    same_core = [[x * CORES + c for x in range(chips)] for c in range(CORES)]

    def local_layer(resid_in, seg_pos, gain_temporal, w_x, bias_x, w_y, bias_y, conv_w, conv_bias, lam_param, rgate_w, rgate_b, igate_w, igate_b, w_o, bias_o, gain_mlp, w_g, bias_g, w_u, bias_u, w_d, bias_d):
        tokens, local_width = resid_in.shape
        model_width = local_width * wd_count
        share = tokens // ch_count
        rnn = w_x.shape[1]
        mine = rnn // wd_count
        wd_i = lax.axis_index('wd')
        core = wd_i % CORES
        block = wd_i // CORES
        positions = seg_pos.reshape(tokens)

        def own(vec):
            return lax.dynamic_slice_in_dim(vec, wd_i * mine, mine, axis=vec.ndim - 1)

        def both(vec):
            pair = lax.dynamic_slice_in_dim(vec, block * CORES * mine, CORES * mine, axis=vec.ndim - 1)
            return jnp.where(core == 0, pair, jnp.concatenate([pair[..., mine:], pair[..., :mine]], axis=-1))

        ff = w_g.shape[1] // wd_count
        pieces = jnp.concatenate([w_g.reshape(local_width, wd_count, ff), w_u.reshape(local_width, wd_count, ff)], axis=2)
        mlp_w = lax.all_to_all(pieces.transpose(1, 0, 2), 'wd', 0, 0)

        resid32 = resid_in.astype(jnp.float32)
        sum_sq = lax.psum(jnp.sum(resid32 * resid32, axis=1, keepdims=True), 'wd')
        normed = rms_apply(resid32, sum_sq, model_width, gain_temporal)
        normed_pair = lax.ppermute(normed, 'wd', swap)
        w_xy = jnp.concatenate([w_x.reshape(local_width, chips, CORES, mine), w_y.reshape(local_width, chips, CORES, mine)], axis=3)
        w_keep = lax.dynamic_index_in_dim(w_xy, core, 2, keepdims=False).reshape(local_width, rnn)
        w_send = lax.dynamic_index_in_dim(w_xy, 1 - core, 2, keepdims=False).reshape(local_width, rnn)
        w_pair = lax.ppermute(w_send, 'wd', swap)
        part = (jnp.dot(normed, w_keep, preferred_element_type=jnp.float32) + jnp.dot(normed_pair, w_pair, preferred_element_type=jnp.float32)).astype(jnp.bfloat16)
        got = lax.all_to_all(part.reshape(tokens, chips, CORES * mine).transpose(1, 0, 2), 'wd', 0, 0, axis_index_groups=same_core)
        uy = jnp.sum(got.astype(jnp.float32), axis=0)
        u_own = (uy[:, :mine] + own(bias_x).astype(jnp.float32)).astype(jnp.bfloat16)
        y_own = jax.nn.gelu(uy[:, mine:] + own(bias_y).astype(jnp.float32), approximate=True).astype(jnp.bfloat16)
        u_pair = jnp.concatenate([u_own, lax.ppermute(u_own, 'wd', swap)], axis=1)
        gate_w = jnp.concatenate([lax.dynamic_index_in_dim(w, block, 0, keepdims=False) for w in (rgate_w, igate_w)], axis=1)
        gate_w = gate_w.reshape(CORES, mine, 2, CORES, mine)
        gate_w = lax.dynamic_index_in_dim(gate_w, core, 3, keepdims=False).reshape(CORES, mine, 2 * mine)
        gate_w = jnp.where(core == 0, gate_w, gate_w[::-1]).reshape(CORES * mine, 2 * mine)
        gate_b = jnp.concatenate([own(rgate_b), own(igate_b)])[None]
        mixed = lru(u_pair, y_own, positions[:, None], both(conv_w), both(conv_bias)[None], gate_w, gate_b, own(lam_param)[None])
        mixed_all = lax.all_gather(mixed, 'wd', axis=0)
        mix_part = jnp.dot(mixed_all.transpose(1, 0, 2).reshape(tokens, rnn), w_o, preferred_element_type=jnp.float32).astype(jnp.bfloat16)
        mix_sum = jnp.sum(lax.all_to_all(mix_part.reshape(ch_count, share, local_width), 'ch', 0, 0).astype(jnp.float32), axis=0)
        resid_rows = lax.dynamic_slice_in_dim(resid32, lax.axis_index('ch') * share, share, axis=0)
        resid = resid_rows + mix_sum + bias_o.astype(jnp.float32)
        sum_sq2 = lax.psum(jnp.sum(resid * resid, axis=1, keepdims=True), 'wd')
        normed2 = rms_apply(resid, sum_sq2, model_width, gain_mlp)
        all2 = lax.all_gather(normed2, ('ch', 'wd'), axis=0).reshape(ch_count, wd_count, share, local_width)
        mlp_b = jnp.concatenate([lax.dynamic_slice_in_dim(b, wd_i * ff, ff) for b in (bias_g, bias_u)])[None]
        inner = gate_up(all2, mlp_w, mlp_b)
        inner_all = lax.all_gather(inner, 'wd', axis=0)
        down_part = down(inner_all, w_d)
        down_sum = jnp.sum(lax.all_to_all(down_part.reshape(ch_count, share, local_width), 'ch', 0, 0).astype(jnp.float32), axis=0)
        out_rows = (resid + down_sum + bias_d.astype(jnp.float32)).astype(jnp.bfloat16)
        return lax.all_gather(out_rows, 'ch', axis=0, tiled=True)

    return jax.shard_map(local_layer, mesh=mesh, in_specs=specs, out_specs=row_spec, check_vma=False)
```

```python
import functools

import jax
import jax.numpy as jnp
from jax import lax
from jax.experimental import pallas as pl
from jax.experimental.pallas import tpu as pltpu
from jax.sharding import PartitionSpec as P

EPS = 1e-6
CORES = 2
SEGS = 8
PAD = 8


def rms_apply(vals, sum_sq, width, gain):
    return (vals * lax.rsqrt(sum_sq / width + EPS) * (1.0 + gain.astype(jnp.float32))).astype(jnp.bfloat16)


def neg_expm1(z):
    series = -z * (1.0 + z * (0.5 + z * (1.0 / 6.0 + z * (1.0 / 24.0))))
    return jnp.where(z > -0.03, series, 1.0 - jnp.exp(z))


def lru_kernel(u_ref, y_ref, pos_ref, taps_ref, cbias_ref, gate_w_ref, gate_b_ref, lam_ref, out_ref, u32, a_s, b_s):
    tokens, wide = u_ref.shape
    width = y_ref.shape[1]
    tile = tokens // SEGS
    pitch = tile + PAD
    taps = taps_ref[...].astype(jnp.float32)
    n_taps = taps_ref.shape[0]
    cbias = cbias_ref[...].astype(jnp.float32)
    gate_b = gate_b_ref[...].astype(jnp.float32)
    lam = -lam_ref[...]
    soft = -8.0 * (jnp.maximum(lam, 0.0) + jnp.log(1.0 + jnp.exp(-jnp.abs(lam))))
    u32[0:PAD, :] = jnp.zeros((PAD, wide), jnp.float32)

    def widen(i, carry):
        rows = pl.multiple_of(i * tile, tile)
        u32[pl.ds(rows + PAD, tile), :] = u_ref[pl.ds(rows, tile), :].astype(jnp.float32)
        return carry
    lax.fori_loop(0, SEGS, widen, 0)

    sub = tile // 4

    def gates(i, carry):
        rows = pl.multiple_of(i * sub, sub)
        window = u32[pl.ds(rows, sub + PAD), :]
        pos = pos_ref[pl.ds(rows, sub), :]
        total = cbias + window[PAD:] * taps[0:1]
        for k in range(1, n_taps):
            total = total + jnp.where(pos >= k, window[PAD - k:PAD - k + sub], 0.0) * taps[k:k + 1]
        conv = total.astype(jnp.bfloat16)
        pre = jnp.dot(conv, gate_w_ref[...], preferred_element_type=jnp.float32) + gate_b
        both = jax.nn.sigmoid(pre)
        log_a = both[:, :width] * soft
        reset = pos == 0
        decay = jnp.where(reset, 0.0, jnp.exp(log_a))
        scale = jnp.where(reset, 1.0, jnp.sqrt(neg_expm1(2.0 * log_a)))
        drive = scale * both[:, width:] * conv[:, :width].astype(jnp.float32)
        seg = i // 4
        at = pl.multiple_of(seg * pitch + (i - seg * 4) * sub, 8)
        a_s[pl.ds(at, sub), :] = decay
        b_s[pl.ds(at, sub), :] = drive
        return carry
    lax.fori_loop(0, SEGS * 4, gates, 0)

    def steps(i, carry):
        hid, acc = carry
        for j in range(8):
            t = i * 8 + j
            a = a_s[pl.ds(t, SEGS, stride=pitch), :]
            hid = a * hid + b_s[pl.ds(t, SEGS, stride=pitch), :]
            acc = a * acc
            b_s[pl.ds(t, SEGS, stride=pitch), :] = hid
            a_s[pl.ds(t, SEGS, stride=pitch), :] = acc
        return hid, acc
    hid, acc = lax.fori_loop(0, tile // 8, steps, (jnp.zeros((SEGS, width), jnp.float32), jnp.ones((SEGS, width), jnp.float32)))

    entry = jnp.zeros((1, width), jnp.float32)
    for seg in range(SEGS):
        for q in range(4):
            at = seg * pitch + q * sub
            hidden = b_s[at:at + sub, :] + a_s[at:at + sub, :] * entry
            rows = slice(seg * tile + q * sub, seg * tile + (q + 1) * sub)
            out_ref[rows, :] = (hidden * y_ref[rows, :].astype(jnp.float32)).astype(jnp.bfloat16)
        entry = hid[seg:seg + 1] + acc[seg:seg + 1] * entry


def lru(u_pair, y_rows, pos, taps, cbias, gate_w, gate_b, lam):
    tokens, wide = u_pair.shape
    width = y_rows.shape[1]
    rows = SEGS * (tokens // SEGS + PAD)
    return pl.pallas_call(
        lru_kernel,
        out_shape=jax.ShapeDtypeStruct((tokens, width), jnp.bfloat16),
        in_specs=[pl.BlockSpec(memory_space=pltpu.VMEM)] * 8,
        out_specs=pl.BlockSpec(memory_space=pltpu.VMEM),
        scratch_shapes=[pltpu.VMEM((tokens + PAD, wide), jnp.float32), pltpu.VMEM((rows, width), jnp.float32), pltpu.VMEM((rows, width), jnp.float32)],
        compiler_params=pltpu.CompilerParams(vmem_limit_bytes=48 << 20),
        name='lru',
    )(u_pair, y_rows, pos, taps, cbias, gate_w, gate_b, lam)


def gate_up_kernel(n_ref, w_ref, bias_ref, out_ref, acc):
    step = pl.program_id(2)
    half = out_ref.shape[1]
    part = jnp.dot(n_ref[0, 0], w_ref[0], preferred_element_type=jnp.float32)

    @pl.when(step == 0)
    def _():
        acc[...] = part

    @pl.when(step > 0)
    def _():
        acc[...] += part

    @pl.when(step == pl.num_programs(2) - 1)
    def _():
        bias = bias_ref[...].astype(jnp.float32)
        total = acc[...] + bias
        out_ref[...] = (jax.nn.gelu(total[:, :half], approximate=True) * total[:, half:]).astype(jnp.bfloat16)


def gate_up(normed, weight, bias):
    ch, wd, share, depth = normed.shape
    cols = weight.shape[2]
    tile = 512
    return pl.pallas_call(
        gate_up_kernel,
        grid=(ch, share // tile, wd),
        out_shape=jax.ShapeDtypeStruct((ch * share, cols // 2), jnp.bfloat16),
        in_specs=[pl.BlockSpec((1, 1, tile, depth), lambda c, t, i: (c, i, t, 0)),
                  pl.BlockSpec((1, depth, cols), lambda c, t, i: (i, 0, 0)),
                  pl.BlockSpec((1, cols), lambda c, t, i: (0, 0))],
        out_specs=pl.BlockSpec((tile, cols // 2), lambda c, t, i: (c * (share // tile) + t, 0)),
        scratch_shapes=[pltpu.VMEM((tile, cols), jnp.float32)],
        compiler_params=pltpu.CompilerParams(vmem_limit_bytes=40 << 20),
        name='gate_up',
    )(normed, weight, bias)


MESH = pl.DeviceIdType.MESH
ROUNDS = 4


def ring_kernel(regather, h_ref, w_ref, resid_ref, bias_ref, out_ref, hbuf, pbuf, opp_buf, side, xs, xr, ys, yr, own_sem):
    share, depth = h_ref.shape[1:]
    rr = share // ROUNDS
    half = rr // 2
    ring_x = lax.axis_size('wd') // CORES
    ring_y = lax.axis_size('ch')
    ch = lax.axis_index('ch')
    wd = lax.axis_index('wd')
    core = lax.rem(wd, CORES)
    chip = wd // CORES
    other = 1 - 2 * core

    def along_x(step):
        return lax.rem(chip + step, ring_x) * CORES + core

    x_right, x_opp, x_left = along_x(1), along_x(2), along_x(3)
    y_right, y_opp, y_left = (lax.rem(ch + step, ring_y) for step in (1, 2, 3))
    partner = wd + other

    def span(r, part):
        if part is None:
            return pl.ds(r * rr, rr)
        return pl.ds(r * rr + part * half, half)

    def cols(owner, r, part=None):
        return hbuf.at[:, span(r, part), pl.ds(pl.multiple_of(owner * depth, depth), depth)]

    def x_send(k, r):
        if k in (0, 1, 4):
            src, dst = h_ref.at[:, span(r, None)], cols(wd, r)
        else:
            owner, part = {2: (x_left, 0), 3: (x_right, 1), 5: (x_left, None), 6: (x_right, None), 7: (x_opp, 0), 8: (x_opp, 1)}[k]
            src = dst = cols(owner, r, part)
        to = {0: x_right, 1: x_left, 2: x_right, 3: x_left}.get(k, partner)
        return pltpu.make_async_remote_copy(src_ref=src, dst_ref=dst, send_sem=xs.at[r, k], recv_sem=xr.at[r, k], device_id={'wd': to}, device_id_type=MESH)

    def x_recv(k, r):
        owner, part = {0: (x_left, None), 1: (x_right, None), 2: (x_opp, 0), 3: (x_opp, 1), 4: (partner, None), 5: (x_left + other, None),
                       6: (x_right + other, None), 7: (x_opp + other, 0), 8: (x_opp + other, 1)}[k]
        ref = cols(owner, r, part)
        pltpu.make_async_remote_copy(src_ref=ref, dst_ref=ref, send_sem=xs.at[r, k], recv_sem=xr.at[r, k], device_id={'wd': partner}, device_id_type=MESH).wait_recv()

    def y_refs(k, r):
        opp_rows = pl.ds(r * half, half)
        a, b, full = span(r, 0), span(r, 1), span(r, None)
        if k < 6:
            src, dst, to = {
                0: (pbuf.at[0, a], opp_buf.at[0, opp_rows], y_right),
                1: (pbuf.at[0, b], opp_buf.at[1, opp_rows], y_left),
                2: (pbuf.at[3, b], side.at[0, b], y_right),
                3: (pbuf.at[1, a], side.at[1, a], y_left),
                4: (pbuf.at[3, a], side.at[0, a], y_right),
                5: (pbuf.at[1, b], side.at[1, b], y_left),
            }[k]
            return src, dst, to, dst
        owner, part, to, got = {
            6: (ch, full, y_right, y_left),
            7: (ch, full, y_left, y_right),
            8: (y_left, a, y_right, y_opp),
            9: (y_right, b, y_left, y_opp),
        }[k]
        return out_ref.at[owner, part], out_ref.at[owner, part], to, out_ref.at[got, part]

    def y_send(k, r):
        src, dst, to, _ = y_refs(k, r)
        return pltpu.make_async_remote_copy(src_ref=src, dst_ref=dst, send_sem=ys.at[r, k], recv_sem=yr.at[r, k], device_id={'ch': to}, device_id_type=MESH)

    def y_recv(k, r):
        ref = y_refs(k, r)[3]
        pltpu.make_async_remote_copy(src_ref=ref, dst_ref=ref, send_sem=ys.at[r, k], recv_sem=yr.at[r, k], device_id={'ch': y_right}, device_id_type=MESH).wait_recv()

    def start_own(r):
        for k in (0, 1, 4):
            x_send(k, r).start()

    def dots(r):
        def one(slot, carry):
            rows_of = lax.rem(ch + 2 + slot, ring_y)
            block = hbuf[rows_of, pl.ds(r * rr, rr), :]
            pbuf[slot, pl.ds(r * rr, rr), :] = jnp.dot(block, w_ref[...], preferred_element_type=jnp.float32).astype(jnp.bfloat16)
            return carry
        lax.fori_loop(0, ring_y, one, 0)
        for k in range(4):
            y_send(k, r).start()

    def combine(r):
        opp_rows = pl.ds(r * half, half)
        y_recv(0, r)
        pbuf[3, span(r, 0), :] = (pbuf[3, span(r, 0), :].astype(jnp.float32) + opp_buf[0, opp_rows, :].astype(jnp.float32)).astype(jnp.bfloat16)
        y_send(4, r).start()
        y_recv(1, r)
        pbuf[1, span(r, 1), :] = (pbuf[1, span(r, 1), :].astype(jnp.float32) + opp_buf[1, opp_rows, :].astype(jnp.float32)).astype(jnp.bfloat16)
        y_send(5, r).start()

    def final(r):
        for k in range(2, 6):
            y_recv(k, r)
        rows = span(r, None)
        total = pbuf[2, rows, :].astype(jnp.float32) + side[0, rows, :].astype(jnp.float32) + side[1, rows, :].astype(jnp.float32)
        total = resid_ref[rows, :].astype(jnp.float32) + total + bias_ref[...].astype(jnp.float32)
        if regather:
            out_ref[ch, rows, :] = total.astype(out_ref.dtype)
            y_send(6, r).start()
            y_send(7, r).start()
        else:
            out_ref[rows, :] = total.astype(out_ref.dtype)

    def relay(r):
        if regather:
            y_recv(6, r)
            y_recv(7, r)
            y_send(8, r).start()
            y_send(9, r).start()

    barrier = pltpu.get_barrier_semaphore()
    for to in ({'wd': partner}, {'wd': x_left}, {'wd': x_right}, {'ch': y_left}, {'ch': y_right}):
        pl.semaphore_signal(barrier, inc=1, device_id=to, device_id_type=MESH)
    own = pltpu.make_async_copy(h_ref, hbuf.at[:, :, pl.ds(pl.multiple_of(wd * depth, depth), depth)], own_sem)
    own.start()
    pl.semaphore_wait(barrier, 5)
    start_own(0)
    start_own(1)
    for r in range(ROUNDS):
        x_recv(0, r)
        x_send(2, r).start()
        x_recv(1, r)
        x_send(3, r).start()
        x_send(5, r).start()
        x_send(6, r).start()
        if r + 2 < ROUNDS:
            start_own(r + 2)
        if r >= 1:
            combine(r - 1)
        x_recv(2, r)
        x_send(7, r).start()
        x_recv(3, r)
        x_send(8, r).start()
        for k in range(4, 9):
            x_recv(k, r)
        if r == 0:
            own.wait()
        dots(r)
        if r >= 1:
            final(r - 1)
        if r >= 2:
            relay(r - 2)
    combine(ROUNDS - 1)
    relay(ROUNDS - 2)
    final(ROUNDS - 1)
    relay(ROUNDS - 1)
    for r in range(ROUNDS):
        if regather:
            y_recv(8, r)
            y_recv(9, r)
        for k in range(9):
            x_send(k, r).wait_send()
        for k in range(10 if regather else 6):
            y_send(k, r).wait_send()


def ring_layer(h, w, resid, bias, ring_y, regather, cid):
    tokens, depth = h.shape
    share = tokens // ring_y
    wide, cols = w.shape
    dtype = jnp.bfloat16 if regather else jnp.float32
    out = jax.ShapeDtypeStruct((ring_y, share, cols) if regather else (share, cols), dtype)
    vmem = pl.BlockSpec(memory_space=pltpu.VMEM)
    res = pl.pallas_call(
        functools.partial(ring_kernel, regather),
        out_shape=out,
        in_specs=[pl.BlockSpec(memory_space=pl.ANY), vmem, vmem, vmem],
        out_specs=vmem,
        scratch_shapes=[
            pltpu.VMEM((ring_y, share, wide), jnp.bfloat16),
            pltpu.VMEM((ring_y, share, cols), jnp.bfloat16),
            pltpu.VMEM((2, share // 2, cols), jnp.bfloat16),
            pltpu.VMEM((2, share, cols), jnp.bfloat16),
            pltpu.SemaphoreType.DMA((ROUNDS, 9)), pltpu.SemaphoreType.DMA((ROUNDS, 9)),
            pltpu.SemaphoreType.DMA((ROUNDS, 10)), pltpu.SemaphoreType.DMA((ROUNDS, 10)),
            pltpu.SemaphoreType.DMA,
        ],
        compiler_params=pltpu.CompilerParams(collective_id=cid, has_side_effects=True, vmem_limit_bytes=60 << 20),
        name='ring_layer',
    )(h.reshape(ring_y, share, depth), w, resid, bias)
    return res.reshape(tokens, cols) if regather else res


def solution(mesh):
    wd_count = mesh.shape['wd']
    ch_count = mesh.shape['ch']
    chips = wd_count // CORES
    row_spec = P('dp', 'wd')
    specs = (row_spec, P('dp', None), P('wd'), P('wd', 'ch'), P('ch'), P('wd', 'ch'), P('ch'), P(None, 'ch'), P('ch'), P('ch'), P('ch', None, None), P('ch'), P('ch', None, None), P('ch'), P('ch', 'wd'), P('wd'), P('wd'), P('wd', 'ch'), P('ch'), P('wd', 'ch'), P('ch'), P('ch', 'wd'), P('wd'))
    swap = [(i, i + 1 - 2 * (i % CORES)) for i in range(wd_count)]
    same_core = [[x * CORES + c for x in range(chips)] for c in range(CORES)]

    def local_layer(resid_in, seg_pos, gain_temporal, w_x, bias_x, w_y, bias_y, conv_w, conv_bias, lam_param, rgate_w, rgate_b, igate_w, igate_b, w_o, bias_o, gain_mlp, w_g, bias_g, w_u, bias_u, w_d, bias_d):
        tokens, local_width = resid_in.shape
        model_width = local_width * wd_count
        share = tokens // ch_count
        rnn = w_x.shape[1]
        mine = rnn // wd_count
        wd_i = lax.axis_index('wd')
        core = wd_i % CORES
        block = wd_i // CORES
        positions = seg_pos.reshape(tokens)

        def own(vec):
            return lax.dynamic_slice_in_dim(vec, wd_i * mine, mine, axis=vec.ndim - 1)

        def both(vec):
            pair = lax.dynamic_slice_in_dim(vec, block * CORES * mine, CORES * mine, axis=vec.ndim - 1)
            return jnp.where(core == 0, pair, jnp.concatenate([pair[..., mine:], pair[..., :mine]], axis=-1))

        ff = w_g.shape[1] // wd_count
        pieces = jnp.concatenate([w_g.reshape(local_width, wd_count, ff), w_u.reshape(local_width, wd_count, ff)], axis=2)
        mlp_w = lax.all_to_all(pieces.transpose(1, 0, 2), 'wd', 0, 0)

        resid32 = resid_in.astype(jnp.float32)
        sum_sq = lax.psum(jnp.sum(resid32 * resid32, axis=1, keepdims=True), 'wd')
        normed = rms_apply(resid32, sum_sq, model_width, gain_temporal)
        normed_pair = lax.ppermute(normed, 'wd', swap)
        w_xy = jnp.concatenate([w_x.reshape(local_width, chips, CORES, mine), w_y.reshape(local_width, chips, CORES, mine)], axis=3)
        w_keep = lax.dynamic_index_in_dim(w_xy, core, 2, keepdims=False).reshape(local_width, rnn)
        w_send = lax.dynamic_index_in_dim(w_xy, 1 - core, 2, keepdims=False).reshape(local_width, rnn)
        w_pair = lax.ppermute(w_send, 'wd', swap)
        part = (jnp.dot(normed, w_keep, preferred_element_type=jnp.float32) + jnp.dot(normed_pair, w_pair, preferred_element_type=jnp.float32)).astype(jnp.bfloat16)
        got = lax.all_to_all(part.reshape(tokens, chips, CORES * mine).transpose(1, 0, 2), 'wd', 0, 0, axis_index_groups=same_core)
        uy = jnp.sum(got.astype(jnp.float32), axis=0)
        u_own = (uy[:, :mine] + own(bias_x).astype(jnp.float32)).astype(jnp.bfloat16)
        y_own = jax.nn.gelu(uy[:, mine:] + own(bias_y).astype(jnp.float32), approximate=True).astype(jnp.bfloat16)
        u_pair = jnp.concatenate([u_own, lax.ppermute(u_own, 'wd', swap)], axis=1)
        gate_w = jnp.concatenate([lax.dynamic_index_in_dim(w, block, 0, keepdims=False) for w in (rgate_w, igate_w)], axis=1)
        gate_w = gate_w.reshape(CORES, mine, 2, CORES, mine)
        gate_w = lax.dynamic_index_in_dim(gate_w, core, 3, keepdims=False).reshape(CORES, mine, 2 * mine)
        gate_w = jnp.where(core == 0, gate_w, gate_w[::-1]).reshape(CORES * mine, 2 * mine)
        gate_b = jnp.concatenate([own(rgate_b), own(igate_b)])[None]
        mixed = lru(u_pair, y_own, positions[:, None], both(conv_w), both(conv_bias)[None], gate_w, gate_b, own(lam_param)[None])
        resid_rows = lax.dynamic_slice_in_dim(resid_in, lax.axis_index('ch') * share, share, axis=0)
        resid = ring_layer(mixed, w_o, resid_rows, bias_o[None], ch_count, False, 1)
        sum_sq2 = lax.psum(jnp.sum(resid * resid, axis=1, keepdims=True), 'wd')
        normed2 = rms_apply(resid, sum_sq2, model_width, gain_mlp)
        all2 = lax.all_gather(normed2, ('ch', 'wd'), axis=0).reshape(ch_count, wd_count, share, local_width)
        mlp_b = jnp.concatenate([lax.dynamic_slice_in_dim(b, wd_i * ff, ff) for b in (bias_g, bias_u)])[None]
        inner = gate_up(all2, mlp_w, mlp_b)
        return ring_layer(inner, w_d, resid, bias_d[None], ch_count, True, 2)

    return jax.shard_map(local_layer, mesh=mesh, in_specs=specs, out_specs=row_spec, check_vma=False)
```

```python
import functools

import jax
import jax.numpy as jnp
from jax import lax
from jax.experimental import pallas as pl
from jax.experimental.pallas import tpu as pltpu
from jax.sharding import PartitionSpec as P

EPS = 1e-6
CORES = 2
SEGS = 8
PAD = 8


def rms_apply(vals, sum_sq, width, gain):
    return (vals * lax.rsqrt(sum_sq / width + EPS) * (1.0 + gain.astype(jnp.float32))).astype(jnp.bfloat16)


def neg_expm1(z):
    series = -z * (1.0 + z * (0.5 + z * (1.0 / 6.0 + z * (1.0 / 24.0))))
    return jnp.where(z > -0.03, series, 1.0 - jnp.exp(z))


def lru_kernel(u_ref, y_ref, pos_ref, taps_ref, cbias_ref, gate_w_ref, gate_b_ref, lam_ref, w_g_ref, w_u_ref, out_ref, mlp_w_ref, u32, a_s, b_s, own_w, own_sem, ws, wr):
    ring_x, _, _, wd, core, chip = ring_refs()
    depth = w_g_ref.shape[0]
    ff = own_w.shape[2]
    here = pl.ds(pl.multiple_of(chip * depth, depth), depth)

    def piece(src_ref, k, to_chip):
        return src_ref.at[:, pl.ds(pl.multiple_of((to_chip * CORES + k) * ff, ff), ff)]

    def exchange(step):
        to = lax.rem(chip + step, ring_x)
        return [pltpu.make_async_remote_copy(src_ref=piece(src, k, to), dst_ref=mlp_w_ref.at[k, here, pl.ds(m * ff, ff)],
                                             send_sem=ws.at[step, 2 * k + m], recv_sem=wr.at[step, 2 * k + m],
                                             device_id={'wd': to * CORES + core}, device_id_type=MESH)
                for k in range(CORES) for m, src in enumerate((w_g_ref, w_u_ref))]

    barrier = pltpu.get_barrier_semaphore()
    for step in range(1, ring_x):
        pl.semaphore_signal(barrier, inc=1, device_id={'wd': lax.rem(chip + step, ring_x) * CORES + core}, device_id_type=MESH)
    inward = [pltpu.make_async_copy(piece(src, k, chip), own_w.at[2 * k + m], own_sem.at[2 * k + m]) for k in range(CORES) for m, src in enumerate((w_g_ref, w_u_ref))]
    for one in inward:
        one.start()
    pl.semaphore_wait(barrier, ring_x - 1)
    for step in range(1, ring_x):
        for one in exchange(step):
            one.start()
    for one in inward:
        one.wait()
    outward = [pltpu.make_async_copy(own_w.at[2 * k + m], mlp_w_ref.at[k, here, pl.ds(m * ff, ff)], own_sem.at[2 * k + m]) for k in range(CORES) for m in range(2)]
    for one in outward:
        one.start()
    tokens, wide = u_ref.shape
    width = y_ref.shape[1]
    tile = tokens // SEGS
    pitch = tile + PAD
    taps = taps_ref[...].astype(jnp.float32)
    n_taps = taps_ref.shape[0]
    cbias = cbias_ref[...].astype(jnp.float32)
    gate_b = gate_b_ref[...].astype(jnp.float32)
    lam = -lam_ref[...]
    soft = -8.0 * (jnp.maximum(lam, 0.0) + jnp.log(1.0 + jnp.exp(-jnp.abs(lam))))
    u32[0:PAD, :] = jnp.zeros((PAD, wide), jnp.float32)

    def widen(i, carry):
        rows = pl.multiple_of(i * tile, tile)
        u32[pl.ds(rows + PAD, tile), :] = u_ref[pl.ds(rows, tile), :].astype(jnp.float32)
        return carry
    lax.fori_loop(0, SEGS, widen, 0)

    sub = tile // 4

    def gates(i, carry):
        rows = pl.multiple_of(i * sub, sub)
        window = u32[pl.ds(rows, sub + PAD), :]
        pos = pos_ref[pl.ds(rows, sub), :]
        total = cbias + window[PAD:] * taps[0:1]
        for k in range(1, n_taps):
            total = total + jnp.where(pos >= k, window[PAD - k:PAD - k + sub], 0.0) * taps[k:k + 1]
        conv = total.astype(jnp.bfloat16)
        pre = jnp.dot(conv, gate_w_ref[...], preferred_element_type=jnp.float32) + gate_b
        both = jax.nn.sigmoid(pre)
        log_a = both[:, :width] * soft
        reset = pos == 0
        decay = jnp.where(reset, 0.0, jnp.exp(log_a))
        scale = jnp.where(reset, 1.0, jnp.sqrt(neg_expm1(2.0 * log_a)))
        drive = scale * both[:, width:] * conv[:, :width].astype(jnp.float32)
        seg = i // 4
        at = pl.multiple_of(seg * pitch + (i - seg * 4) * sub, 8)
        a_s[pl.ds(at, sub), :] = decay
        b_s[pl.ds(at, sub), :] = drive
        return carry
    lax.fori_loop(0, SEGS * 4, gates, 0)

    def steps(i, carry):
        hid, acc = carry
        for j in range(8):
            t = i * 8 + j
            a = a_s[pl.ds(t, SEGS, stride=pitch), :]
            hid = a * hid + b_s[pl.ds(t, SEGS, stride=pitch), :]
            acc = a * acc
            b_s[pl.ds(t, SEGS, stride=pitch), :] = hid
            a_s[pl.ds(t, SEGS, stride=pitch), :] = acc
        return hid, acc
    hid, acc = lax.fori_loop(0, tile // 8, steps, (jnp.zeros((SEGS, width), jnp.float32), jnp.ones((SEGS, width), jnp.float32)))

    entry = jnp.zeros((1, width), jnp.float32)
    for seg in range(SEGS):
        for q in range(4):
            at = seg * pitch + q * sub
            hidden = b_s[at:at + sub, :] + a_s[at:at + sub, :] * entry
            rows = slice(seg * tile + q * sub, seg * tile + (q + 1) * sub)
            out_ref[rows, :] = (hidden * y_ref[rows, :].astype(jnp.float32)).astype(jnp.bfloat16)
        entry = hid[seg:seg + 1] + acc[seg:seg + 1] * entry
    for one in outward:
        one.wait()
    for step in range(1, ring_x):
        for one in exchange(step):
            one.wait()


def lru(u_pair, y_rows, pos, taps, cbias, gate_w, gate_b, lam, w_g, w_u, ring_x, cid):
    tokens, wide = u_pair.shape
    width = y_rows.shape[1]
    rows = SEGS * (tokens // SEGS + PAD)
    depth, ff = w_g.shape[0], w_g.shape[1] // (ring_x * CORES)
    vmem, anywhere = pl.BlockSpec(memory_space=pltpu.VMEM), pl.BlockSpec(memory_space=pl.ANY)
    return pl.pallas_call(
        lru_kernel,
        out_shape=(jax.ShapeDtypeStruct((tokens, width), jnp.bfloat16), jax.ShapeDtypeStruct((CORES, ring_x * depth, 2 * ff), jnp.bfloat16)),
        in_specs=[vmem] * 8 + [anywhere] * 2,
        out_specs=(vmem, anywhere),
        scratch_shapes=[pltpu.VMEM((tokens + PAD, wide), jnp.float32), pltpu.VMEM((rows, width), jnp.float32), pltpu.VMEM((rows, width), jnp.float32),
                        pltpu.VMEM((2 * CORES, depth, ff), jnp.bfloat16), pltpu.SemaphoreType.DMA((2 * CORES,)),
                        pltpu.SemaphoreType.DMA((ring_x, 2 * CORES)), pltpu.SemaphoreType.DMA((ring_x, 2 * CORES))],
        compiler_params=pltpu.CompilerParams(collective_id=cid, has_side_effects=True, vmem_limit_bytes=48 << 20),
        name='lru',
    )(u_pair, y_rows, pos, taps, cbias, gate_w, gate_b, lam, w_g, w_u)


MESH = pl.DeviceIdType.MESH
ROUNDS = 4


def ring_kernel(regather, h_ref, w_ref, resid_ref, bias_ref, out_ref, hbuf, pbuf, opp_buf, side, xs, xr, ys, yr, own_sem):
    share, depth = h_ref.shape[1:]
    rr = share // ROUNDS
    half = rr // 2
    ring_x = lax.axis_size('wd') // CORES
    ring_y = lax.axis_size('ch')
    ch = lax.axis_index('ch')
    wd = lax.axis_index('wd')
    core = lax.rem(wd, CORES)
    chip = wd // CORES
    other = 1 - 2 * core

    def along_x(step):
        return lax.rem(chip + step, ring_x) * CORES + core

    x_right, x_opp, x_left = along_x(1), along_x(2), along_x(3)
    y_right, y_opp, y_left = (lax.rem(ch + step, ring_y) for step in (1, 2, 3))
    partner = wd + other

    def span(r, part):
        if part is None:
            return pl.ds(r * rr, rr)
        return pl.ds(r * rr + part * half, half)

    def cols(owner, r, part=None):
        return hbuf.at[:, span(r, part), pl.ds(pl.multiple_of(owner * depth, depth), depth)]

    def x_send(k, r):
        if k in (0, 1, 4):
            src, dst = h_ref.at[:, span(r, None)], cols(wd, r)
        else:
            owner, part = {2: (x_left, 0), 3: (x_right, 1), 5: (x_left, None), 6: (x_right, None), 7: (x_opp, 0), 8: (x_opp, 1)}[k]
            src = dst = cols(owner, r, part)
        to = {0: x_right, 1: x_left, 2: x_right, 3: x_left}.get(k, partner)
        return pltpu.make_async_remote_copy(src_ref=src, dst_ref=dst, send_sem=xs.at[r, k], recv_sem=xr.at[r, k], device_id={'wd': to}, device_id_type=MESH)

    def x_recv(k, r):
        owner, part = {0: (x_left, None), 1: (x_right, None), 2: (x_opp, 0), 3: (x_opp, 1), 4: (partner, None), 5: (x_left + other, None),
                       6: (x_right + other, None), 7: (x_opp + other, 0), 8: (x_opp + other, 1)}[k]
        ref = cols(owner, r, part)
        pltpu.make_async_remote_copy(src_ref=ref, dst_ref=ref, send_sem=xs.at[r, k], recv_sem=xr.at[r, k], device_id={'wd': partner}, device_id_type=MESH).wait_recv()

    def y_refs(k, r):
        opp_rows = pl.ds(r * half, half)
        a, b, full = span(r, 0), span(r, 1), span(r, None)
        if k < 6:
            src, dst, to = {
                0: (pbuf.at[0, a], opp_buf.at[0, opp_rows], y_right),
                1: (pbuf.at[0, b], opp_buf.at[1, opp_rows], y_left),
                2: (pbuf.at[3, b], side.at[0, b], y_right),
                3: (pbuf.at[1, a], side.at[1, a], y_left),
                4: (pbuf.at[3, a], side.at[0, a], y_right),
                5: (pbuf.at[1, b], side.at[1, b], y_left),
            }[k]
            return src, dst, to, dst
        owner, part, to, got = {
            6: (ch, full, y_right, y_left),
            7: (ch, full, y_left, y_right),
            8: (y_left, a, y_right, y_opp),
            9: (y_right, b, y_left, y_opp),
        }[k]
        return out_ref.at[owner, part], out_ref.at[owner, part], to, out_ref.at[got, part]

    def y_send(k, r):
        src, dst, to, _ = y_refs(k, r)
        return pltpu.make_async_remote_copy(src_ref=src, dst_ref=dst, send_sem=ys.at[r, k], recv_sem=yr.at[r, k], device_id={'ch': to}, device_id_type=MESH)

    def y_recv(k, r):
        ref = y_refs(k, r)[3]
        pltpu.make_async_remote_copy(src_ref=ref, dst_ref=ref, send_sem=ys.at[r, k], recv_sem=yr.at[r, k], device_id={'ch': y_right}, device_id_type=MESH).wait_recv()

    def start_own(r):
        for k in (0, 1, 4):
            x_send(k, r).start()

    def dots(r):
        def one(slot, carry):
            rows_of = lax.rem(ch + 2 + slot, ring_y)
            block = hbuf[rows_of, pl.ds(r * rr, rr), :]
            pbuf[slot, pl.ds(r * rr, rr), :] = jnp.dot(block, w_ref[...], preferred_element_type=jnp.float32).astype(jnp.bfloat16)
            return carry
        lax.fori_loop(0, ring_y, one, 0)
        for k in range(4):
            y_send(k, r).start()

    def combine(r):
        opp_rows = pl.ds(r * half, half)
        y_recv(0, r)
        pbuf[3, span(r, 0), :] = (pbuf[3, span(r, 0), :].astype(jnp.float32) + opp_buf[0, opp_rows, :].astype(jnp.float32)).astype(jnp.bfloat16)
        y_send(4, r).start()
        y_recv(1, r)
        pbuf[1, span(r, 1), :] = (pbuf[1, span(r, 1), :].astype(jnp.float32) + opp_buf[1, opp_rows, :].astype(jnp.float32)).astype(jnp.bfloat16)
        y_send(5, r).start()

    def final(r):
        for k in range(2, 6):
            y_recv(k, r)
        rows = span(r, None)
        total = pbuf[2, rows, :].astype(jnp.float32) + side[0, rows, :].astype(jnp.float32) + side[1, rows, :].astype(jnp.float32)
        total = resid_ref[rows, :].astype(jnp.float32) + total + bias_ref[...].astype(jnp.float32)
        if regather:
            out_ref[ch, rows, :] = total.astype(out_ref.dtype)
            y_send(6, r).start()
            y_send(7, r).start()
        else:
            out_ref[rows, :] = total.astype(out_ref.dtype)

    def relay(r):
        if regather:
            y_recv(6, r)
            y_recv(7, r)
            y_send(8, r).start()
            y_send(9, r).start()

    barrier = pltpu.get_barrier_semaphore()
    for to in ({'wd': partner}, {'wd': x_left}, {'wd': x_right}, {'ch': y_left}, {'ch': y_right}):
        pl.semaphore_signal(barrier, inc=1, device_id=to, device_id_type=MESH)
    own = pltpu.make_async_copy(h_ref, hbuf.at[:, :, pl.ds(pl.multiple_of(wd * depth, depth), depth)], own_sem)
    own.start()
    pl.semaphore_wait(barrier, 5)
    start_own(0)
    start_own(1)
    for r in range(ROUNDS):
        x_recv(0, r)
        x_send(2, r).start()
        x_recv(1, r)
        x_send(3, r).start()
        x_send(5, r).start()
        x_send(6, r).start()
        if r + 2 < ROUNDS:
            start_own(r + 2)
        if r >= 1:
            combine(r - 1)
        x_recv(2, r)
        x_send(7, r).start()
        x_recv(3, r)
        x_send(8, r).start()
        for k in range(4, 9):
            x_recv(k, r)
        if r == 0:
            own.wait()
        dots(r)
        if r >= 1:
            final(r - 1)
        if r >= 2:
            relay(r - 2)
    combine(ROUNDS - 1)
    relay(ROUNDS - 2)
    final(ROUNDS - 1)
    relay(ROUNDS - 1)
    for r in range(ROUNDS):
        if regather:
            y_recv(8, r)
            y_recv(9, r)
        for k in range(9):
            x_send(k, r).wait_send()
        for k in range(10 if regather else 6):
            y_send(k, r).wait_send()


def ring_layer(h, w, resid, bias, ring_y, regather, cid):
    tokens, depth = h.shape
    share = tokens // ring_y
    wide, cols = w.shape
    dtype = jnp.bfloat16 if regather else jnp.float32
    out = jax.ShapeDtypeStruct((ring_y, share, cols) if regather else (share, cols), dtype)
    vmem = pl.BlockSpec(memory_space=pltpu.VMEM)
    res = pl.pallas_call(
        functools.partial(ring_kernel, regather),
        out_shape=out,
        in_specs=[pl.BlockSpec(memory_space=pl.ANY), vmem, vmem, vmem],
        out_specs=vmem,
        scratch_shapes=[
            pltpu.VMEM((ring_y, share, wide), jnp.bfloat16),
            pltpu.VMEM((ring_y, share, cols), jnp.bfloat16),
            pltpu.VMEM((2, share // 2, cols), jnp.bfloat16),
            pltpu.VMEM((2, share, cols), jnp.bfloat16),
            pltpu.SemaphoreType.DMA((ROUNDS, 9)), pltpu.SemaphoreType.DMA((ROUNDS, 9)),
            pltpu.SemaphoreType.DMA((ROUNDS, 10)), pltpu.SemaphoreType.DMA((ROUNDS, 10)),
            pltpu.SemaphoreType.DMA,
        ],
        compiler_params=pltpu.CompilerParams(collective_id=cid, has_side_effects=True, vmem_limit_bytes=60 << 20),
        name='ring_layer',
    )(h.reshape(ring_y, share, depth), w, resid, bias)
    return res.reshape(tokens, cols) if regather else res


def ring_refs():
    ring_x = lax.axis_size('wd') // CORES
    ring_y = lax.axis_size('ch')
    ch = lax.axis_index('ch')
    wd = lax.axis_index('wd')
    core = lax.rem(wd, CORES)
    return ring_x, ring_y, ch, wd, core, wd // CORES


def mlp_in_kernel(resid_ref, gain_ref, w_ref, bias_ref, out_ref, nbuf, keep, send, got, sums, all_sums, ns, nr, ss, sr):
    share, width = resid_ref.shape
    ring_x, ring_y, ch, wd, core, chip = ring_refs()
    wd_count = ring_x * CORES
    rr = share // ROUNDS
    half = rr // 2
    partner = wd + 1 - 2 * core
    lanes = sums.shape[1]

    def device(d1, d2):
        return {'ch': lax.rem(ch + d1 * (1 - core) + d2 * core, ring_y), 'wd': lax.rem(chip + d1 * core + d2 * (1 - core), ring_x) * CORES + core}

    def block(d1, d2, r, part=None):
        rows = pl.ds(r * rr, rr) if part is None else pl.ds(r * rr + part * half, half)
        at = lax.rem(chip + d1 * core + d2 * (1 - core), ring_x)
        return nbuf.at[lax.rem(ch + d1 * (1 - core) + d2 * core, ring_y), rows, pl.ds(pl.multiple_of(at * width, width), width)]

    firsts = (0, 3, 1, 2)

    def route(k, r):
        if k < 4:
            src, to, dst = (((0, 0, r), (1, 0), (3, 0, r)), ((0, 0, r), (3, 0), (1, 0, r)),
                            ((3, 0, r, 0), (1, 0), (2, 0, r, 0)), ((1, 0, r, 1), (3, 0), (2, 0, r, 1)))[k]
        else:
            d1 = firsts[(k - 4) // 4]
            src, to, dst = (((d1, 0, r), (0, 1), (d1, 3, r)), ((d1, 0, r), (0, 3), (d1, 1, r)),
                            ((d1, 3, r, 0), (0, 1), (d1, 2, r, 0)), ((d1, 1, r, 1), (0, 3), (d1, 2, r, 1)))[k % 4]
        return block(*src), to, block(*dst)

    def start(r, *ks):
        for k in ks:
            src, to, _ = route(k, r)
            pltpu.make_async_remote_copy(src_ref=src, dst_ref=src, send_sem=ns.at[r, k], recv_sem=nr.at[r, k], device_id=device(*to), device_id_type=MESH).start()

    def wait(r, *ks):
        for k in ks:
            ref = route(k, r)[2]
            pltpu.make_async_remote_copy(src_ref=ref, dst_ref=ref, send_sem=ns.at[r, k], recv_sem=nr.at[r, k], device_id=device(1, 0), device_id_type=MESH).wait_recv()

    def own(r):
        if r < ROUNDS:
            start(r, 0, 1, 4, 5)

    def stage1(r):
        if r < ROUNDS:
            wait(r, 0, 1)
            start(r, 2, 3, 8, 9, 12, 13)
            wait(r, 4, 5)
            start(r, 6, 7)

    def stage2(r):
        if r < ROUNDS:
            wait(r, 2, 3)
            start(r, 16, 17)
            wait(r, 8, 9)
            start(r, 10, 11)
            wait(r, 12, 13)
            start(r, 14, 15)

    def stage3(r):
        if r < ROUNDS:
            wait(r, 16, 17)
            start(r, 18, 19)

    def halves(r):
        return pltpu.make_async_remote_copy(src_ref=send.at[r], dst_ref=got.at[r], send_sem=ns.at[r, 20], recv_sem=nr.at[r, 20], device_id={'wd': partner}, device_id_type=MESH)

    def dots(r, mine):
        def one(q, carry):
            block_in = nbuf[q, pl.ds(r * rr, rr), :]
            if mine:
                keep[q] = jnp.dot(block_in, w_ref[core], preferred_element_type=jnp.float32)
            else:
                send[r, q] = jnp.dot(block_in, w_ref[1 - core], preferred_element_type=jnp.float32).astype(jnp.bfloat16)
            return carry
        lax.fori_loop(0, ring_y, one, 0)

    def finish(r):
        halves(r).wait_recv()
        mid = out_ref.shape[2]

        def one(q, carry):
            total = keep[q] + got[r, q].astype(jnp.float32) + bias_ref[...].astype(jnp.float32)
            out_ref[q, pl.ds(r * rr, rr), :] = (jax.nn.gelu(total[:, :mid], approximate=True) * total[:, mid:]).astype(jnp.bfloat16)
            return carry
        lax.fori_loop(0, ring_y, one, 0)

    barrier = pltpu.get_barrier_semaphore()
    for step in range(1, wd_count):
        pl.semaphore_signal(barrier, inc=1, device_id={'wd': lax.rem(wd + step, wd_count)}, device_id_type=MESH)
    for step in (1, 3):
        pl.semaphore_signal(barrier, inc=1, device_id={'ch': lax.rem(ch + step, ring_y)}, device_id_type=MESH)

    tiles = share // lanes
    for i in range(tiles):
        sq = jnp.zeros((lanes, lanes), jnp.float32)
        for j in range(width // lanes):
            val = resid_ref[i * lanes:(i + 1) * lanes, j * lanes:(j + 1) * lanes]
            sq = sq + val * val
        sums[i:i + 1, :] = jnp.sum(sq.T, axis=0, keepdims=True)
    all_sums[wd] = sums[...]
    pl.semaphore_wait(barrier, wd_count + 1)
    for step in range(1, wd_count):
        pltpu.make_async_remote_copy(src_ref=sums, dst_ref=all_sums.at[wd], send_sem=ss.at[step], recv_sem=sr.at[step], device_id={'wd': lax.rem(wd + step, wd_count)}, device_id_type=MESH).start()
    for step in range(1, wd_count):
        ref = all_sums.at[lax.rem(wd + wd_count - step, wd_count)]
        pltpu.make_async_remote_copy(src_ref=ref, dst_ref=ref, send_sem=ss.at[step], recv_sem=sr.at[step], device_id={'wd': partner}, device_id_type=MESH).wait_recv()
    scale = lax.rsqrt(jnp.sum(all_sums[...], axis=0) / (width * wd_count) + EPS)
    at = pl.ds(pl.multiple_of(chip * width, width), width)
    gain = 1.0 + gain_ref[...].astype(jnp.float32)
    for i in range(tiles):
        factor = jnp.broadcast_to(scale[i:i + 1, :], (lanes, lanes)).T[:, 0:1]
        rows = slice(i * lanes, (i + 1) * lanes)
        nbuf[ch, rows, at] = (resid_ref[rows, :] * factor * gain).astype(jnp.bfloat16)
    own(0)
    own(1)
    stage1(0)
    own(2)
    stage2(0)
    stage1(1)
    stage3(0)
    stage2(1)
    for r in range(ROUNDS):
        wait(r, 6, 7, 10, 11, 14, 15, 18, 19)
        dots(r, False)
        halves(r).start()
        own(r + 3)
        stage1(r + 2)
        stage3(r + 1)
        dots(r, True)
        stage2(r + 2)
        finish(r)
    for step in range(1, wd_count):
        pltpu.make_async_remote_copy(src_ref=sums, dst_ref=all_sums.at[wd], send_sem=ss.at[step], recv_sem=sr.at[step], device_id={'wd': partner}, device_id_type=MESH).wait_send()
    for r in range(ROUNDS):
        halves(r).wait_send()
        for k in range(20):
            src, to, _ = route(k, r)
            pltpu.make_async_remote_copy(src_ref=src, dst_ref=src, send_sem=ns.at[r, k], recv_sem=nr.at[r, k], device_id=device(*to), device_id_type=MESH).wait_send()


def mlp_in(resid, gain, weight, bias, ring_x, ring_y, cid):
    share, width = resid.shape
    _, depth, cols = weight.shape
    lanes = 128
    rr = share // ROUNDS
    vmem = pl.BlockSpec(memory_space=pltpu.VMEM)
    out = pl.pallas_call(
        mlp_in_kernel,
        out_shape=jax.ShapeDtypeStruct((ring_y, share, cols // 2), jnp.bfloat16),
        in_specs=[vmem] * 4,
        out_specs=vmem,
        scratch_shapes=[
            pltpu.VMEM((ring_y, share, depth), jnp.bfloat16),
            pltpu.VMEM((ring_y, rr, cols), jnp.float32),
            pltpu.VMEM((ROUNDS, ring_y, rr, cols), jnp.bfloat16),
            pltpu.VMEM((ROUNDS, ring_y, rr, cols), jnp.bfloat16),
            pltpu.VMEM((share // lanes, lanes), jnp.float32),
            pltpu.VMEM((ring_x * CORES, share // lanes, lanes), jnp.float32),
            pltpu.SemaphoreType.DMA((ROUNDS, 21)), pltpu.SemaphoreType.DMA((ROUNDS, 21)),
            pltpu.SemaphoreType.DMA((ring_x * CORES,)), pltpu.SemaphoreType.DMA((ring_x * CORES,)),
        ],
        compiler_params=pltpu.CompilerParams(collective_id=cid, has_side_effects=True, vmem_limit_bytes=60 << 20),
        name='mlp_in',
    )(resid, gain, weight, bias)
    return out.reshape(ring_y * share, cols // 2)


def solution(mesh):
    wd_count = mesh.shape['wd']
    ch_count = mesh.shape['ch']
    chips = wd_count // CORES
    row_spec = P('dp', 'wd')
    specs = (row_spec, P('dp', None), P('wd'), P('wd', 'ch'), P('ch'), P('wd', 'ch'), P('ch'), P(None, 'ch'), P('ch'), P('ch'), P('ch', None, None), P('ch'), P('ch', None, None), P('ch'), P('ch', 'wd'), P('wd'), P('wd'), P('wd', 'ch'), P('ch'), P('wd', 'ch'), P('ch'), P('ch', 'wd'), P('wd'))
    swap = [(i, i + 1 - 2 * (i % CORES)) for i in range(wd_count)]
    same_core = [[x * CORES + c for x in range(chips)] for c in range(CORES)]

    def local_layer(resid_in, seg_pos, gain_temporal, w_x, bias_x, w_y, bias_y, conv_w, conv_bias, lam_param, rgate_w, rgate_b, igate_w, igate_b, w_o, bias_o, gain_mlp, w_g, bias_g, w_u, bias_u, w_d, bias_d):
        tokens, local_width = resid_in.shape
        model_width = local_width * wd_count
        share = tokens // ch_count
        rnn = w_x.shape[1]
        mine = rnn // wd_count
        wd_i = lax.axis_index('wd')
        core = wd_i % CORES
        block = wd_i // CORES
        positions = seg_pos.reshape(tokens)

        def own(vec):
            return lax.dynamic_slice_in_dim(vec, wd_i * mine, mine, axis=vec.ndim - 1)

        def both(vec):
            pair = lax.dynamic_slice_in_dim(vec, block * CORES * mine, CORES * mine, axis=vec.ndim - 1)
            return jnp.where(core == 0, pair, jnp.concatenate([pair[..., mine:], pair[..., :mine]], axis=-1))

        ff = w_g.shape[1] // wd_count
        resid32 = resid_in.astype(jnp.float32)
        sum_sq = lax.psum(jnp.sum(resid32 * resid32, axis=1, keepdims=True), 'wd')
        normed = rms_apply(resid32, sum_sq, model_width, gain_temporal)
        normed_pair = lax.ppermute(normed, 'wd', swap)
        w_xy = jnp.concatenate([w_x.reshape(local_width, chips, CORES, mine), w_y.reshape(local_width, chips, CORES, mine)], axis=3)
        w_keep = lax.dynamic_index_in_dim(w_xy, core, 2, keepdims=False).reshape(local_width, rnn)
        w_send = lax.dynamic_index_in_dim(w_xy, 1 - core, 2, keepdims=False).reshape(local_width, rnn)
        w_pair = lax.ppermute(w_send, 'wd', swap)
        part = (jnp.dot(normed, w_keep, preferred_element_type=jnp.float32) + jnp.dot(normed_pair, w_pair, preferred_element_type=jnp.float32)).astype(jnp.bfloat16)
        got = lax.all_to_all(part.reshape(tokens, chips, CORES * mine).transpose(1, 0, 2), 'wd', 0, 0, axis_index_groups=same_core)
        uy = jnp.sum(got.astype(jnp.float32), axis=0)
        u_own = (uy[:, :mine] + own(bias_x).astype(jnp.float32)).astype(jnp.bfloat16)
        y_own = jax.nn.gelu(uy[:, mine:] + own(bias_y).astype(jnp.float32), approximate=True).astype(jnp.bfloat16)
        u_pair = jnp.concatenate([u_own, lax.ppermute(u_own, 'wd', swap)], axis=1)
        gate_w = jnp.concatenate([lax.dynamic_index_in_dim(w, block, 0, keepdims=False) for w in (rgate_w, igate_w)], axis=1)
        gate_w = gate_w.reshape(CORES, mine, 2, CORES, mine)
        gate_w = lax.dynamic_index_in_dim(gate_w, core, 3, keepdims=False).reshape(CORES, mine, 2 * mine)
        gate_w = jnp.where(core == 0, gate_w, gate_w[::-1]).reshape(CORES * mine, 2 * mine)
        gate_b = jnp.concatenate([own(rgate_b), own(igate_b)])[None]
        mixed, mlp_w = lru(u_pair, y_own, positions[:, None], both(conv_w), both(conv_bias)[None], gate_w, gate_b, own(lam_param)[None], w_g, w_u, chips, 3)
        resid_rows = lax.dynamic_slice_in_dim(resid_in, lax.axis_index('ch') * share, share, axis=0)
        resid = ring_layer(mixed, w_o, resid_rows, bias_o[None], ch_count, False, 1)
        mlp_b = jnp.concatenate([lax.dynamic_slice_in_dim(b, wd_i * ff, ff) for b in (bias_g, bias_u)])[None]
        inner = mlp_in(resid, gain_mlp[None], mlp_w, mlp_b, chips, ch_count, 4)
        return ring_layer(inner, w_d, resid, bias_d[None], ch_count, True, 2)

    return jax.shard_map(local_layer, mesh=mesh, in_specs=specs, out_specs=row_spec, check_vma=False)
```

```python
import functools

import jax
import jax.numpy as jnp
from jax import lax
from jax.experimental import pallas as pl
from jax.experimental.pallas import tpu as pltpu
from jax.sharding import PartitionSpec as P

EPS = 1e-6
CORES = 2
SEGS = 8
PAD = 8


def neg_expm1(z):
    series = -z * (1.0 + z * (0.5 + z * (1.0 / 6.0 + z * (1.0 / 24.0))))
    return jnp.where(z > -0.03, series, 1.0 - jnp.exp(z))


def lru_kernel(u_ref, y_ref, pos_ref, taps_ref, cbias_ref, gate_w_ref, gate_b_ref, lam_ref, w_g_ref, w_u_ref, out_ref, mlp_w_ref, u32, a_s, b_s, own_w, own_sem, ws, wr):
    ring_x, _, _, wd, core, chip = ring_refs()
    depth = w_g_ref.shape[0]
    ff = own_w.shape[2]
    here = pl.ds(pl.multiple_of(chip * depth, depth), depth)

    def piece(src_ref, k, to_chip):
        return src_ref.at[:, pl.ds(pl.multiple_of((to_chip * CORES + k) * ff, ff), ff)]

    def exchange(step):
        to = lax.rem(chip + step, ring_x)
        return [pltpu.make_async_remote_copy(src_ref=piece(src, k, to), dst_ref=mlp_w_ref.at[k, here, pl.ds(m * ff, ff)],
                                             send_sem=ws.at[step, 2 * k + m], recv_sem=wr.at[step, 2 * k + m],
                                             device_id={'wd': to * CORES + core}, device_id_type=MESH)
                for k in range(CORES) for m, src in enumerate((w_g_ref, w_u_ref))]

    barrier = pltpu.get_barrier_semaphore()
    for step in range(1, ring_x):
        pl.semaphore_signal(barrier, inc=1, device_id={'wd': lax.rem(chip + step, ring_x) * CORES + core}, device_id_type=MESH)
    inward = [pltpu.make_async_copy(piece(src, k, chip), own_w.at[2 * k + m], own_sem.at[2 * k + m]) for k in range(CORES) for m, src in enumerate((w_g_ref, w_u_ref))]
    for one in inward:
        one.start()
    pl.semaphore_wait(barrier, ring_x - 1)
    for step in range(1, ring_x):
        for one in exchange(step):
            one.start()
    for one in inward:
        one.wait()
    outward = [pltpu.make_async_copy(own_w.at[2 * k + m], mlp_w_ref.at[k, here, pl.ds(m * ff, ff)], own_sem.at[2 * k + m]) for k in range(CORES) for m in range(2)]
    for one in outward:
        one.start()
    tokens, wide = u_ref.shape
    width = y_ref.shape[1]
    tile = tokens // SEGS
    pitch = tile + PAD
    taps = taps_ref[...].astype(jnp.float32)
    n_taps = taps_ref.shape[0]
    cbias = cbias_ref[...].astype(jnp.float32)
    gate_b = gate_b_ref[...].astype(jnp.float32)
    lam = -lam_ref[...]
    soft = -8.0 * (jnp.maximum(lam, 0.0) + jnp.log(1.0 + jnp.exp(-jnp.abs(lam))))
    u32[0:PAD, :] = jnp.zeros((PAD, wide), jnp.float32)

    def widen(i, carry):
        rows = pl.multiple_of(i * tile, tile)
        u32[pl.ds(rows + PAD, tile), :] = u_ref[pl.ds(rows, tile), :].astype(jnp.float32)
        return carry
    lax.fori_loop(0, SEGS, widen, 0)

    sub = tile // 4

    def gates(i, carry):
        rows = pl.multiple_of(i * sub, sub)
        window = u32[pl.ds(rows, sub + PAD), :]
        pos = pos_ref[pl.ds(rows, sub), :]
        total = cbias + window[PAD:] * taps[0:1]
        for k in range(1, n_taps):
            total = total + jnp.where(pos >= k, window[PAD - k:PAD - k + sub], 0.0) * taps[k:k + 1]
        conv = total.astype(jnp.bfloat16)
        pre = jnp.dot(conv, gate_w_ref[...], preferred_element_type=jnp.float32) + gate_b
        both = jax.nn.sigmoid(pre)
        log_a = both[:, :width] * soft
        reset = pos == 0
        decay = jnp.where(reset, 0.0, jnp.exp(log_a))
        scale = jnp.where(reset, 1.0, jnp.sqrt(neg_expm1(2.0 * log_a)))
        drive = scale * both[:, width:] * conv[:, :width].astype(jnp.float32)
        seg = i // 4
        at = pl.multiple_of(seg * pitch + (i - seg * 4) * sub, 8)
        a_s[pl.ds(at, sub), :] = decay
        b_s[pl.ds(at, sub), :] = drive
        return carry
    lax.fori_loop(0, SEGS * 4, gates, 0)

    def steps(i, carry):
        hid, acc = carry
        for j in range(8):
            t = i * 8 + j
            a = a_s[pl.ds(t, SEGS, stride=pitch), :]
            hid = a * hid + b_s[pl.ds(t, SEGS, stride=pitch), :]
            acc = a * acc
            b_s[pl.ds(t, SEGS, stride=pitch), :] = hid
            a_s[pl.ds(t, SEGS, stride=pitch), :] = acc
        return hid, acc
    hid, acc = lax.fori_loop(0, tile // 8, steps, (jnp.zeros((SEGS, width), jnp.float32), jnp.ones((SEGS, width), jnp.float32)))

    entry = jnp.zeros((1, width), jnp.float32)
    for seg in range(SEGS):
        for q in range(4):
            at = seg * pitch + q * sub
            hidden = b_s[at:at + sub, :] + a_s[at:at + sub, :] * entry
            rows = slice(seg * tile + q * sub, seg * tile + (q + 1) * sub)
            out_ref[rows, :] = (hidden * y_ref[rows, :].astype(jnp.float32)).astype(jnp.bfloat16)
        entry = hid[seg:seg + 1] + acc[seg:seg + 1] * entry
    for one in outward:
        one.wait()
    for step in range(1, ring_x):
        for one in exchange(step):
            one.wait()


def lru(u_pair, y_rows, pos, taps, cbias, gate_w, gate_b, lam, w_g, w_u, ring_x, cid):
    tokens, wide = u_pair.shape
    width = y_rows.shape[1]
    rows = SEGS * (tokens // SEGS + PAD)
    depth, ff = w_g.shape[0], w_g.shape[1] // (ring_x * CORES)
    vmem, anywhere = pl.BlockSpec(memory_space=pltpu.VMEM), pl.BlockSpec(memory_space=pl.ANY)
    return pl.pallas_call(
        lru_kernel,
        out_shape=(jax.ShapeDtypeStruct((tokens, width), jnp.bfloat16), jax.ShapeDtypeStruct((CORES, ring_x * depth, 2 * ff), jnp.bfloat16)),
        in_specs=[vmem] * 8 + [anywhere] * 2,
        out_specs=(vmem, anywhere),
        scratch_shapes=[pltpu.VMEM((tokens + PAD, wide), jnp.float32), pltpu.VMEM((rows, width), jnp.float32), pltpu.VMEM((rows, width), jnp.float32),
                        pltpu.VMEM((2 * CORES, depth, ff), jnp.bfloat16), pltpu.SemaphoreType.DMA((2 * CORES,)),
                        pltpu.SemaphoreType.DMA((ring_x, 2 * CORES)), pltpu.SemaphoreType.DMA((ring_x, 2 * CORES))],
        compiler_params=pltpu.CompilerParams(collective_id=cid, has_side_effects=True, vmem_limit_bytes=48 << 20),
        name='lru',
    )(u_pair, y_rows, pos, taps, cbias, gate_w, gate_b, lam, w_g, w_u)


MESH = pl.DeviceIdType.MESH
ROUNDS = 4


def ring_kernel(regather, h_ref, w_ref, resid_ref, bias_ref, out_ref, hbuf, pbuf, opp_buf, side, xs, xr, ys, yr, own_sem):
    share, depth = h_ref.shape[1:]
    rr = share // ROUNDS
    half = rr // 2
    ring_x = lax.axis_size('wd') // CORES
    ring_y = lax.axis_size('ch')
    ch = lax.axis_index('ch')
    wd = lax.axis_index('wd')
    core = lax.rem(wd, CORES)
    chip = wd // CORES
    other = 1 - 2 * core

    def along_x(step):
        return lax.rem(chip + step, ring_x) * CORES + core

    x_right, x_opp, x_left = along_x(1), along_x(2), along_x(3)
    y_right, y_opp, y_left = (lax.rem(ch + step, ring_y) for step in (1, 2, 3))
    partner = wd + other

    def span(r, part):
        if part is None:
            return pl.ds(r * rr, rr)
        return pl.ds(r * rr + part * half, half)

    def cols(owner, r, part=None):
        return hbuf.at[:, span(r, part), pl.ds(pl.multiple_of(owner * depth, depth), depth)]

    def x_send(k, r):
        if k in (0, 1, 4):
            src, dst = h_ref.at[:, span(r, None)], cols(wd, r)
        else:
            owner, part = {2: (x_left, 0), 3: (x_right, 1), 5: (x_left, None), 6: (x_right, None), 7: (x_opp, 0), 8: (x_opp, 1)}[k]
            src = dst = cols(owner, r, part)
        to = {0: x_right, 1: x_left, 2: x_right, 3: x_left}.get(k, partner)
        return pltpu.make_async_remote_copy(src_ref=src, dst_ref=dst, send_sem=xs.at[r, k], recv_sem=xr.at[r, k], device_id={'wd': to}, device_id_type=MESH)

    def x_recv(k, r):
        owner, part = {0: (x_left, None), 1: (x_right, None), 2: (x_opp, 0), 3: (x_opp, 1), 4: (partner, None), 5: (x_left + other, None),
                       6: (x_right + other, None), 7: (x_opp + other, 0), 8: (x_opp + other, 1)}[k]
        ref = cols(owner, r, part)
        pltpu.make_async_remote_copy(src_ref=ref, dst_ref=ref, send_sem=xs.at[r, k], recv_sem=xr.at[r, k], device_id={'wd': partner}, device_id_type=MESH).wait_recv()

    def y_refs(k, r):
        opp_rows = pl.ds(r * half, half)
        a, b, full = span(r, 0), span(r, 1), span(r, None)
        if k < 6:
            src, dst, to = {
                0: (pbuf.at[0, a], opp_buf.at[0, opp_rows], y_right),
                1: (pbuf.at[0, b], opp_buf.at[1, opp_rows], y_left),
                2: (pbuf.at[3, b], side.at[0, b], y_right),
                3: (pbuf.at[1, a], side.at[1, a], y_left),
                4: (pbuf.at[3, a], side.at[0, a], y_right),
                5: (pbuf.at[1, b], side.at[1, b], y_left),
            }[k]
            return src, dst, to, dst
        owner, part, to, got = {
            6: (ch, full, y_right, y_left),
            7: (ch, full, y_left, y_right),
            8: (y_left, a, y_right, y_opp),
            9: (y_right, b, y_left, y_opp),
        }[k]
        return out_ref.at[owner, part], out_ref.at[owner, part], to, out_ref.at[got, part]

    def y_send(k, r):
        src, dst, to, _ = y_refs(k, r)
        return pltpu.make_async_remote_copy(src_ref=src, dst_ref=dst, send_sem=ys.at[r, k], recv_sem=yr.at[r, k], device_id={'ch': to}, device_id_type=MESH)

    def y_recv(k, r):
        ref = y_refs(k, r)[3]
        pltpu.make_async_remote_copy(src_ref=ref, dst_ref=ref, send_sem=ys.at[r, k], recv_sem=yr.at[r, k], device_id={'ch': y_right}, device_id_type=MESH).wait_recv()

    def start_own(r):
        for k in (0, 1, 4):
            x_send(k, r).start()

    def dots(r):
        def one(slot, carry):
            rows_of = lax.rem(ch + 2 + slot, ring_y)
            block = hbuf[rows_of, pl.ds(r * rr, rr), :]
            pbuf[slot, pl.ds(r * rr, rr), :] = jnp.dot(block, w_ref[...], preferred_element_type=jnp.float32).astype(jnp.bfloat16)
            return carry
        lax.fori_loop(0, ring_y, one, 0)
        for k in range(4):
            y_send(k, r).start()

    def combine(r):
        opp_rows = pl.ds(r * half, half)
        y_recv(0, r)
        pbuf[3, span(r, 0), :] = (pbuf[3, span(r, 0), :].astype(jnp.float32) + opp_buf[0, opp_rows, :].astype(jnp.float32)).astype(jnp.bfloat16)
        y_send(4, r).start()
        y_recv(1, r)
        pbuf[1, span(r, 1), :] = (pbuf[1, span(r, 1), :].astype(jnp.float32) + opp_buf[1, opp_rows, :].astype(jnp.float32)).astype(jnp.bfloat16)
        y_send(5, r).start()

    def final(r):
        for k in range(2, 6):
            y_recv(k, r)
        rows = span(r, None)
        total = pbuf[2, rows, :].astype(jnp.float32) + side[0, rows, :].astype(jnp.float32) + side[1, rows, :].astype(jnp.float32)
        total = resid_ref[rows, :].astype(jnp.float32) + total + bias_ref[...].astype(jnp.float32)
        if regather:
            out_ref[ch, rows, :] = total.astype(out_ref.dtype)
            y_send(6, r).start()
            y_send(7, r).start()
        else:
            out_ref[rows, :] = total.astype(out_ref.dtype)

    def relay(r):
        if regather:
            y_recv(6, r)
            y_recv(7, r)
            y_send(8, r).start()
            y_send(9, r).start()

    barrier = pltpu.get_barrier_semaphore()
    for to in ({'wd': partner}, {'wd': x_left}, {'wd': x_right}, {'ch': y_left}, {'ch': y_right}):
        pl.semaphore_signal(barrier, inc=1, device_id=to, device_id_type=MESH)
    own = pltpu.make_async_copy(h_ref, hbuf.at[:, :, pl.ds(pl.multiple_of(wd * depth, depth), depth)], own_sem)
    own.start()
    pl.semaphore_wait(barrier, 5)
    start_own(0)
    start_own(1)
    for r in range(ROUNDS):
        x_recv(0, r)
        x_send(2, r).start()
        x_recv(1, r)
        x_send(3, r).start()
        x_send(5, r).start()
        x_send(6, r).start()
        if r + 2 < ROUNDS:
            start_own(r + 2)
        if r >= 1:
            combine(r - 1)
        x_recv(2, r)
        x_send(7, r).start()
        x_recv(3, r)
        x_send(8, r).start()
        for k in range(4, 9):
            x_recv(k, r)
        if r == 0:
            own.wait()
        dots(r)
        if r >= 1:
            final(r - 1)
        if r >= 2:
            relay(r - 2)
    combine(ROUNDS - 1)
    relay(ROUNDS - 2)
    final(ROUNDS - 1)
    relay(ROUNDS - 1)
    for r in range(ROUNDS):
        if regather:
            y_recv(8, r)
            y_recv(9, r)
        for k in range(9):
            x_send(k, r).wait_send()
        for k in range(10 if regather else 6):
            y_send(k, r).wait_send()


def ring_layer(h, w, resid, bias, ring_y, regather, cid):
    tokens, depth = h.shape
    share = tokens // ring_y
    wide, cols = w.shape
    dtype = jnp.bfloat16 if regather else jnp.float32
    out = jax.ShapeDtypeStruct((ring_y, share, cols) if regather else (share, cols), dtype)
    vmem = pl.BlockSpec(memory_space=pltpu.VMEM)
    res = pl.pallas_call(
        functools.partial(ring_kernel, regather),
        out_shape=out,
        in_specs=[pl.BlockSpec(memory_space=pl.ANY), vmem, vmem, vmem],
        out_specs=vmem,
        scratch_shapes=[
            pltpu.VMEM((ring_y, share, wide), jnp.bfloat16),
            pltpu.VMEM((ring_y, share, cols), jnp.bfloat16),
            pltpu.VMEM((2, share // 2, cols), jnp.bfloat16),
            pltpu.VMEM((2, share, cols), jnp.bfloat16),
            pltpu.SemaphoreType.DMA((ROUNDS, 9)), pltpu.SemaphoreType.DMA((ROUNDS, 9)),
            pltpu.SemaphoreType.DMA((ROUNDS, 10)), pltpu.SemaphoreType.DMA((ROUNDS, 10)),
            pltpu.SemaphoreType.DMA,
        ],
        compiler_params=pltpu.CompilerParams(collective_id=cid, has_side_effects=True, vmem_limit_bytes=60 << 20),
        name='ring_layer',
    )(h.reshape(ring_y, share, depth), w, resid, bias)
    return res.reshape(tokens, cols) if regather else res


def ring_refs():
    ring_x = lax.axis_size('wd') // CORES
    ring_y = lax.axis_size('ch')
    ch = lax.axis_index('ch')
    wd = lax.axis_index('wd')
    core = lax.rem(wd, CORES)
    return ring_x, ring_y, ch, wd, core, wd // CORES


def mlp_in_kernel(resid_ref, gain_ref, w_ref, bias_ref, out_ref, nbuf, keep, send, got, sums, all_sums, ns, nr, ss, sr):
    share, width = resid_ref.shape
    ring_x, ring_y, ch, wd, core, chip = ring_refs()
    wd_count = ring_x * CORES
    rr = share // ROUNDS
    half = rr // 2
    partner = wd + 1 - 2 * core
    lanes = sums.shape[1]

    def device(d1, d2):
        return {'ch': lax.rem(ch + d1 * (1 - core) + d2 * core, ring_y), 'wd': lax.rem(chip + d1 * core + d2 * (1 - core), ring_x) * CORES + core}

    def block(d1, d2, r, part=None):
        rows = pl.ds(r * rr, rr) if part is None else pl.ds(r * rr + part * half, half)
        at = lax.rem(chip + d1 * core + d2 * (1 - core), ring_x)
        return nbuf.at[lax.rem(ch + d1 * (1 - core) + d2 * core, ring_y), rows, pl.ds(pl.multiple_of(at * width, width), width)]

    firsts = (0, 3, 1, 2)

    def route(k, r):
        if k < 4:
            src, to, dst = (((0, 0, r), (1, 0), (3, 0, r)), ((0, 0, r), (3, 0), (1, 0, r)),
                            ((3, 0, r, 0), (1, 0), (2, 0, r, 0)), ((1, 0, r, 1), (3, 0), (2, 0, r, 1)))[k]
        else:
            d1 = firsts[(k - 4) // 4]
            src, to, dst = (((d1, 0, r), (0, 1), (d1, 3, r)), ((d1, 0, r), (0, 3), (d1, 1, r)),
                            ((d1, 3, r, 0), (0, 1), (d1, 2, r, 0)), ((d1, 1, r, 1), (0, 3), (d1, 2, r, 1)))[k % 4]
        return block(*src), to, block(*dst)

    def start(r, *ks):
        for k in ks:
            src, to, _ = route(k, r)
            pltpu.make_async_remote_copy(src_ref=src, dst_ref=src, send_sem=ns.at[r, k], recv_sem=nr.at[r, k], device_id=device(*to), device_id_type=MESH).start()

    def wait(r, *ks):
        for k in ks:
            ref = route(k, r)[2]
            pltpu.make_async_remote_copy(src_ref=ref, dst_ref=ref, send_sem=ns.at[r, k], recv_sem=nr.at[r, k], device_id=device(1, 0), device_id_type=MESH).wait_recv()

    def own(r):
        if r < ROUNDS:
            start(r, 0, 1, 4, 5)

    def stage1(r):
        if r < ROUNDS:
            wait(r, 0, 1)
            start(r, 2, 3, 8, 9, 12, 13)
            wait(r, 4, 5)
            start(r, 6, 7)

    def stage2(r):
        if r < ROUNDS:
            wait(r, 2, 3)
            start(r, 16, 17)
            wait(r, 8, 9)
            start(r, 10, 11)
            wait(r, 12, 13)
            start(r, 14, 15)

    def stage3(r):
        if r < ROUNDS:
            wait(r, 16, 17)
            start(r, 18, 19)

    def halves(r):
        return pltpu.make_async_remote_copy(src_ref=send.at[r], dst_ref=got.at[r], send_sem=ns.at[r, 20], recv_sem=nr.at[r, 20], device_id={'wd': partner}, device_id_type=MESH)

    def dots(r, mine):
        def one(q, carry):
            block_in = nbuf[q, pl.ds(r * rr, rr), :]
            if mine:
                keep[q] = jnp.dot(block_in, w_ref[core], preferred_element_type=jnp.float32)
            else:
                send[r, q] = jnp.dot(block_in, w_ref[1 - core], preferred_element_type=jnp.float32).astype(jnp.bfloat16)
            return carry
        lax.fori_loop(0, ring_y, one, 0)

    def finish(r):
        halves(r).wait_recv()
        mid = out_ref.shape[2]

        def one(q, carry):
            total = keep[q] + got[r, q].astype(jnp.float32) + bias_ref[...].astype(jnp.float32)
            out_ref[q, pl.ds(r * rr, rr), :] = (jax.nn.gelu(total[:, :mid], approximate=True) * total[:, mid:]).astype(jnp.bfloat16)
            return carry
        lax.fori_loop(0, ring_y, one, 0)

    barrier = pltpu.get_barrier_semaphore()
    for step in range(1, wd_count):
        pl.semaphore_signal(barrier, inc=1, device_id={'wd': lax.rem(wd + step, wd_count)}, device_id_type=MESH)
    for step in (1, 3):
        pl.semaphore_signal(barrier, inc=1, device_id={'ch': lax.rem(ch + step, ring_y)}, device_id_type=MESH)

    tiles = share // lanes
    for i in range(tiles):
        sq = jnp.zeros((lanes, lanes), jnp.float32)
        for j in range(width // lanes):
            val = resid_ref[i * lanes:(i + 1) * lanes, j * lanes:(j + 1) * lanes]
            sq = sq + val * val
        sums[i:i + 1, :] = jnp.sum(sq.T, axis=0, keepdims=True)
    all_sums[wd] = sums[...]
    pl.semaphore_wait(barrier, wd_count + 1)
    for step in range(1, wd_count):
        pltpu.make_async_remote_copy(src_ref=sums, dst_ref=all_sums.at[wd], send_sem=ss.at[step], recv_sem=sr.at[step], device_id={'wd': lax.rem(wd + step, wd_count)}, device_id_type=MESH).start()
    for step in range(1, wd_count):
        ref = all_sums.at[lax.rem(wd + wd_count - step, wd_count)]
        pltpu.make_async_remote_copy(src_ref=ref, dst_ref=ref, send_sem=ss.at[step], recv_sem=sr.at[step], device_id={'wd': partner}, device_id_type=MESH).wait_recv()
    scale = lax.rsqrt(jnp.sum(all_sums[...], axis=0) / (width * wd_count) + EPS)
    at = pl.ds(pl.multiple_of(chip * width, width), width)
    gain = 1.0 + gain_ref[...].astype(jnp.float32)
    for i in range(tiles):
        factor = jnp.broadcast_to(scale[i:i + 1, :], (lanes, lanes)).T[:, 0:1]
        rows = slice(i * lanes, (i + 1) * lanes)
        nbuf[ch, rows, at] = (resid_ref[rows, :] * factor * gain).astype(jnp.bfloat16)
    own(0)
    own(1)
    stage1(0)
    own(2)
    stage2(0)
    stage1(1)
    stage3(0)
    stage2(1)
    for r in range(ROUNDS):
        wait(r, 6, 7, 10, 11, 14, 15, 18, 19)
        dots(r, False)
        halves(r).start()
        own(r + 3)
        stage1(r + 2)
        stage3(r + 1)
        dots(r, True)
        stage2(r + 2)
        finish(r)
    for step in range(1, wd_count):
        pltpu.make_async_remote_copy(src_ref=sums, dst_ref=all_sums.at[wd], send_sem=ss.at[step], recv_sem=sr.at[step], device_id={'wd': partner}, device_id_type=MESH).wait_send()
    for r in range(ROUNDS):
        halves(r).wait_send()
        for k in range(20):
            src, to, _ = route(k, r)
            pltpu.make_async_remote_copy(src_ref=src, dst_ref=src, send_sem=ns.at[r, k], recv_sem=nr.at[r, k], device_id=device(*to), device_id_type=MESH).wait_send()


def mlp_in(resid, gain, weight, bias, ring_x, ring_y, cid):
    share, width = resid.shape
    _, depth, cols = weight.shape
    lanes = 128
    rr = share // ROUNDS
    vmem = pl.BlockSpec(memory_space=pltpu.VMEM)
    out = pl.pallas_call(
        mlp_in_kernel,
        out_shape=jax.ShapeDtypeStruct((ring_y, share, cols // 2), jnp.bfloat16),
        in_specs=[vmem] * 4,
        out_specs=vmem,
        scratch_shapes=[
            pltpu.VMEM((ring_y, share, depth), jnp.bfloat16),
            pltpu.VMEM((ring_y, rr, cols), jnp.float32),
            pltpu.VMEM((ROUNDS, ring_y, rr, cols), jnp.bfloat16),
            pltpu.VMEM((ROUNDS, ring_y, rr, cols), jnp.bfloat16),
            pltpu.VMEM((share // lanes, lanes), jnp.float32),
            pltpu.VMEM((ring_x * CORES, share // lanes, lanes), jnp.float32),
            pltpu.SemaphoreType.DMA((ROUNDS, 21)), pltpu.SemaphoreType.DMA((ROUNDS, 21)),
            pltpu.SemaphoreType.DMA((ring_x * CORES,)), pltpu.SemaphoreType.DMA((ring_x * CORES,)),
        ],
        compiler_params=pltpu.CompilerParams(collective_id=cid, has_side_effects=True, vmem_limit_bytes=60 << 20),
        name='mlp_in',
    )(resid, gain, weight, bias)
    return out.reshape(ring_y * share, cols // 2)


def front_kernel(x_ref, gain_ref, w_x_ref, w_y_ref, bias_ref, u_ref, y_ref, nbuf, wbuf, pbuf, opp_buf, side, sums, all_sums, local_sem, ps, pr, xs, xr, ss, sr):
    tokens, width = x_ref.shape
    ring_x, _, _, wd, core, chip = ring_refs()
    wd_count = ring_x * CORES
    rr = tokens // ROUNDS
    half = rr // 2
    mine = y_ref.shape[1]
    piece = CORES * mine
    lanes = sums.shape[1]
    partner = wd + 1 - 2 * core
    right, opp, left = (lax.rem(chip + step, ring_x) for step in (1, 2, 3))

    def span(r, part=None):
        return pl.ds(r * rr, rr) if part is None else pl.ds(r * rr + part * half, half)

    def weight(k, of):
        j, m = k // 2, k % 2
        src = (w_x_ref, w_y_ref)[m].at[:, pl.ds(pl.multiple_of((j * CORES + of) * mine, mine), mine)]
        return src, wbuf.at[pl.ds(pl.multiple_of(core * width, width), width), pl.ds(j * piece + m * mine, mine)]

    def weight_out(k):
        src, dst = weight(k, 1 - core)
        return pltpu.make_async_remote_copy(src_ref=src, dst_ref=dst, send_sem=ps.at[ROUNDS, k], recv_sem=pr.at[ROUNDS, k], device_id={'wd': partner}, device_id_type=MESH)

    def weight_own(k):
        src, dst = weight(k, core)
        return pltpu.make_async_copy(src, dst, local_sem.at[k])

    def weight_in(k):
        ref = wbuf.at[pl.ds(pl.multiple_of((1 - core) * width, width), width), pl.ds((k // 2) * piece + (k % 2) * mine, mine)]
        pltpu.make_async_remote_copy(src_ref=ref, dst_ref=ref, send_sem=ps.at[ROUNDS, k], recv_sem=pr.at[ROUNDS, k], device_id={'wd': partner}, device_id_type=MESH).wait_recv()

    def normed(r, of):
        ref = nbuf.at[span(r), pl.ds(pl.multiple_of(of * width, width), width)]
        return pltpu.make_async_remote_copy(src_ref=ref, dst_ref=ref, send_sem=ps.at[r, 0], recv_sem=pr.at[r, 0], device_id={'wd': partner}, device_id_type=MESH)

    def u_copy(r):
        return pltpu.make_async_remote_copy(src_ref=u_ref.at[span(r), pl.ds(0, mine)], dst_ref=u_ref.at[span(r), pl.ds(mine, mine)],
                                            send_sem=ps.at[r, 1], recv_sem=pr.at[r, 1], device_id={'wd': partner}, device_id_type=MESH)

    def part_of(dest, r, part):
        return pbuf.at[span(r, part), pl.ds(pl.multiple_of(dest * piece, piece), piece)]

    def x_send(k, r):
        rows = pl.ds(r * half, half)
        src, dst, to = {
            0: (part_of(opp, r, 0), opp_buf.at[0, rows], right),
            1: (part_of(opp, r, 1), opp_buf.at[1, rows], left),
            2: (part_of(right, r, 1), side.at[0, span(r, 1)], right),
            3: (part_of(left, r, 0), side.at[1, span(r, 0)], left),
            4: (part_of(right, r, 0), side.at[0, span(r, 0)], right),
            5: (part_of(left, r, 1), side.at[1, span(r, 1)], left),
        }[k]
        return pltpu.make_async_remote_copy(src_ref=src, dst_ref=dst, send_sem=xs.at[r, k], recv_sem=xr.at[r, k], device_id={'wd': to * CORES + core}, device_id_type=MESH)

    def norm(r):
        for i in range(rr // lanes):
            tile = r * (rr // lanes) + i
            factor = jnp.broadcast_to(scale[tile:tile + 1, :], (lanes, lanes)).T[:, 0:1]
            rows = slice(tile * lanes, (tile + 1) * lanes)
            nbuf[rows, pl.ds(pl.multiple_of(core * width, width), width)] = (x_ref[rows, :].astype(jnp.float32) * factor * gain).astype(jnp.bfloat16)
        normed(r, core).start()

    def dots(r):
        normed(r, 1 - core).wait_recv()
        step_rows = rr // 4

        def one(i, carry):
            rows = pl.ds(pl.multiple_of(r * rr + i * step_rows, step_rows), step_rows)
            pbuf[rows, :] = jnp.dot(nbuf[rows, :], wbuf[...], preferred_element_type=jnp.float32).astype(jnp.bfloat16)
            return carry
        lax.fori_loop(0, 4, one, 0)
        for k in range(4):
            x_send(k, r).start()

    def combine(r):
        rows = pl.ds(r * half, half)
        for k, dest, part, back in ((0, right, 0, 4), (1, left, 1, 5)):
            x_send(k, r).wait_recv()
            at = (span(r, part), pl.ds(pl.multiple_of(dest * piece, piece), piece))
            pbuf[at] = (pbuf[at].astype(jnp.float32) + opp_buf[k, rows, :].astype(jnp.float32)).astype(jnp.bfloat16)
            x_send(back, r).start()

    def final(r):
        for k in range(2, 6):
            x_send(k, r).wait_recv()
        rows = span(r)
        total = pbuf[rows, pl.ds(pl.multiple_of(chip * piece, piece), piece)].astype(jnp.float32) + side[0, rows, :].astype(jnp.float32) + side[1, rows, :].astype(jnp.float32)
        total = total + bias_ref[...].astype(jnp.float32)
        u_ref[rows, 0:mine] = total[:, :mine].astype(jnp.bfloat16)
        u_copy(r).start()
        y_ref[rows, :] = jax.nn.gelu(total[:, mine:], approximate=True).astype(jnp.bfloat16)

    barrier = pltpu.get_barrier_semaphore()
    for step in range(1, wd_count):
        pl.semaphore_signal(barrier, inc=1, device_id={'wd': lax.rem(wd + step, wd_count)}, device_id_type=MESH)
    for k in range(2 * ring_x):
        weight_own(k).start()
    for i in range(tokens // lanes):
        sq = jnp.zeros((lanes, lanes), jnp.float32)
        for j in range(width // lanes):
            val = x_ref[i * lanes:(i + 1) * lanes, j * lanes:(j + 1) * lanes].astype(jnp.float32)
            sq = sq + val * val
        sums[i:i + 1, :] = jnp.sum(sq.T, axis=0, keepdims=True)
    all_sums[wd] = sums[...]
    pl.semaphore_wait(barrier, wd_count - 1)
    for step in range(1, wd_count):
        pltpu.make_async_remote_copy(src_ref=sums, dst_ref=all_sums.at[wd], send_sem=ss.at[step], recv_sem=sr.at[step], device_id={'wd': lax.rem(wd + step, wd_count)}, device_id_type=MESH).start()
    for k in range(2 * ring_x):
        weight_out(k).start()
    for step in range(1, wd_count):
        ref = all_sums.at[lax.rem(wd + wd_count - step, wd_count)]
        pltpu.make_async_remote_copy(src_ref=ref, dst_ref=ref, send_sem=ss.at[step], recv_sem=sr.at[step], device_id={'wd': partner}, device_id_type=MESH).wait_recv()
    scale = lax.rsqrt(jnp.sum(all_sums[...], axis=0) / (width * wd_count) + EPS)
    gain = 1.0 + gain_ref[...].astype(jnp.float32)
    norm(0)
    for k in range(2 * ring_x):
        weight_own(k).wait()
        weight_in(k)
    for r in range(ROUNDS):
        if r + 1 < ROUNDS:
            norm(r + 1)
        dots(r)
        if r >= 1:
            combine(r - 1)
        if r >= 2:
            final(r - 2)
    combine(ROUNDS - 1)
    final(ROUNDS - 2)
    final(ROUNDS - 1)
    for step in range(1, wd_count):
        pltpu.make_async_remote_copy(src_ref=sums, dst_ref=all_sums.at[wd], send_sem=ss.at[step], recv_sem=sr.at[step], device_id={'wd': partner}, device_id_type=MESH).wait_send()
    for k in range(2 * ring_x):
        weight_out(k).wait_send()
    for r in range(ROUNDS):
        normed(r, core).wait_send()
        u_copy(r).wait()
        for k in range(6):
            x_send(k, r).wait_send()


def front(x, gain, w_x, w_y, bias, ring_x, cid):
    tokens, width = x.shape
    rnn = w_x.shape[1]
    mine = rnn // (ring_x * CORES)
    lanes = 128
    vmem, anywhere = pl.BlockSpec(memory_space=pltpu.VMEM), pl.BlockSpec(memory_space=pl.ANY)
    return pl.pallas_call(
        front_kernel,
        out_shape=(jax.ShapeDtypeStruct((tokens, CORES * mine), jnp.bfloat16), jax.ShapeDtypeStruct((tokens, mine), jnp.bfloat16)),
        in_specs=[vmem, vmem, anywhere, anywhere, vmem],
        out_specs=(vmem, vmem),
        scratch_shapes=[
            pltpu.VMEM((tokens, CORES * width), jnp.bfloat16),
            pltpu.VMEM((CORES * width, rnn), jnp.bfloat16),
            pltpu.VMEM((tokens, rnn), jnp.bfloat16),
            pltpu.VMEM((2, tokens // 2, CORES * mine), jnp.bfloat16),
            pltpu.VMEM((2, tokens, CORES * mine), jnp.bfloat16),
            pltpu.VMEM((tokens // lanes, lanes), jnp.float32),
            pltpu.VMEM((ring_x * CORES, tokens // lanes, lanes), jnp.float32),
            pltpu.SemaphoreType.DMA((2 * ring_x,)),
            pltpu.SemaphoreType.DMA((ROUNDS + 1, 2 * ring_x)), pltpu.SemaphoreType.DMA((ROUNDS + 1, 2 * ring_x)),
            pltpu.SemaphoreType.DMA((ROUNDS, 6)), pltpu.SemaphoreType.DMA((ROUNDS, 6)),
            pltpu.SemaphoreType.DMA((ring_x * CORES,)), pltpu.SemaphoreType.DMA((ring_x * CORES,)),
        ],
        compiler_params=pltpu.CompilerParams(collective_id=cid, has_side_effects=True, vmem_limit_bytes=56 << 20),
        name='front',
    )(x, gain, w_x, w_y, bias)


def solution(mesh):
    wd_count = mesh.shape['wd']
    ch_count = mesh.shape['ch']
    chips = wd_count // CORES
    row_spec = P('dp', 'wd')
    specs = (row_spec, P('dp', None), P('wd'), P('wd', 'ch'), P('ch'), P('wd', 'ch'), P('ch'), P(None, 'ch'), P('ch'), P('ch'), P('ch', None, None), P('ch'), P('ch', None, None), P('ch'), P('ch', 'wd'), P('wd'), P('wd'), P('wd', 'ch'), P('ch'), P('wd', 'ch'), P('ch'), P('ch', 'wd'), P('wd'))
    swap = [(i, i + 1 - 2 * (i % CORES)) for i in range(wd_count)]
    same_core = [[x * CORES + c for x in range(chips)] for c in range(CORES)]

    def local_layer(resid_in, seg_pos, gain_temporal, w_x, bias_x, w_y, bias_y, conv_w, conv_bias, lam_param, rgate_w, rgate_b, igate_w, igate_b, w_o, bias_o, gain_mlp, w_g, bias_g, w_u, bias_u, w_d, bias_d):
        tokens, local_width = resid_in.shape
        model_width = local_width * wd_count
        share = tokens // ch_count
        rnn = w_x.shape[1]
        mine = rnn // wd_count
        wd_i = lax.axis_index('wd')
        core = wd_i % CORES
        block = wd_i // CORES
        positions = seg_pos.reshape(tokens)

        def own(vec):
            return lax.dynamic_slice_in_dim(vec, wd_i * mine, mine, axis=vec.ndim - 1)

        def both(vec):
            pair = lax.dynamic_slice_in_dim(vec, block * CORES * mine, CORES * mine, axis=vec.ndim - 1)
            return jnp.where(core == 0, pair, jnp.concatenate([pair[..., mine:], pair[..., :mine]], axis=-1))

        ff = w_g.shape[1] // wd_count
        u_pair, y_own = front(resid_in, gain_temporal[None], w_x, w_y, jnp.concatenate([own(bias_x), own(bias_y)])[None], chips, 5)
        gate_w = jnp.concatenate([lax.dynamic_index_in_dim(w, block, 0, keepdims=False) for w in (rgate_w, igate_w)], axis=1)
        gate_w = gate_w.reshape(CORES, mine, 2, CORES, mine)
        gate_w = lax.dynamic_index_in_dim(gate_w, core, 3, keepdims=False).reshape(CORES, mine, 2 * mine)
        gate_w = jnp.where(core == 0, gate_w, gate_w[::-1]).reshape(CORES * mine, 2 * mine)
        gate_b = jnp.concatenate([own(rgate_b), own(igate_b)])[None]
        mixed, mlp_w = lru(u_pair, y_own, positions[:, None], both(conv_w), both(conv_bias)[None], gate_w, gate_b, own(lam_param)[None], w_g, w_u, chips, 3)
        resid_rows = lax.dynamic_slice_in_dim(resid_in, lax.axis_index('ch') * share, share, axis=0)
        resid = ring_layer(mixed, w_o, resid_rows, bias_o[None], ch_count, False, 1)
        mlp_b = jnp.concatenate([lax.dynamic_slice_in_dim(b, wd_i * ff, ff) for b in (bias_g, bias_u)])[None]
        inner = mlp_in(resid, gain_mlp[None], mlp_w, mlp_b, chips, ch_count, 4)
        return ring_layer(inner, w_d, resid, bias_d[None], ch_count, True, 2)

    return jax.shard_map(local_layer, mesh=mesh, in_specs=specs, out_specs=row_spec, check_vma=False)
```

```python
import functools

import jax
import jax.numpy as jnp
from jax import lax
from jax.experimental import pallas as pl
from jax.experimental.pallas import tpu as pltpu
from jax.sharding import PartitionSpec as P

EPS = 1e-6
CORES = 2
SEGS = 8
PAD = 8
LANES = 128
RIGHT, OPP, LEFT = 1, 2, 3
MESH = pl.DeviceIdType.MESH
F32 = jnp.float32
BF16 = jnp.bfloat16
VMEM = pl.BlockSpec(memory_space=pltpu.VMEM)
ANY = pl.BlockSpec(memory_space=pl.ANY)
DMA = pltpu.SemaphoreType.DMA


def neg_expm1(z):
    series = -z * (1.0 + z * (0.5 + z * (1.0 / 6.0 + z * (1.0 / 24.0))))
    return jnp.where(z > -0.03, series, 1.0 - jnp.exp(z))


def where_am_i():
    ring_x = lax.axis_size('wd') // CORES
    wd = lax.axis_index('wd')
    return ring_x, lax.axis_size('ch'), lax.axis_index('ch'), wd, lax.rem(wd, CORES), wd // CORES


def aligned(index, size):
    return pl.ds(pl.multiple_of(index * size, size), size)


def remote(src, dst, send, recv, device):
    return pltpu.make_async_remote_copy(src_ref=src, dst_ref=dst, send_sem=send, recv_sem=recv, device_id=device, device_id_type=MESH)


def greet(devices):
    barrier = pltpu.get_barrier_semaphore()
    for device in devices:
        pl.semaphore_signal(barrier, inc=1, device_id=device, device_id_type=MESH)
    return functools.partial(pl.semaphore_wait, barrier, len(devices))


def chip_peers():
    ring_x, _, _, _, core, chip = where_am_i()
    return [{'wd': lax.rem(chip + step, ring_x) * CORES + core} for step in range(1, ring_x)]


def swaps(src, dst, k, sends, recvs):
    ring_x, _, _, _, core, chip = where_am_i()
    depth, ff = src.shape[0], dst.shape[1]
    return [remote(src.at[:, aligned(lax.rem(chip + step, ring_x) * CORES + k, ff)], dst.at[aligned(chip, depth), :],
                   sends.at[step], recvs.at[step], {'wd': lax.rem(chip + step, ring_x) * CORES + core}) for step in range(1, ring_x)]


def row_sums(x_ref, sums):
    for i in range(x_ref.shape[0] // LANES):
        sq = jnp.zeros((LANES, LANES), F32)
        for j in range(x_ref.shape[1] // LANES):
            val = x_ref[i * LANES:(i + 1) * LANES, j * LANES:(j + 1) * LANES].astype(F32)
            sq = sq + val * val
        sums[i:i + 1, :] = jnp.sum(sq.T, axis=0, keepdims=True)


def sum_copies(sums, all_sums, ss, sr):
    ring_x, _, _, wd, _, _ = where_am_i()
    count = ring_x * CORES
    return [remote(sums, all_sums.at[wd], ss.at[step], sr.at[step], {'wd': lax.rem(wd + step, count)}) for step in range(1, count)]


def as_column(row):
    return jnp.broadcast_to(row, (LANES, LANES)).T


def lru_kernel(offs, u_ref, y_ref, pos_ref, vec_ref, rg_ref, ig_ref, w_ref, out_ref, part_ref, u32, a_s, b_s, gate_w, ws, wr):
    ring_x, _, _, wd, core, chip = where_am_i()
    tokens, wide = u_ref.shape
    width = y_ref.shape[1]
    tile = tokens // SEGS
    pitch = tile + PAD
    per_seg = tile // LANES
    rnn = offs['rnn']
    n_taps = offs['taps']

    def vec(name, index, size):
        return vec_ref[:, pl.ds(pl.multiple_of(offs[name] + index * size, size), size)]

    ready = greet(chip_peers())
    taps = [vec_ref[:, pl.ds(pl.multiple_of(offs['conv_w'] + k * rnn + chip * wide, wide), wide)] for k in range(n_taps)]
    cbias = vec('conv_bias', chip, wide)
    gate_b = jnp.concatenate([vec('rgate_b', wd, width), vec('igate_b', wd, width)], axis=1)
    lam = -vec('lam_param', wd, width)
    soft = -8.0 * (jnp.maximum(lam, 0.0) + jnp.log(1.0 + jnp.exp(-jnp.abs(lam))))
    gate_w[:, :width] = rg_ref[chip, :, aligned(core, width)]
    gate_w[:, width:] = ig_ref[chip, :, aligned(core, width)]
    u32[0:PAD, :] = jnp.zeros((PAD, wide), F32)
    ready()
    moves = swaps(w_ref, part_ref, 0, ws, wr)
    for one in moves:
        one.start()

    def widen(i, carry):
        rows = pl.multiple_of(i * tile, tile)
        u32[pl.ds(rows + PAD, tile), :] = u_ref[pl.ds(rows, tile), :].astype(F32)
        return carry
    lax.fori_loop(0, SEGS, widen, 0)

    def gates(i, carry):
        rows = pl.multiple_of(i * LANES, LANES)
        window = u32[pl.ds(rows, LANES + PAD), :]
        pos = as_column(pos_ref[:, pl.ds(rows, LANES)].astype(F32))
        pair = jnp.concatenate([pos, pos], axis=1)
        total = cbias + window[PAD:] * taps[0]
        for k in range(1, n_taps):
            total = total + jnp.where(pair >= k, window[PAD - k:PAD - k + LANES], 0.0) * taps[k]
        conv = total.astype(BF16)
        both = jax.nn.sigmoid(jnp.dot(conv, gate_w[...], preferred_element_type=F32) + gate_b)
        log_a = both[:, :width] * soft
        reset = pos == 0
        decay = jnp.where(reset, 0.0, jnp.exp(log_a))
        scale = jnp.where(reset, 1.0, jnp.sqrt(neg_expm1(2.0 * log_a)))
        mine = conv.astype(F32)
        drive = scale * both[:, width:] * jnp.where(core == 0, mine[:, :width], mine[:, width:])
        seg = i // per_seg
        at = pl.multiple_of(seg * pitch + (i - seg * per_seg) * LANES, PAD)
        a_s[pl.ds(at, LANES), :] = decay
        b_s[pl.ds(at, LANES), :] = drive
        return carry
    lax.fori_loop(0, tokens // LANES, gates, 0)

    def steps(i, carry):
        hid, acc = carry
        for j in range(8):
            at = pl.ds(i * 8 + j, SEGS, stride=pitch)
            a = a_s[at, :]
            hid = a * hid + b_s[at, :]
            acc = a * acc
            b_s[at, :] = hid
            a_s[at, :] = acc
        return hid, acc
    hid, acc = lax.fori_loop(0, tile // 8, steps, (jnp.zeros((SEGS, width), F32), jnp.ones((SEGS, width), F32)))

    entry = jnp.zeros((1, width), F32)
    for seg in range(SEGS):
        for q in range(per_seg):
            at = seg * pitch + q * LANES
            hidden = b_s[at:at + LANES, :] + a_s[at:at + LANES, :] * entry
            rows = slice(seg * tile + q * LANES, seg * tile + (q + 1) * LANES)
            out_ref[rows, :] = (hidden * y_ref[rows, :].astype(F32)).astype(BF16)
        entry = hid[seg:seg + 1] + acc[seg:seg + 1] * entry
    for one in moves:
        one.wait()


def lru(offs, u_pair, y_rows, pos, vec, rgate_w, igate_w, weight, part, ring_x, cid):
    tokens, wide = u_pair.shape
    width = y_rows.shape[1]
    rows = SEGS * (tokens // SEGS + PAD)
    return pl.pallas_call(
        functools.partial(lru_kernel, offs),
        out_shape=(jax.ShapeDtypeStruct((tokens, width), BF16), part),
        in_specs=[VMEM] * 6 + [ANY],
        out_specs=(VMEM, ANY),
        scratch_shapes=[pltpu.VMEM((tokens + PAD, wide), F32), pltpu.VMEM((rows, width), F32), pltpu.VMEM((rows, width), F32),
                        pltpu.VMEM((wide, 2 * width), BF16), DMA((ring_x,)), DMA((ring_x,))],
        compiler_params=pltpu.CompilerParams(collective_id=cid, has_side_effects=True, vmem_limit_bytes=48 << 20),
        name='lru',
    )(u_pair, y_rows, pos, vec, rgate_w, igate_w, weight)


def ring_kernel(rounds, regather, bias_at, h_ref, w_ref, resid_ref, vec_ref, *refs):
    if regather:
        out_ref, hbuf, pbuf, opp_buf, side, resid, xs, xr, ys, yr, local_sem = refs
    else:
        wg_ref, wu_ref, out_ref, part_g, part_u, hbuf, pbuf, opp_buf, side, resid, xs, xr, ys, yr, local_sem, ws, wr = refs
    share, depth = h_ref.shape[1:]
    cols_out = w_ref.shape[1]
    rr = share // rounds
    half = rr // 2
    ring_x, ring_y, ch, wd, core, chip = where_am_i()
    other = 1 - 2 * core
    partner = wd + other
    x_at = [lax.rem(chip + step, ring_x) * CORES + core for step in range(ring_x)]
    y_at = [lax.rem(ch + step, ring_y) for step in range(ring_y)]
    first, second, whole = 0, 1, None

    def span(r, part=None):
        return pl.ds(r * rr, rr) if part is None else pl.ds(r * rr + part * half, half)

    def cols(owner, r, part=None):
        return hbuf.at[:, span(r, part), aligned(owner, depth)]

    x_plan = [(wd, whole, x_at[RIGHT], x_at[LEFT]), (wd, whole, x_at[LEFT], x_at[RIGHT]),
              (x_at[LEFT], first, x_at[RIGHT], x_at[OPP]), (x_at[RIGHT], second, x_at[LEFT], x_at[OPP]),
              (wd, whole, partner, partner), (x_at[LEFT], whole, partner, x_at[LEFT] + other), (x_at[RIGHT], whole, partner, x_at[RIGHT] + other),
              (x_at[OPP], first, partner, x_at[OPP] + other), (x_at[OPP], second, partner, x_at[OPP] + other)]
    own_both, own_side, relay_both, side_both, opp_both, core_in = (0, 1), (4,), (2, 3), (5, 6), (7, 8), (4, 5, 6, 7, 8)

    def x_copy(k, r):
        owner, part, to, _ = x_plan[k]
        dst = cols(owner, r, part)
        src = h_ref.at[:, span(r), :] if k in own_both + own_side else dst
        return remote(src, dst, xs.at[r, k], xr.at[r, k], {'wd': to})

    def x_start(r, *ks):
        for k in ks:
            x_copy(k, r).start()

    def x_wait(r, *ks):
        for k in ks:
            ref = cols(x_plan[k][-1], r, x_plan[k][1])
            remote(ref, ref, xs.at[r, k], xr.at[r, k], {'wd': partner}).wait_recv()

    def y_refs(k, r):
        rows = pl.ds(r * half, half)
        sums = [(OPP, first, opp_buf.at[0, rows], RIGHT), (OPP, second, opp_buf.at[1, rows], LEFT),
                (RIGHT, second, side.at[0, span(r, second)], RIGHT), (LEFT, first, side.at[1, span(r, first)], LEFT),
                (RIGHT, first, side.at[0, span(r, first)], RIGHT), (LEFT, second, side.at[1, span(r, second)], LEFT)]
        if k < len(sums):
            piece, part, dst, to = sums[k]
            return pbuf.at[y_at[piece], span(r, part)], dst, to, dst
        owner, part, to, got = [(0, whole, RIGHT, LEFT), (0, whole, LEFT, RIGHT), (LEFT, first, RIGHT, OPP), (RIGHT, second, LEFT, OPP)][k - len(sums)]
        src = out_ref.at[y_at[owner], span(r, part)]
        return src, src, to, out_ref.at[y_at[got], span(r, part)]

    to_opp, to_side, relayed, out_own, out_relay = (0, 1), (2, 3), (4, 5), (6, 7), (8, 9)

    def y_start(r, *ks):
        for k in ks:
            src, dst, to, _ = y_refs(k, r)
            remote(src, dst, ys.at[r, k], yr.at[r, k], {'ch': y_at[to]}).start()

    def y_wait(r, *ks):
        for k in ks:
            ref = y_refs(k, r)[-1]
            remote(ref, ref, ys.at[r, k], yr.at[r, k], {'ch': y_at[RIGHT]}).wait_recv()

    def own(r):
        if r < rounds:
            x_start(r, *own_both, *own_side)

    def stage1(r):
        if r < rounds:
            for side_in, on in zip(own_both, relay_both):
                x_wait(r, side_in)
                x_start(r, on)
            x_start(r, *side_both)
            own(r + 2)
            if not regather and r == rounds - 1:
                for one in moves:
                    one.start()

    def stage2(r):
        for side_in, on in zip(relay_both, opp_both):
            x_wait(r, side_in)
            x_start(r, on)

    def dots(r):
        x_wait(r, *core_in)
        each = max(1, 256 // rr)

        def one(i, carry):
            at = pl.ds(i * each, each)
            block = hbuf[at, pl.ds(r * rr, rr), :].reshape(each * rr, hbuf.shape[2])
            part = jnp.dot(block, w_ref[...], preferred_element_type=F32)
            pbuf[at, pl.ds(r * rr, rr), :] = part.astype(BF16).reshape(each, rr, cols_out)
            return carry
        lax.fori_loop(0, ring_y // each, one, 0)
        y_start(r, *to_opp, *to_side)

    def combine(r):
        for k, piece, part in zip(to_opp, (RIGHT, LEFT), (first, second)):
            y_wait(r, k)
            at = y_at[piece], span(r, part)
            pbuf[at] = (pbuf[at].astype(F32) + opp_buf[k, pl.ds(r * half, half), :].astype(F32)).astype(BF16)
            y_start(r, relayed[k])

    def final(r):
        y_wait(r, *to_side, *relayed)
        rows = span(r)
        total = pbuf[ch, rows, :].astype(F32) + side[0, rows, :].astype(F32) + side[1, rows, :].astype(F32)
        total = resid[rows, :].astype(F32) + total + vec_ref[:, bias_at:bias_at + cols_out]
        if regather:
            out_ref[ch, rows, :] = total.astype(out_ref.dtype)
            y_start(r, *out_own)
        else:
            out_ref[rows, :] = total.astype(out_ref.dtype)

    def relay(r):
        if regather:
            y_wait(r, *out_own)
            y_start(r, *out_relay)

    peers = [{'wd': partner}, {'ch': y_at[LEFT]}, {'ch': y_at[RIGHT]}]
    if regather:
        ready = greet(peers + [{'wd': x_at[LEFT]}, {'wd': x_at[RIGHT]}])
        resid_rows = resid_ref
    else:
        ready = greet(peers + chip_peers())
        moves = swaps(wg_ref, part_g, 1, ws.at[0], wr.at[0]) + swaps(wu_ref, part_u, 1, ws.at[1], wr.at[1])
        resid_rows = resid_ref.at[aligned(ch, share), :]
    local = [pltpu.make_async_copy(h_ref, hbuf.at[:, :, aligned(wd, depth)], local_sem.at[0]), pltpu.make_async_copy(resid_rows, resid, local_sem.at[1])]
    for one in local:
        one.start()
    ready()
    own(0)
    own(1)
    for one in local:
        one.wait()
    stage1(0)
    for r in range(rounds):
        stage1(r + 1)
        stage2(r)
        if r >= 1:
            combine(r - 1)
        dots(r)
        if r >= 1:
            final(r - 1)
        if r >= 2:
            relay(r - 2)
    combine(rounds - 1)
    relay(rounds - 2)
    final(rounds - 1)
    relay(rounds - 1)
    for r in range(rounds):
        if regather:
            y_wait(r, *out_relay)
        for k in range(len(x_plan)):
            x_copy(k, r).wait_send()
        for k in range(10 if regather else 6):
            src, dst, to, _ = y_refs(k, r)
            remote(src, dst, ys.at[r, k], yr.at[r, k], {'ch': y_at[to]}).wait_send()
    if not regather:
        for one in moves:
            one.wait()


def ring_layer(h, w, resid, vec, bias_at, weights, part, ring_x, ring_y, rounds, cid):
    tokens, depth = h.shape
    share = tokens // ring_y
    wide, cols = w.shape
    regather = not weights
    out = jax.ShapeDtypeStruct((ring_y, share, cols), BF16) if regather else (jax.ShapeDtypeStruct((share, cols), F32), part, part)
    res = pl.pallas_call(
        functools.partial(ring_kernel, rounds, regather, bias_at),
        out_shape=out,
        in_specs=[ANY, VMEM, ANY, VMEM] + [ANY] * len(weights),
        out_specs=VMEM if regather else (VMEM, ANY, ANY),
        scratch_shapes=[
            pltpu.VMEM((ring_y, share, wide), BF16),
            pltpu.VMEM((ring_y, share, cols), BF16),
            pltpu.VMEM((2, share // 2, cols), BF16),
            pltpu.VMEM((2, share, cols), BF16),
            pltpu.VMEM((share, cols), resid.dtype),
            DMA((rounds, 9)), DMA((rounds, 9)), DMA((rounds, 10)), DMA((rounds, 10)), DMA((2,)),
        ] + ([] if regather else [DMA((2, ring_x)), DMA((2, ring_x))]),
        compiler_params=pltpu.CompilerParams(collective_id=cid, has_side_effects=True, vmem_limit_bytes=60 << 20),
        name='ring_layer',
    )(h.reshape(ring_y, share, depth), w, resid, vec, *weights)
    return res.reshape(tokens, cols) if regather else res


def mlp_in_kernel(rounds, offs, resid_ref, vec_ref, wg_ref, wu_ref, g0_ref, u0_ref, g1_ref, u1_ref, out_ref, nbuf, w_ref, keep, send, got, sums, all_sums, ns, nr, ss, sr, local_sem):
    share, width = resid_ref.shape
    ring_x, ring_y, ch, wd, core, chip = where_am_i()
    wd_count = ring_x * CORES
    rr = share // rounds
    half = rr // 2
    partner = wd + 1 - 2 * core
    ff = out_ref.shape[2]

    def device(d1, d2):
        return {'ch': lax.rem(ch + d1 * (1 - core) + d2 * core, ring_y), 'wd': lax.rem(chip + d1 * core + d2 * (1 - core), ring_x) * CORES + core}

    def block(d1, d2, r, part=None):
        rows = pl.ds(r * rr, rr) if part is None else pl.ds(r * rr + part * half, half)
        at = lax.rem(chip + d1 * core + d2 * (1 - core), ring_x)
        return nbuf.at[lax.rem(ch + d1 * (1 - core) + d2 * core, ring_y), rows, aligned(at, width)]

    whole = None
    plan = [((0, 0), (RIGHT, 0), (LEFT, 0), whole), ((0, 0), (LEFT, 0), (RIGHT, 0), whole),
            ((LEFT, 0), (RIGHT, 0), (OPP, 0), 0), ((RIGHT, 0), (LEFT, 0), (OPP, 0), 1)]
    for d1 in (0, LEFT, RIGHT, OPP):
        plan += [((d1, 0), (0, RIGHT), (d1, LEFT), whole), ((d1, 0), (0, LEFT), (d1, RIGHT), whole),
                 ((d1, LEFT), (0, RIGHT), (d1, OPP), 0), ((d1, RIGHT), (0, LEFT), (d1, OPP), 1)]
    core_step = len(plan)

    def copy(k, r):
        src, to, _, part = plan[k]
        ref = block(*src, r, part)
        return remote(ref, ref, ns.at[r, k], nr.at[r, k], device(*to))

    def start(r, *ks):
        for k in ks:
            copy(k, r).start()

    def wait(r, *ks):
        for k in ks:
            ref = block(*plan[k][2], r, plan[k][3])
            remote(ref, ref, ns.at[r, k], nr.at[r, k], device(RIGHT, 0)).wait_recv()

    def own(r):
        if r < rounds:
            start(r, 0, 1, 4, 5)

    def stage1(r):
        if r < rounds:
            wait(r, 0, 1)
            start(r, 2, 3, 8, 9, 12, 13)
            wait(r, 4, 5)
            start(r, 6, 7)

    def stage2(r):
        if r < rounds:
            wait(r, 2, 3)
            start(r, 16, 17)
            wait(r, 8, 9)
            start(r, 10, 11)
            wait(r, 12, 13)
            start(r, 14, 15)

    def stage3(r):
        if r < rounds:
            wait(r, 16, 17)
            start(r, 18, 19)

    def halves(r):
        return remote(send.at[r], got.at[r], ns.at[r, core_step], nr.at[r, core_step], {'wd': partner})

    each = max(1, 256 // rr)

    def dots(r, mine):
        def one(i, carry):
            at = pl.ds(i * each, each)
            rows = nbuf[at, pl.ds(r * rr, rr), :].reshape(each * rr, nbuf.shape[2])
            if mine:
                keep[at] = jnp.dot(rows, w_ref[core], preferred_element_type=F32).reshape(each, rr, 2 * ff)
            else:
                send[r, at] = jnp.dot(rows, w_ref[1 - core], preferred_element_type=F32).astype(BF16).reshape(each, rr, 2 * ff)
            return carry
        lax.fori_loop(0, ring_y // each, one, 0)

    def finish(r):
        halves(r).wait_recv()
        b_g, b_u = (vec_ref[:, pl.ds(pl.multiple_of(offs[name] + wd * ff, LANES), ff)] for name in ('bias_g', 'bias_u'))

        def one(q, carry):
            total = keep[q] + got[r, q].astype(F32)
            out_ref[q, pl.ds(r * rr, rr), :] = (jax.nn.gelu(total[:, :ff] + b_g, approximate=True) * (total[:, ff:] + b_u)).astype(BF16)
            return carry
        lax.fori_loop(0, ring_y, one, 0)

    ready = greet([{'wd': lax.rem(wd + step, wd_count)} for step in range(1, wd_count)] + [{'ch': lax.rem(ch + step, ring_y)} for step in (RIGHT, LEFT)])
    loads = []
    for k, (g_part, u_part) in enumerate(((g0_ref, u0_ref), (g1_ref, u1_ref))):
        for m, (full, part) in enumerate(((wg_ref, g_part), (wu_ref, u_part))):
            sems = local_sem.at[k, m]
            for step in range(ring_x):
                rows = aligned(lax.rem(chip + step, ring_x), width)
                src = part.at[rows, :] if step else full.at[:, aligned(chip * CORES + k, ff)]
                loads.append(pltpu.make_async_copy(src, w_ref.at[k, rows, pl.ds(m * ff, ff)], sems.at[step]))
    for one in loads:
        one.start()
    row_sums(resid_ref, sums)
    all_sums[wd] = sums[...]
    ready()
    for one in sum_copies(sums, all_sums, ss, sr):
        one.start()
    for one in sum_copies(sums, all_sums, ss, sr):
        one.wait()
    scale = lax.rsqrt(jnp.sum(all_sums[...], axis=0) / (width * wd_count) + EPS)
    gain = 1.0 + vec_ref[:, offs['gain_mlp']:offs['gain_mlp'] + width]

    def norm(r):
        for i in range(r * rr // LANES, (r + 1) * rr // LANES):
            factor = as_column(scale[i:i + 1, :])[:, 0:1]
            rows = slice(i * LANES, (i + 1) * LANES)
            nbuf[ch, rows, aligned(chip, width)] = (resid_ref[rows, :] * factor * gain).astype(BF16)

    for r in range(rounds):
        norm(r)
        if r < 3:
            own(r)
    stage1(0)
    stage2(0)
    stage1(1)
    stage3(0)
    stage2(1)
    for one in loads:
        one.wait()
    for r in range(rounds):
        wait(r, 6, 7, 10, 11, 14, 15, 18, 19)
        dots(r, False)
        halves(r).start()
        own(r + 3)
        stage1(r + 2)
        stage3(r + 1)
        dots(r, True)
        stage2(r + 2)
        finish(r)
    for r in range(rounds):
        halves(r).wait_send()
        for k in range(core_step):
            copy(k, r).wait_send()


def mlp_in(offs, resid, vec, w_g, w_u, parts, ring_x, ring_y, rounds, cid):
    share, width = resid.shape
    depth, ff = parts[0].shape
    cols = 2 * ff
    rr = share // rounds
    out = pl.pallas_call(
        functools.partial(mlp_in_kernel, rounds, offs),
        out_shape=jax.ShapeDtypeStruct((ring_y, share, ff), BF16),
        in_specs=[VMEM] * 2 + [ANY] * 6,
        out_specs=VMEM,
        scratch_shapes=[
            pltpu.VMEM((ring_y, share, depth), BF16),
            pltpu.VMEM((CORES, depth, cols), BF16),
            pltpu.VMEM((ring_y, rr, cols), F32),
            pltpu.VMEM((rounds, ring_y, rr, cols), BF16),
            pltpu.VMEM((rounds, ring_y, rr, cols), BF16),
            pltpu.VMEM((share // LANES, LANES), F32),
            pltpu.VMEM((ring_x * CORES, share // LANES, LANES), F32),
            DMA((rounds, 21)), DMA((rounds, 21)), DMA((ring_x * CORES,)), DMA((ring_x * CORES,)), DMA((CORES, 2, ring_x)),
        ],
        compiler_params=pltpu.CompilerParams(collective_id=cid, has_side_effects=True, vmem_limit_bytes=60 << 20),
        name='mlp_in',
    )(resid, vec, w_g, w_u, *parts)
    return out.reshape(ring_y * share, ff)


def front_kernel(rounds, offs, x_ref, vec_ref, w_x_ref, w_y_ref, w_ref, u_ref, y_ref, part_ref, nbuf, wbuf, pbuf, opp_buf, side, sums, all_sums, local_sem, ps, pr, xs, xr, ss, sr, ws, wr):
    tokens, width = x_ref.shape
    ring_x, _, _, wd, core, chip = where_am_i()
    wd_count = ring_x * CORES
    rr = tokens // rounds
    half = rr // 2
    mine = y_ref.shape[1]
    piece = CORES * mine
    partner = wd + 1 - 2 * core
    right, opp, left = (lax.rem(chip + step, ring_x) for step in (RIGHT, OPP, LEFT))
    first, second = 0, 1

    def span(r, part=None):
        return pl.ds(r * rr, rr) if part is None else pl.ds(r * rr + part * half, half)

    def weight(k, of):
        j, m = k // 2, k % 2
        src = (w_x_ref, w_y_ref)[m].at[:, pl.ds(pl.multiple_of((j * CORES + of) * mine, mine), mine)]
        return src, wbuf.at[aligned(core, width), pl.ds(j * piece + m * mine, mine)]

    def weight_out(k):
        src, dst = weight(k, 1 - core)
        return pltpu.make_async_remote_copy(src_ref=src, dst_ref=dst, send_sem=ps.at[rounds, k], recv_sem=pr.at[rounds, k], device_id={'wd': partner}, device_id_type=MESH)

    def weight_own(k):
        src, dst = weight(k, core)
        return pltpu.make_async_copy(src, dst, local_sem.at[k])

    def weight_in(k):
        ref = wbuf.at[aligned(1 - core, width), pl.ds((k // 2) * piece + (k % 2) * mine, mine)]
        pltpu.make_async_remote_copy(src_ref=ref, dst_ref=ref, send_sem=ps.at[rounds, k], recv_sem=pr.at[rounds, k], device_id={'wd': partner}, device_id_type=MESH).wait_recv()

    def normed(r, of):
        ref = nbuf.at[span(r), aligned(of, width)]
        return pltpu.make_async_remote_copy(src_ref=ref, dst_ref=ref, send_sem=ps.at[r, 0], recv_sem=pr.at[r, 0], device_id={'wd': partner}, device_id_type=MESH)

    def u_copy(r, of):
        ref = u_ref.at[span(r), aligned(of, mine)]
        return remote(ref, ref, ps.at[r, 1], pr.at[r, 1], {'wd': partner})

    def part_of(dest, r, part):
        return pbuf.at[span(r, part), aligned(dest, piece)]

    def x_send(k, r):
        rows = pl.ds(r * half, half)
        dest, part, dst, to = [
            (opp, first, opp_buf.at[0, rows], right), (opp, second, opp_buf.at[1, rows], left),
            (right, second, side.at[0, span(r, second)], right), (left, first, side.at[1, span(r, first)], left),
            (right, first, side.at[0, span(r, first)], right), (left, second, side.at[1, span(r, second)], left)][k]
        return remote(part_of(dest, r, part), dst, xs.at[r, k], xr.at[r, k], {'wd': to * CORES + core})

    def norm(r):
        for i in range(rr // LANES):
            tile = r * (rr // LANES) + i
            factor = as_column(scale[tile:tile + 1, :])[:, 0:1]
            rows = slice(tile * LANES, (tile + 1) * LANES)
            nbuf[rows, aligned(core, width)] = (x_ref[rows, :].astype(F32) * factor * gain).astype(BF16)
        normed(r, core).start()

    def dots(r):
        normed(r, 1 - core).wait_recv()
        step_rows = rr // 4

        def one(i, carry):
            rows = pl.ds(pl.multiple_of(r * rr + i * step_rows, step_rows), step_rows)
            pbuf[rows, :] = jnp.dot(nbuf[rows, :], wbuf[...], preferred_element_type=F32).astype(BF16)
            return carry
        lax.fori_loop(0, 4, one, 0)
        for k in range(4):
            x_send(k, r).start()

    def combine(r):
        rows = pl.ds(r * half, half)
        for k, dest, part, back in ((0, right, first, 4), (1, left, second, 5)):
            x_send(k, r).wait_recv()
            at = (span(r, part), aligned(dest, piece))
            pbuf[at] = (pbuf[at].astype(F32) + opp_buf[k, rows, :].astype(F32)).astype(BF16)
            x_send(back, r).start()

    def final(r):
        for k in range(2, 6):
            x_send(k, r).wait_recv()
        rows = span(r)
        total = pbuf[rows, aligned(chip, piece)].astype(F32) + side[0, rows, :].astype(F32) + side[1, rows, :].astype(F32)
        b_x, b_y = (vec_ref[:, pl.ds(pl.multiple_of(offs[name] + wd * mine, mine), mine)] for name in ('bias_x', 'bias_y'))
        u_ref[rows, aligned(core, mine)] = (total[:, :mine] + b_x).astype(BF16)
        u_copy(r, core).start()
        y_ref[rows, :] = jax.nn.gelu(total[:, mine:] + b_y, approximate=True).astype(BF16)

    ready = greet([{'wd': lax.rem(wd + step, wd_count)} for step in range(1, wd_count)])
    for k in range(2 * ring_x):
        weight_own(k).start()
    row_sums(x_ref, sums)
    all_sums[wd] = sums[...]
    ready()
    for one in sum_copies(sums, all_sums, ss, sr):
        one.start()
    for k in range(2 * ring_x):
        weight_out(k).start()
    moves = swaps(w_ref, part_ref, 0, ws, wr)
    for one in moves:
        one.start()
    for one in sum_copies(sums, all_sums, ss, sr):
        one.wait()
    scale = lax.rsqrt(jnp.sum(all_sums[...], axis=0) / (width * wd_count) + EPS)
    gain = 1.0 + vec_ref[:, offs['gain_temporal']:offs['gain_temporal'] + width]
    norm(0)
    for k in range(2 * ring_x):
        weight_own(k).wait()
        weight_in(k)
    for r in range(rounds):
        if r + 1 < rounds:
            norm(r + 1)
        dots(r)
        if r >= 1:
            combine(r - 1)
        if r >= 2:
            final(r - 2)
    combine(rounds - 1)
    final(rounds - 2)
    final(rounds - 1)
    for k in range(2 * ring_x):
        weight_out(k).wait_send()
    for r in range(rounds):
        normed(r, core).wait_send()
        u_copy(r, core).wait_send()
        u_copy(r, 1 - core).wait_recv()
        for k in range(6):
            x_send(k, r).wait_send()
    for one in moves:
        one.wait()


def front(offs, x, vec, w_x, w_y, weight, part, ring_x, rounds, cid):
    tokens, width = x.shape
    rnn = w_x.shape[1]
    mine = rnn // (ring_x * CORES)
    return pl.pallas_call(
        functools.partial(front_kernel, rounds, offs),
        out_shape=(jax.ShapeDtypeStruct((tokens, CORES * mine), BF16), jax.ShapeDtypeStruct((tokens, mine), BF16), part),
        in_specs=[VMEM, VMEM, ANY, ANY, ANY],
        out_specs=(VMEM, VMEM, ANY),
        scratch_shapes=[
            pltpu.VMEM((tokens, CORES * width), BF16),
            pltpu.VMEM((CORES * width, rnn), BF16),
            pltpu.VMEM((tokens, rnn), BF16),
            pltpu.VMEM((2, tokens // 2, CORES * mine), BF16),
            pltpu.VMEM((2, tokens, CORES * mine), BF16),
            pltpu.VMEM((tokens // LANES, LANES), F32),
            pltpu.VMEM((ring_x * CORES, tokens // LANES, LANES), F32),
            DMA((2 * ring_x,)), DMA((rounds + 1, 2 * ring_x)), DMA((rounds + 1, 2 * ring_x)), DMA((rounds, 6)), DMA((rounds, 6)),
            DMA((ring_x * CORES,)), DMA((ring_x * CORES,)), DMA((ring_x,)), DMA((ring_x,)),
        ],
        compiler_params=pltpu.CompilerParams(collective_id=cid, has_side_effects=True, vmem_limit_bytes=56 << 20),
        name='front',
    )(x, vec, w_x, w_y, weight)


def solution(mesh):
    wd_count = mesh.shape['wd']
    ch_count = mesh.shape['ch']
    chips = wd_count // CORES
    row_spec = P('dp', 'wd')
    specs = (row_spec, P('dp', None), P('wd'), P('wd', 'ch'), P('ch'), P('wd', 'ch'), P('ch'), P(None, 'ch'), P('ch'), P('ch'), P('ch', None, None), P('ch'), P('ch', None, None), P('ch'), P('ch', 'wd'), P('wd'), P('wd'), P('wd', 'ch'), P('ch'), P('wd', 'ch'), P('ch'), P('ch', 'wd'), P('wd'))

    def local_layer(resid_in, seg_pos, gain_temporal, w_x, bias_x, w_y, bias_y, conv_w, conv_bias, lam_param, rgate_w, rgate_b, igate_w, igate_b, w_o, bias_o, gain_mlp, w_g, bias_g, w_u, bias_u, w_d, bias_d):
        small = {'gain_temporal': gain_temporal, 'bias_x': bias_x, 'bias_y': bias_y, 'conv_w': conv_w, 'conv_bias': conv_bias, 'lam_param': lam_param, 'rgate_b': rgate_b,
                 'igate_b': igate_b, 'bias_o': bias_o, 'gain_mlp': gain_mlp, 'bias_g': bias_g, 'bias_u': bias_u, 'bias_d': bias_d}
        offs = {'rnn': w_x.shape[1], 'taps': conv_w.shape[0]}
        end = 0
        for name, val in sorted(small.items(), key=lambda item: -item[1].size):
            offs[name] = end
            end += val.size
        order = sorted(small, key=lambda name: offs[name])
        vec = jnp.concatenate([small[name].astype(F32).reshape(-1) for name in order]).reshape(1, end)
        tokens = resid_in.shape[0]
        part = jax.ShapeDtypeStruct((chips * w_g.shape[0], w_g.shape[1] // wd_count), BF16)
        u_pair, y_own, g0 = front(offs, resid_in, vec, w_x, w_y, w_g, part, chips, 4, 1)
        mixed, u0 = lru(offs, u_pair, y_own, seg_pos.reshape(1, tokens), vec, rgate_w, igate_w, w_u, part, chips, 2)
        resid, g1, u1 = ring_layer(mixed, w_o, resid_in, vec, offs['bias_o'], (w_g, w_u), part, chips, ch_count, 4, 3)
        inner = mlp_in(offs, resid, vec, w_g, w_u, (g0, u0, g1, u1), chips, ch_count, 4, 4)
        return ring_layer(inner, w_d, resid, vec, offs['bias_d'], (), part, chips, ch_count, 8, 5)

    return jax.shard_map(local_layer, mesh=mesh, in_specs=specs, out_specs=row_spec, check_vma=False)
```

```python
import functools

import jax
import jax.numpy as jnp
from jax import lax
from jax.experimental import pallas as pl
from jax.experimental.pallas import tpu as pltpu
from jax.sharding import PartitionSpec as P

EPS = 1e-6
CORES = 2
SEGS = 8
PAD = 8
LANES = 128
RIGHT, OPP, LEFT = 1, 2, 3
MESH = pl.DeviceIdType.MESH
F32 = jnp.float32
BF16 = jnp.bfloat16
VMEM = pl.BlockSpec(memory_space=pltpu.VMEM)
ANY = pl.BlockSpec(memory_space=pl.ANY)
DMA = pltpu.SemaphoreType.DMA
GRANT = 67043328


def neg_expm1(z):
    series = -z * (1.0 + z * (0.5 + z * (1.0 / 6.0 + z * (1.0 / 24.0))))
    return jnp.where(z > -0.03, series, 1.0 - jnp.exp(z))


def where_am_i():
    ring_x = lax.axis_size('wd') // CORES
    wd = lax.axis_index('wd')
    return ring_x, lax.axis_size('ch'), lax.axis_index('ch'), wd, lax.rem(wd, CORES), wd // CORES


def aligned(index, size):
    return pl.ds(pl.multiple_of(index * size, size), size)


def remote(src, dst, send, recv, device):
    return pltpu.make_async_remote_copy(src_ref=src, dst_ref=dst, send_sem=send, recv_sem=recv, device_id=device, device_id_type=MESH)


def greet(devices):
    barrier = pltpu.get_barrier_semaphore()
    for device in devices:
        pl.semaphore_signal(barrier, inc=1, device_id=device, device_id_type=MESH)
    return functools.partial(pl.semaphore_wait, barrier, len(devices))


def swaps(src, dst, k, sends, recvs):
    ring_x, _, _, _, core, chip = where_am_i()
    depth, ff = src.shape[0], dst.shape[1]
    return [remote(src.at[:, aligned(lax.rem(chip + step, ring_x) * CORES + k, ff)], dst.at[aligned(chip, depth), :],
                   sends.at[step], recvs.at[step], {'wd': lax.rem(chip + step, ring_x) * CORES + core}) for step in range(1, ring_x)]


def row_sums(x_ref, sums):
    for i in range(x_ref.shape[0] // LANES):
        sq = jnp.zeros((LANES, LANES), F32)
        for j in range(x_ref.shape[1] // LANES):
            val = x_ref[i * LANES:(i + 1) * LANES, j * LANES:(j + 1) * LANES].astype(F32)
            sq = sq + val * val
        sums[i:i + 1, :] = jnp.sum(sq.T, axis=0, keepdims=True)


def sum_copies(sums, all_sums, ss, sr):
    ring_x, _, _, wd, _, _ = where_am_i()
    count = ring_x * CORES
    return [remote(sums, all_sums.at[wd], ss.at[step], sr.at[step], {'wd': lax.rem(wd + step, count)}) for step in range(1, count)]


def as_column(row):
    return jnp.broadcast_to(row, (LANES, LANES)).T


def ring_body(rounds, bias_at, h_ref, w_ref, resid, vec_ref, out_ref, obuf, hbuf, pbuf, side, opp_buf, xs, xr, ys, yr, own_sem, ready, loads, after):
    share, depth = h_ref.shape[1:]
    cols_out = w_ref.shape[1]
    rr = share // rounds
    ring_x, ring_y, ch, wd, core, chip = where_am_i()
    regather = obuf is not None
    other = 1 - 2 * core
    partner = wd + other
    x_at = [lax.rem(chip + step, ring_x) * CORES + core for step in range(ring_x)]
    y_at = [lax.rem(ch + step, ring_y) for step in range(ring_y)]
    first, second, whole = 0, 1, None
    steps = (RIGHT, LEFT, OPP)

    def span(r, part=None):
        return aligned(r, rr) if part is None else aligned(2 * r + part, rr // 2)

    def cols(owner, r, part=None):
        return hbuf.at[:, span(r, part), aligned(owner, depth)]

    x_plan = [(wd, whole, x_at[RIGHT], x_at[LEFT]), (wd, whole, x_at[LEFT], x_at[RIGHT]),
              (x_at[LEFT], first, x_at[RIGHT], x_at[OPP]), (x_at[RIGHT], second, x_at[LEFT], x_at[OPP]),
              (wd, whole, partner, partner), (x_at[LEFT], whole, partner, x_at[LEFT] + other), (x_at[RIGHT], whole, partner, x_at[RIGHT] + other),
              (x_at[OPP], first, partner, x_at[OPP] + other), (x_at[OPP], second, partner, x_at[OPP] + other)]
    own_both, own_side, relay_both, side_both, opp_both, core_in = (0, 1), (4,), (2, 3), (5, 6), (7, 8), (4, 5, 6, 7, 8)

    def x_copy(k, r):
        owner, part, to, _ = x_plan[k]
        dst = cols(owner, r, part)
        src = h_ref.at[:, span(r), :] if k in own_both + own_side else dst
        return remote(src, dst, xs.at[r, k], xr.at[r, k], {'wd': to})

    def x_start(r, *ks):
        for k in ks:
            x_copy(k, r).start()

    def x_wait(r, *ks):
        for k in ks:
            ref = cols(x_plan[k][-1], r, x_plan[k][1])
            remote(ref, ref, xs.at[r, k], xr.at[r, k], {'wd': partner}).wait_recv()

    def sum_copy(step, r):
        return remote(pbuf.at[y_at[step], span(r), :], side.at[step - 1, span(r), :], ys.at[r, step], yr.at[r, step], {'ch': y_at[step]})

    def out_copy(step, r, owner):
        return remote(obuf.at[span(r), :], out_ref.at[y_at[owner], span(r), :], ys.at[r, ring_y + step], yr.at[r, ring_y + step], {'ch': y_at[step]})

    def keep_copy(r):
        return pltpu.make_async_copy(obuf.at[span(r), :], out_ref.at[ch, span(r), :], ys.at[r, 0])

    to_opp, to_side, relayed = (0, 1), (2, 3), (4, 5)

    def y_copy(k, r):
        piece, part, dst, to = [
            (OPP, first, opp_buf.at[0, span(r, first)], RIGHT), (OPP, second, opp_buf.at[1, span(r, second)], LEFT),
            (RIGHT, second, side.at[0, span(r, second)], RIGHT), (LEFT, first, side.at[1, span(r, first)], LEFT),
            (RIGHT, first, side.at[0, span(r, first)], RIGHT), (LEFT, second, side.at[1, span(r, second)], LEFT)][k]
        return remote(pbuf.at[y_at[piece], span(r, part)], dst, ys.at[r, k], yr.at[r, k], {'ch': y_at[to]})

    def known(r, bound):
        return not isinstance(r, int) or r < bound

    def own(r):
        if known(r, rounds):
            x_start(r, *own_both, *own_side)

    def stage1(r):
        if known(r, rounds):
            for side_in, on in zip(own_both, relay_both):
                x_wait(r, side_in)
                x_start(r, on)
            x_start(r, *side_both)
            own(r + 2)
            if isinstance(r, int) and r == rounds - 1:
                after()

    def stage2(r):
        for side_in, on in zip(relay_both, opp_both):
            x_wait(r, side_in)
            x_start(r, on)

    def dots(r):
        x_wait(r, *core_in)
        each = max(1, 256 // rr)

        def one(i, carry):
            at = pl.ds(i * each, each)
            block = hbuf[at, span(r), :].reshape(each * rr, hbuf.shape[2])
            part = jnp.dot(block, w_ref[...], preferred_element_type=F32)
            pbuf[at, span(r), :] = part.astype(BF16).reshape(each, rr, cols_out)
            return carry
        lax.fori_loop(0, ring_y // each, one, 0)
        if regather:
            for step in steps:
                sum_copy(step, r).start()
        else:
            for k in to_opp + to_side:
                y_copy(k, r).start()

    def combine(r):
        for k, piece, part in zip(to_opp, (RIGHT, LEFT), (first, second)):
            y_copy(k, r).wait_recv()
            at = y_at[piece], span(r, part)
            pbuf[at] = (pbuf[at].astype(F32) + opp_buf[k, span(r, part), :].astype(F32)).astype(BF16)
            y_copy(relayed[k], r).start()

    def final(r):
        rows = span(r)
        if regather:
            for step in steps:
                sum_copy(step, r).wait_recv()
        else:
            for k in to_side + relayed:
                y_copy(k, r).wait_recv()
        total = pbuf[ch, rows, :].astype(F32)
        for slot in range(side.shape[0]):
            total = total + side[slot, rows, :].astype(F32)
        total = resid[rows, :].astype(F32) + total + vec_ref[:, bias_at:bias_at + cols_out]
        if regather:
            obuf[rows, :] = total.astype(obuf.dtype)
            for step in steps:
                out_copy(step, r, 0).start()
            keep_copy(r).start()
        else:
            out_ref[rows, :] = total

    def turn(r):
        stage1(r + 1)
        stage2(r)
        later = not isinstance(r, int) or r >= 1
        if later and not regather:
            combine(r - 1)
        dots(r)
        if later:
            final(r - 1)

    mine = pltpu.make_async_copy(h_ref, hbuf.at[:, :, aligned(wd, depth)], own_sem)
    mine.start()
    ready()
    own(0)
    own(1)
    mine.wait()
    for one in loads:
        one.wait()
    stage1(0)
    turn(0)

    def middle(r, carry):
        turn(r)
        return carry
    lax.fori_loop(1, rounds - 3, middle, 0)
    for r in range(max(1, rounds - 3), rounds):
        turn(r)
    if not regather:
        combine(rounds - 1)
    final(rounds - 1)

    def finish():
        def drain(r, carry):
            for k in range(len(x_plan)):
                x_copy(k, r).wait_send()
            if regather:
                for step in steps:
                    sum_copy(step, r).wait_send()
                    out_copy(step, r, ring_y - step).wait_recv()
                    out_copy(step, r, 0).wait_send()
                keep_copy(r).wait()
            else:
                for k in to_opp + to_side + relayed:
                    y_copy(k, r).wait_send()
            return carry
        lax.fori_loop(0, rounds, drain, 0)
    return finish


def ring_peers():
    ring_x, ring_y, ch, wd, core, chip = where_am_i()
    return [{'wd': wd + 1 - 2 * core}] + [{'wd': lax.rem(chip + step, ring_x) * CORES + core} for step in (RIGHT, LEFT)] + [{'ch': lax.rem(ch + step, ring_y)} for step in range(1, ring_y)]


def mlp_out_kernel(rounds, bias_at, h_ref, w_in_ref, resid_ref, vec_ref, out_ref, w_ref, resid, obuf, hbuf, pbuf, side, xs, xr, ys, yr, local_sem):
    ready = greet(ring_peers())
    loads = [pltpu.make_async_copy(w_in_ref, w_ref, local_sem.at[1]), pltpu.make_async_copy(resid_ref, resid, local_sem.at[2])]
    for one in loads:
        one.start()
    ring_body(rounds, bias_at, h_ref, w_ref, resid, vec_ref, out_ref, obuf, hbuf, pbuf, side, None, xs, xr, ys, yr, local_sem.at[0], ready, loads, lambda: None)()


def ring_scratch(ring_y, share, wide, cols, rounds, regather):
    return [pltpu.VMEM((ring_y, share, wide), BF16), pltpu.VMEM((ring_y, share, cols), BF16),
            pltpu.VMEM((ring_y - 1 if regather else 2, share, cols), BF16)]


def ring_sems(rounds, ring_y):
    return [DMA((rounds, 9)), DMA((rounds, 9)), DMA((rounds, 2 * ring_y)), DMA((rounds, 2 * ring_y))]


def mlp_out(h, w, resid, vec, bias_at, ring_y, rounds, cid):
    share, cols = resid.shape
    return pl.pallas_call(
        functools.partial(mlp_out_kernel, rounds, bias_at),
        out_shape=jax.ShapeDtypeStruct((ring_y, share, cols), BF16),
        in_specs=[ANY, ANY, ANY, VMEM],
        out_specs=ANY,
        scratch_shapes=[pltpu.VMEM(w.shape, BF16), pltpu.VMEM(resid.shape, F32), pltpu.VMEM(resid.shape, BF16)]
        + ring_scratch(ring_y, share, w.shape[0], cols, rounds, True) + ring_sems(rounds, ring_y) + [DMA((3,))],
        compiler_params=pltpu.CompilerParams(collective_id=cid, has_side_effects=True, vmem_limit_bytes=GRANT),
        name='mlp_out',
    )(h, w, resid, vec).reshape(ring_y * share, cols)


def mid_kernel(rounds, offs, h_ref, w_o_ref, x_ref, vec_ref, wg_ref, wu_ref, g0_ref, u0_ref, inner_ref, resid_out, resid_ref, x_rows, hbuf, pbuf, side, opp_buf, out_ref, nbuf, w_ref, keep, send, got, sums, all_sums,
               xs, xr, ys, yr, ns, nr, ss, sr, load_sem, local_sem, ws, wr, io_sem):
    share, width = resid_ref.shape
    ring_x, ring_y, ch, wd, core, chip = where_am_i()
    wd_count = ring_x * CORES
    rr = share // rounds
    half = rr // 2
    partner = wd + 1 - 2 * core
    ff = out_ref.shape[2]

    def device(d1, d2):
        return {'ch': lax.rem(ch + d1 * (1 - core) + d2 * core, ring_y), 'wd': lax.rem(chip + d1 * core + d2 * (1 - core), ring_x) * CORES + core}

    def block(d1, d2, r, part=None):
        rows = pl.ds(r * rr, rr) if part is None else pl.ds(r * rr + part * half, half)
        at = lax.rem(chip + d1 * core + d2 * (1 - core), ring_x)
        return nbuf.at[lax.rem(ch + d1 * (1 - core) + d2 * core, ring_y), rows, aligned(at, width)]

    whole = None
    plan = [((0, 0), (RIGHT, 0), (LEFT, 0), whole), ((0, 0), (LEFT, 0), (RIGHT, 0), whole),
            ((LEFT, 0), (RIGHT, 0), (OPP, 0), 0), ((RIGHT, 0), (LEFT, 0), (OPP, 0), 1)]
    for d1 in (0, LEFT, RIGHT, OPP):
        plan += [((d1, 0), (0, RIGHT), (d1, LEFT), whole), ((d1, 0), (0, LEFT), (d1, RIGHT), whole),
                 ((d1, LEFT), (0, RIGHT), (d1, OPP), 0), ((d1, RIGHT), (0, LEFT), (d1, OPP), 1)]
    core_step = len(plan)

    def copy(k, r):
        src, to, _, part = plan[k]
        ref = block(*src, r, part)
        return remote(ref, ref, ns.at[r, k], nr.at[r, k], device(*to))

    def start(r, *ks):
        for k in ks:
            copy(k, r).start()

    def wait(r, *ks):
        for k in ks:
            ref = block(*plan[k][2], r, plan[k][3])
            remote(ref, ref, ns.at[r, k], nr.at[r, k], device(RIGHT, 0)).wait_recv()

    def own(r):
        if r < rounds:
            start(r, 0, 1, 4, 5)

    def stage1(r):
        if r < rounds:
            wait(r, 0, 1)
            start(r, 2, 3, 8, 9, 12, 13)
            wait(r, 4, 5)
            start(r, 6, 7)

    def stage2(r):
        if r < rounds:
            wait(r, 2, 3)
            start(r, 16, 17)
            wait(r, 8, 9)
            start(r, 10, 11)
            wait(r, 12, 13)
            start(r, 14, 15)

    def stage3(r):
        if r < rounds:
            wait(r, 16, 17)
            start(r, 18, 19)

    def halves(r):
        return remote(send.at[r], got.at[r], ns.at[r, core_step], nr.at[r, core_step], {'wd': partner})

    each = max(1, 256 // rr)

    def dots(r, mine):
        def one(i, carry):
            at = pl.ds(i * each, each)
            rows = nbuf[at, pl.ds(r * rr, rr), :].reshape(each * rr, nbuf.shape[2])
            if mine:
                keep[at] = jnp.dot(rows, w_ref[core], preferred_element_type=F32).reshape(each, rr, 2 * ff)
            else:
                send[r, at] = jnp.dot(rows, w_ref[1 - core], preferred_element_type=F32).astype(BF16).reshape(each, rr, 2 * ff)
            return carry
        lax.fori_loop(0, ring_y // each, one, 0)

    def inner_copy(r):
        at = pl.ds(r * rr, rr)
        return pltpu.make_async_copy(out_ref.at[:, at, :], inner_ref.at[:, at, :], io_sem.at[r])

    def finish(r):
        halves(r).wait_recv()
        b_g, b_u = (vec_ref[:, pl.ds(pl.multiple_of(offs[name] + wd * ff, LANES), ff)] for name in ('bias_g', 'bias_u'))

        def one(q, carry):
            total = keep[q] + got[r, q].astype(F32)
            out_ref[q, pl.ds(r * rr, rr), :] = (jax.nn.gelu(total[:, :ff] + b_g, approximate=True) * (total[:, ff:] + b_u)).astype(BF16)
            return carry
        lax.fori_loop(0, ring_y, one, 0)
        inner_copy(r).start()

    ready = greet([{'wd': lax.rem(wd + step, wd_count)} for step in range(1, wd_count)] + [{'ch': lax.rem(ch + step, ring_y)} for step in range(1, ring_y)])
    loads = []
    for m, (full, part) in enumerate(((wg_ref, g0_ref), (wu_ref, u0_ref))):
        for k in range(CORES):
            for step in range(1 if k else ring_x):
                rows = aligned(lax.rem(chip + step, ring_x), width)
                src = part.at[rows, :] if step else full.at[:, aligned(chip * CORES + k, ff)]
                loads.append(pltpu.make_async_copy(src, w_ref.at[k, rows, pl.ds(m * ff, ff)], load_sem.at[k, m, step]))
    moves = [one for m, full in enumerate((wg_ref, wu_ref)) for one in swaps(full, w_ref.at[1, :, pl.ds(m * ff, ff)], 1, ws.at[m], wr.at[m])]
    first_load = pltpu.make_async_copy(x_ref.at[aligned(ch, share), :], x_rows, local_sem.at[1])
    first_load.start()

    def after():
        for one in moves + loads:
            one.start()

    ring_done = ring_body(rounds, offs['bias_o'], h_ref, w_o_ref, x_rows, vec_ref, resid_ref, None, hbuf, pbuf, side, opp_buf, xs, xr, ys, yr, local_sem.at[0], ready, [first_load], after)
    keep_resid = pltpu.make_async_copy(resid_ref, resid_out, local_sem.at[2])
    keep_resid.start()
    row_sums(resid_ref, sums)
    all_sums[wd] = sums[...]
    for one in sum_copies(sums, all_sums, ss, sr):
        one.start()
    for one in sum_copies(sums, all_sums, ss, sr):
        one.wait()
    scale = lax.rsqrt(jnp.sum(all_sums[...], axis=0) / (width * wd_count) + EPS)
    gain = 1.0 + vec_ref[:, offs['gain_mlp']:offs['gain_mlp'] + width]

    def norm(r):
        for i in range(r * rr // LANES, (r + 1) * rr // LANES):
            factor = as_column(scale[i:i + 1, :])[:, 0:1]
            rows = slice(i * LANES, (i + 1) * LANES)
            nbuf[ch, rows, aligned(chip, width)] = (resid_ref[rows, :] * factor * gain).astype(BF16)

    for r in range(rounds):
        norm(r)
        if r < 3:
            own(r)
    stage1(0)
    stage2(0)
    stage1(1)
    stage3(0)
    stage2(1)
    for one in loads + moves:
        one.wait()
    for r in range(rounds):
        wait(r, 6, 7, 10, 11, 14, 15, 18, 19)
        dots(r, False)
        halves(r).start()
        own(r + 3)
        stage1(r + 2)
        stage3(r + 1)
        dots(r, True)
        stage2(r + 2)
        finish(r)
    for r in range(rounds):
        inner_copy(r).wait()
        halves(r).wait_send()
        for k in range(core_step):
            copy(k, r).wait_send()
    keep_resid.wait()
    ring_done()


def mid(offs, h, w_o, x, vec, w_g, w_u, parts, ring_x, ring_y, rounds, cid):
    tokens, width = x.shape
    share = tokens // ring_y
    depth, ff = parts[0].shape
    cols = 2 * ff
    rr = share // rounds
    return pl.pallas_call(
        functools.partial(mid_kernel, rounds, offs),
        out_shape=(jax.ShapeDtypeStruct((ring_y, share, ff), BF16), jax.ShapeDtypeStruct((share, width), F32)),
        in_specs=[ANY, VMEM, ANY, VMEM] + [ANY] * 4,
        out_specs=(ANY, ANY),
        scratch_shapes=[pltpu.VMEM((share, width), F32), pltpu.VMEM((share, width), BF16)] + ring_scratch(ring_y, share, w_o.shape[0], width, rounds, False) + [
            pltpu.VMEM((2, share, width), BF16),
            pltpu.VMEM((ring_y, share, ff), BF16),
            pltpu.VMEM((ring_y, share, depth), BF16),
            pltpu.VMEM((CORES, depth, cols), BF16),
            pltpu.VMEM((ring_y, rr, cols), F32),
            pltpu.VMEM((rounds, ring_y, rr, cols), BF16),
            pltpu.VMEM((rounds, ring_y, rr, cols), BF16),
            pltpu.VMEM((share // LANES, LANES), F32),
            pltpu.VMEM((ring_x * CORES, share // LANES, LANES), F32),
        ] + ring_sems(rounds, ring_y) + [
            DMA((rounds, 21)), DMA((rounds, 21)), DMA((ring_x * CORES,)), DMA((ring_x * CORES,)),
            DMA((CORES, 2, ring_x)), DMA((3,)), DMA((2, ring_x)), DMA((2, ring_x)), DMA((rounds,)),
        ],
        compiler_params=pltpu.CompilerParams(collective_id=cid, has_side_effects=True, vmem_limit_bytes=GRANT),
        name='mid',
    )(h.reshape(ring_y, share, h.shape[1]), w_o, x, vec, w_g, w_u, *parts)


def front_kernel(rounds, offs, x_ref, vec_ref, pos_ref, rg_ref, ig_ref, w_x_ref, w_y_ref, wg_ref, wu_ref, out_ref, part_g, part_u, nbuf, wbuf, pbuf, opp_buf, side, u_ref, y_ref, u32, a_s, b_s, gate_w, sums, all_sums, local_sem, ps, pr, xs, xr, ss, sr, ws, wr):
    tokens, width = x_ref.shape
    ring_x, _, _, wd, core, chip = where_am_i()
    wd_count = ring_x * CORES
    rr = tokens // rounds
    half = rr // 2
    mine = y_ref.shape[1]
    piece = CORES * mine
    partner = wd + 1 - 2 * core
    right, opp, left = (lax.rem(chip + step, ring_x) for step in (RIGHT, OPP, LEFT))
    first, second = 0, 1

    def span(r, part=None):
        return pl.ds(r * rr, rr) if part is None else pl.ds(r * rr + part * half, half)

    def weight(k, of):
        j, m = k // 2, k % 2
        src = (w_x_ref, w_y_ref)[m].at[:, pl.ds(pl.multiple_of((j * CORES + of) * mine, mine), mine)]
        return src, wbuf.at[aligned(core, width), pl.ds(j * piece + m * mine, mine)]

    def weight_out(k):
        src, dst = weight(k, 1 - core)
        return pltpu.make_async_remote_copy(src_ref=src, dst_ref=dst, send_sem=ps.at[rounds, k], recv_sem=pr.at[rounds, k], device_id={'wd': partner}, device_id_type=MESH)

    def weight_own(k):
        src, dst = weight(k, core)
        return pltpu.make_async_copy(src, dst, local_sem.at[k])

    def weight_in(k):
        ref = wbuf.at[aligned(1 - core, width), pl.ds((k // 2) * piece + (k % 2) * mine, mine)]
        pltpu.make_async_remote_copy(src_ref=ref, dst_ref=ref, send_sem=ps.at[rounds, k], recv_sem=pr.at[rounds, k], device_id={'wd': partner}, device_id_type=MESH).wait_recv()

    def normed(r, of):
        ref = nbuf.at[span(r), aligned(of, width)]
        return pltpu.make_async_remote_copy(src_ref=ref, dst_ref=ref, send_sem=ps.at[r, 0], recv_sem=pr.at[r, 0], device_id={'wd': partner}, device_id_type=MESH)

    def u_copy(r, of):
        ref = u_ref.at[span(r), aligned(of, mine)]
        return remote(ref, ref, ps.at[r, 1], pr.at[r, 1], {'wd': partner})

    def part_of(dest, r, part):
        return pbuf.at[span(r, part), aligned(dest, piece)]

    def x_send(k, r):
        rows = pl.ds(r * half, half)
        dest, part, dst, to = [
            (opp, first, opp_buf.at[0, rows], right), (opp, second, opp_buf.at[1, rows], left),
            (right, second, side.at[0, span(r, second)], right), (left, first, side.at[1, span(r, first)], left),
            (right, first, side.at[0, span(r, first)], right), (left, second, side.at[1, span(r, second)], left)][k]
        return remote(part_of(dest, r, part), dst, xs.at[r, k], xr.at[r, k], {'wd': to * CORES + core})

    def norm(r):
        for i in range(rr // LANES):
            tile = r * (rr // LANES) + i
            factor = as_column(scale[tile:tile + 1, :])[:, 0:1]
            rows = slice(tile * LANES, (tile + 1) * LANES)
            nbuf[rows, aligned(core, width)] = (x_ref[rows, :].astype(F32) * factor * gain).astype(BF16)
        normed(r, core).start()

    def dots(r):
        normed(r, 1 - core).wait_recv()
        step_rows = rr // 4

        def one(i, carry):
            rows = pl.ds(pl.multiple_of(r * rr + i * step_rows, step_rows), step_rows)
            pbuf[rows, :] = jnp.dot(nbuf[rows, :], wbuf[...], preferred_element_type=F32).astype(BF16)
            return carry
        lax.fori_loop(0, 4, one, 0)
        for k in range(4):
            x_send(k, r).start()

    def combine(r):
        rows = pl.ds(r * half, half)
        for k, dest, part, back in ((0, right, first, 4), (1, left, second, 5)):
            x_send(k, r).wait_recv()
            at = (span(r, part), aligned(dest, piece))
            pbuf[at] = (pbuf[at].astype(F32) + opp_buf[k, rows, :].astype(F32)).astype(BF16)
            x_send(back, r).start()

    def final(r):
        for k in range(2, 6):
            x_send(k, r).wait_recv()
        rows = span(r)
        total = pbuf[rows, aligned(chip, piece)].astype(F32) + side[0, rows, :].astype(F32) + side[1, rows, :].astype(F32)
        b_x, b_y = (vec_ref[:, pl.ds(pl.multiple_of(offs[name] + wd * mine, mine), mine)] for name in ('bias_x', 'bias_y'))
        u_ref[rows, aligned(core, mine)] = (total[:, :mine] + b_x).astype(BF16)
        u_copy(r, core).start()
        y_ref[rows, :] = jax.nn.gelu(total[:, mine:] + b_y, approximate=True).astype(BF16)

    wide = CORES * mine
    tile = tokens // SEGS
    pitch = tile + PAD
    per_seg = tile // LANES
    per_round = rr // LANES
    n_taps = offs['taps']

    def vec(name, index, size):
        return vec_ref[:, pl.ds(pl.multiple_of(offs[name] + index * size, size), size)]

    taps = [vec_ref[:, pl.ds(pl.multiple_of(offs['conv_w'] + k * offs['rnn'] + chip * wide, wide), wide)] for k in range(n_taps)]
    cbias = vec('conv_bias', chip, wide)
    gate_b = jnp.concatenate([vec('rgate_b', wd, mine), vec('igate_b', wd, mine)], axis=1)
    lam = -vec('lam_param', wd, mine)
    soft = -8.0 * (jnp.maximum(lam, 0.0) + jnp.log(1.0 + jnp.exp(-jnp.abs(lam))))

    def gates(r):
        u_copy(r, 1 - core).wait_recv()

        def widen(i, carry):
            rows = pl.multiple_of(i * LANES, LANES)
            u32[pl.ds(rows + PAD, LANES), :] = u_ref[pl.ds(rows, LANES), :].astype(F32)
            return carry
        lax.fori_loop(r * per_round, (r + 1) * per_round, widen, 0)

        def one(i, carry):
            rows = pl.multiple_of(i * LANES, LANES)
            window = u32[pl.ds(rows, LANES + PAD), :]
            pos = as_column(pos_ref[:, pl.ds(rows, LANES)].astype(F32))
            pair = jnp.concatenate([pos, pos], axis=1)
            total = cbias + window[PAD:] * taps[0]
            for k in range(1, n_taps):
                total = total + jnp.where(pair >= k, window[PAD - k:PAD - k + LANES], 0.0) * taps[k]
            conv = total.astype(BF16)
            both = jax.nn.sigmoid(jnp.dot(conv, gate_w[...], preferred_element_type=F32) + gate_b)
            log_a = both[:, :mine] * soft
            reset = pos == 0
            decay = jnp.where(reset, 0.0, jnp.exp(log_a))
            scale = jnp.where(reset, 1.0, jnp.sqrt(neg_expm1(2.0 * log_a)))
            held = conv.astype(F32)
            drive = scale * both[:, mine:] * jnp.where(core == 0, held[:, :mine], held[:, mine:])
            seg = i // per_seg
            at = pl.multiple_of(seg * pitch + (i - seg * per_seg) * LANES, PAD)
            a_s[pl.ds(at, LANES), :] = decay
            b_s[pl.ds(at, LANES), :] = drive
            return carry
        lax.fori_loop(r * per_round, (r + 1) * per_round, one, 0)

    def scan():
        def steps(i, carry):
            hid, acc = carry
            for j in range(8):
                at = pl.ds(i * 8 + j, SEGS, stride=pitch)
                a = a_s[at, :]
                hid = a * hid + b_s[at, :]
                acc = a * acc
                b_s[at, :] = hid
                a_s[at, :] = acc
            return hid, acc
        hid, acc = lax.fori_loop(0, tile // 8, steps, (jnp.zeros((SEGS, mine), F32), jnp.ones((SEGS, mine), F32)))
        entry = jnp.zeros((1, mine), F32)
        for seg in range(SEGS):
            for q in range(per_seg):
                at = seg * pitch + q * LANES
                hidden = b_s[at:at + LANES, :] + a_s[at:at + LANES, :] * entry
                rows = slice(seg * tile + q * LANES, seg * tile + (q + 1) * LANES)
                out_ref[rows, :] = (hidden * y_ref[rows, :].astype(F32)).astype(BF16)
            entry = hid[seg:seg + 1] + acc[seg:seg + 1] * entry

    ready = greet([{'wd': lax.rem(wd + step, wd_count)} for step in range(1, wd_count)])
    for k in range(2 * ring_x):
        weight_own(k).start()
    row_sums(x_ref, sums)
    all_sums[wd] = sums[...]
    ready()
    for one in sum_copies(sums, all_sums, ss, sr):
        one.start()
    for k in range(2 * ring_x):
        weight_out(k).start()
    moves, later = swaps(wg_ref, part_g, 0, ws.at[0], wr.at[0]), swaps(wu_ref, part_u, 0, ws.at[1], wr.at[1])
    for one in moves:
        one.start()
    gate_w[:, :mine] = rg_ref[chip, :, aligned(core, mine)]
    gate_w[:, mine:] = ig_ref[chip, :, aligned(core, mine)]
    u32[0:PAD, :] = jnp.zeros((PAD, wide), F32)
    for one in sum_copies(sums, all_sums, ss, sr):
        one.wait()
    scale = lax.rsqrt(jnp.sum(all_sums[...], axis=0) / (width * wd_count) + EPS)
    gain = 1.0 + vec_ref[:, offs['gain_temporal']:offs['gain_temporal'] + width]
    norm(0)
    for k in range(2 * ring_x):
        weight_own(k).wait()
        weight_in(k)
    for r in range(rounds):
        if r + 1 < rounds:
            norm(r + 1)
        dots(r)
        if r >= 1:
            combine(r - 1)
        if r >= 2:
            final(r - 2)
        if r >= 3:
            gates(r - 3)
    combine(rounds - 1)
    for one in later:
        one.start()
    final(rounds - 2)
    gates(rounds - 3)
    final(rounds - 1)
    gates(rounds - 2)
    gates(rounds - 1)
    scan()
    for k in range(2 * ring_x):
        weight_out(k).wait_send()
    for r in range(rounds):
        normed(r, core).wait_send()
        u_copy(r, core).wait_send()
        for k in range(6):
            x_send(k, r).wait_send()
    for one in moves + later:
        one.wait()


def front(offs, x, vec, pos, rgate_w, igate_w, w_x, w_y, w_g, w_u, part, ring_x, rounds, cid):
    tokens, width = x.shape
    rnn = w_x.shape[1]
    mine = rnn // (ring_x * CORES)
    wide = CORES * mine
    seg_rows = SEGS * (tokens // SEGS + PAD)
    return pl.pallas_call(
        functools.partial(front_kernel, rounds, offs),
        out_shape=(jax.ShapeDtypeStruct((tokens, mine), BF16), part, part),
        in_specs=[VMEM] * 5 + [ANY] * 4,
        out_specs=(VMEM, ANY, ANY),
        scratch_shapes=[
            pltpu.VMEM((tokens, CORES * width), BF16),
            pltpu.VMEM((CORES * width, rnn), BF16),
            pltpu.VMEM((tokens, rnn), BF16),
            pltpu.VMEM((2, tokens // 2, wide), BF16),
            pltpu.VMEM((2, tokens, wide), BF16),
            pltpu.VMEM((tokens, wide), BF16),
            pltpu.VMEM((tokens, mine), BF16),
            pltpu.VMEM((tokens + PAD, wide), F32),
            pltpu.VMEM((seg_rows, mine), F32),
            pltpu.VMEM((seg_rows, mine), F32),
            pltpu.VMEM((wide, wide), BF16),
            pltpu.VMEM((tokens // LANES, LANES), F32),
            pltpu.VMEM((ring_x * CORES, tokens // LANES, LANES), F32),
            DMA((2 * ring_x,)), DMA((rounds + 1, 2 * ring_x)), DMA((rounds + 1, 2 * ring_x)), DMA((rounds, 6)), DMA((rounds, 6)),
            DMA((ring_x * CORES,)), DMA((ring_x * CORES,)), DMA((2, ring_x)), DMA((2, ring_x)),
        ],
        compiler_params=pltpu.CompilerParams(collective_id=cid, has_side_effects=True, vmem_limit_bytes=GRANT),
        name='front',
    )(x, vec, pos, rgate_w, igate_w, w_x, w_y, w_g, w_u)


def solution(mesh):
    wd_count = mesh.shape['wd']
    ch_count = mesh.shape['ch']
    chips = wd_count // CORES
    row_spec = P('dp', 'wd')
    specs = (row_spec, P('dp', None), P('wd'), P('wd', 'ch'), P('ch'), P('wd', 'ch'), P('ch'), P(None, 'ch'), P('ch'), P('ch'), P('ch', None, None), P('ch'), P('ch', None, None), P('ch'), P('ch', 'wd'), P('wd'), P('wd'), P('wd', 'ch'), P('ch'), P('wd', 'ch'), P('ch'), P('ch', 'wd'), P('wd'))

    def local_layer(resid_in, seg_pos, gain_temporal, w_x, bias_x, w_y, bias_y, conv_w, conv_bias, lam_param, rgate_w, rgate_b, igate_w, igate_b, w_o, bias_o, gain_mlp, w_g, bias_g, w_u, bias_u, w_d, bias_d):
        small = {'gain_temporal': gain_temporal, 'bias_x': bias_x, 'bias_y': bias_y, 'conv_w': conv_w, 'conv_bias': conv_bias, 'lam_param': lam_param, 'rgate_b': rgate_b,
                 'igate_b': igate_b, 'bias_o': bias_o, 'gain_mlp': gain_mlp, 'bias_g': bias_g, 'bias_u': bias_u, 'bias_d': bias_d}
        offs = {'rnn': w_x.shape[1], 'taps': conv_w.shape[0]}
        end = 0
        for name, val in sorted(small.items(), key=lambda item: -item[1].size):
            offs[name] = end
            end += val.size
        spread = [lax.pad(small[name].astype(F32).reshape(-1), jnp.zeros((), F32), [(offs[name], end - offs[name] - small[name].size, 0)]) for name in small]
        vec = functools.reduce(jnp.add, spread).reshape(1, end)
        tokens = resid_in.shape[0]
        part = jax.ShapeDtypeStruct((chips * w_g.shape[0], w_g.shape[1] // wd_count), BF16)
        mixed, g0, u0 = front(offs, resid_in, vec, seg_pos.reshape(1, tokens), rgate_w, igate_w, w_x, w_y, w_g, w_u, part, chips, 8, 1)
        inner, resid = mid(offs, mixed, w_o, resid_in, vec, w_g, w_u, (g0, u0), chips, ch_count, 4, 2)
        return mlp_out(inner, w_d, resid, vec, offs['bias_d'], ch_count, 16, 3)

    return jax.shard_map(local_layer, mesh=mesh, in_specs=specs, out_specs=row_spec, check_vma=False)
```

```python
import functools

import jax
import jax.numpy as jnp
from jax import lax
from jax.experimental import pallas as pl
from jax.experimental.pallas import tpu as pltpu
from jax.sharding import PartitionSpec as P

EPS = 1e-6
CORES = 2
SEGS = 8
PAD = 8
LANES = 128
RIGHT, OPP, LEFT = 1, 2, 3
MESH = pl.DeviceIdType.MESH
F32 = jnp.float32
BF16 = jnp.bfloat16
VMEM = pl.BlockSpec(memory_space=pltpu.VMEM)
ANY = pl.BlockSpec(memory_space=pl.ANY)
DMA = pltpu.SemaphoreType.DMA
GRANT = 67043328


def neg_expm1(z):
    series = -z * (1.0 + z * (0.5 + z * (1.0 / 6.0 + z * (1.0 / 24.0))))
    return jnp.where(z > -0.03, series, 1.0 - jnp.exp(z))


def where_am_i():
    ring_x = lax.axis_size('wd') // CORES
    wd = lax.axis_index('wd')
    return ring_x, lax.axis_size('ch'), lax.axis_index('ch'), wd, lax.rem(wd, CORES), wd // CORES


def aligned(index, size):
    return pl.ds(pl.multiple_of(index * size, size), size)


def remote(src, dst, send, recv, device):
    return pltpu.make_async_remote_copy(src_ref=src, dst_ref=dst, send_sem=send, recv_sem=recv, device_id=device, device_id_type=MESH)


def greet(devices):
    barrier = pltpu.get_barrier_semaphore()
    for device in devices:
        pl.semaphore_signal(barrier, inc=1, device_id=device, device_id_type=MESH)
    return functools.partial(pl.semaphore_wait, barrier, len(devices))


def swaps(src, dst, k, sends, recvs):
    ring_x, _, _, _, core, chip = where_am_i()
    depth, ff = src.shape[0], dst.shape[1]
    return [remote(src.at[:, aligned(lax.rem(chip + step, ring_x) * CORES + k, ff)], dst.at[aligned(chip, depth), :],
                   sends.at[step], recvs.at[step], {'wd': lax.rem(chip + step, ring_x) * CORES + core}) for step in range(1, ring_x)]


def row_sums(x_ref, sums):
    for i in range(x_ref.shape[0] // LANES):
        sq = jnp.zeros((LANES, LANES), F32)
        for j in range(x_ref.shape[1] // LANES):
            val = x_ref[i * LANES:(i + 1) * LANES, j * LANES:(j + 1) * LANES].astype(F32)
            sq = sq + val * val
        sums[i:i + 1, :] = jnp.sum(sq.T, axis=0, keepdims=True)


def sum_copies(sums, all_sums, ss, sr):
    ring_x, _, _, wd, _, _ = where_am_i()
    count = ring_x * CORES
    return [remote(sums, all_sums.at[wd], ss.at[step], sr.at[step], {'wd': lax.rem(wd + step, count)}) for step in range(1, count)]


def as_column(row):
    return jnp.broadcast_to(row, (LANES, LANES)).T


def ring_body(rounds, bias_at, h_ref, w_ref, resid, vec_ref, out_ref, obuf, hbuf, pbuf, side, opp_buf, xs, xr, ys, yr, own_sem, ready, loads, after):
    share, depth = h_ref.shape[1:]
    cols_out = w_ref.shape[1]
    rr = share // rounds
    ring_x, ring_y, ch, wd, core, chip = where_am_i()
    regather = obuf is not None
    other = 1 - 2 * core
    partner = wd + other
    x_at = [lax.rem(chip + step, ring_x) * CORES + core for step in range(ring_x)]
    y_at = [lax.rem(ch + step, ring_y) for step in range(ring_y)]
    first, second, whole = 0, 1, None
    steps = (RIGHT, LEFT, OPP)

    def span(r, part=None):
        return aligned(r, rr) if part is None else aligned(2 * r + part, rr // 2)

    def cols(owner, r, part=None):
        return hbuf.at[:, span(r, part), aligned(owner, depth)]

    x_plan = [(wd, whole, x_at[RIGHT], x_at[LEFT]), (wd, whole, x_at[LEFT], x_at[RIGHT]),
              (x_at[LEFT], first, x_at[RIGHT], x_at[OPP]), (x_at[RIGHT], second, x_at[LEFT], x_at[OPP]),
              (wd, whole, partner, partner), (x_at[LEFT], whole, partner, x_at[LEFT] + other), (x_at[RIGHT], whole, partner, x_at[RIGHT] + other),
              (x_at[OPP], first, partner, x_at[OPP] + other), (x_at[OPP], second, partner, x_at[OPP] + other)]
    own_both, own_side, relay_both, side_both, opp_both, core_in = (0, 1), (4,), (2, 3), (5, 6), (7, 8), (4, 5, 6, 7, 8)

    def x_copy(k, r):
        owner, part, to, _ = x_plan[k]
        dst = cols(owner, r, part)
        src = h_ref.at[:, span(r), :] if k in own_both + own_side else dst
        return remote(src, dst, xs.at[r, k], xr.at[r, k], {'wd': to})

    def x_start(r, *ks):
        for k in ks:
            x_copy(k, r).start()

    def x_wait(r, *ks):
        for k in ks:
            ref = cols(x_plan[k][-1], r, x_plan[k][1])
            remote(ref, ref, xs.at[r, k], xr.at[r, k], {'wd': partner}).wait_recv()

    def sum_copy(step, r):
        return remote(pbuf.at[y_at[step], span(r), :], side.at[step - 1, span(r), :], ys.at[r, step], yr.at[r, step], {'ch': y_at[step]})

    def out_copy(step, r, owner):
        return remote(obuf.at[span(r), :], out_ref.at[y_at[owner], span(r), :], ys.at[r, ring_y + step], yr.at[r, ring_y + step], {'ch': y_at[step]})

    def keep_copy(r):
        return pltpu.make_async_copy(obuf.at[span(r), :], out_ref.at[ch, span(r), :], ys.at[r, 0])

    to_opp, to_side, relayed = (0, 1), (2, 3), (4, 5)

    def y_copy(k, r):
        piece, part, dst, to = [
            (OPP, first, opp_buf.at[0, span(r, first)], RIGHT), (OPP, second, opp_buf.at[1, span(r, second)], LEFT),
            (RIGHT, second, side.at[0, span(r, second)], RIGHT), (LEFT, first, side.at[1, span(r, first)], LEFT),
            (RIGHT, first, side.at[0, span(r, first)], RIGHT), (LEFT, second, side.at[1, span(r, second)], LEFT)][k]
        return remote(pbuf.at[y_at[piece], span(r, part)], dst, ys.at[r, k], yr.at[r, k], {'ch': y_at[to]})

    def known(r, bound):
        return not isinstance(r, int) or r < bound

    def own(r):
        if known(r, rounds):
            x_start(r, *own_both, *own_side)

    def stage1(r):
        if known(r, rounds):
            for side_in, on in zip(own_both, relay_both):
                x_wait(r, side_in)
                x_start(r, on)
            x_start(r, *side_both)
            own(r + 2)
            if isinstance(r, int) and r == rounds - 1:
                after()

    def stage2(r):
        for side_in, on in zip(relay_both, opp_both):
            x_wait(r, side_in)
            x_start(r, on)

    def dots(r):
        x_wait(r, *core_in)
        each = max(1, 256 // rr)

        def one(i, carry):
            at = pl.ds(i * each, each)
            block = hbuf[at, span(r), :].reshape(each * rr, hbuf.shape[2])
            part = jnp.dot(block, w_ref[...], preferred_element_type=F32)
            pbuf[at, span(r), :] = part.astype(BF16).reshape(each, rr, cols_out)
            return carry
        lax.fori_loop(0, ring_y // each, one, 0)
        if regather:
            for step in steps:
                sum_copy(step, r).start()
        else:
            for k in to_opp + to_side:
                y_copy(k, r).start()

    def combine(r):
        for k, piece, part in zip(to_opp, (RIGHT, LEFT), (first, second)):
            y_copy(k, r).wait_recv()
            at = y_at[piece], span(r, part)
            pbuf[at] = (pbuf[at].astype(F32) + opp_buf[k, span(r, part), :].astype(F32)).astype(BF16)
            y_copy(relayed[k], r).start()

    def final(r):
        rows = span(r)
        if regather:
            for step in steps:
                sum_copy(step, r).wait_recv()
        else:
            for k in to_side + relayed:
                y_copy(k, r).wait_recv()
        total = pbuf[ch, rows, :].astype(F32)
        for slot in range(side.shape[0]):
            total = total + side[slot, rows, :].astype(F32)
        total = resid[rows, :].astype(F32) + total + vec_ref[:, bias_at:bias_at + cols_out]
        if regather:
            obuf[rows, :] = total.astype(obuf.dtype)
            for step in steps:
                out_copy(step, r, 0).start()
            keep_copy(r).start()
        else:
            out_ref[rows, :] = total

    def turn(r):
        stage1(r + 1)
        stage2(r)
        later = not isinstance(r, int) or r >= 1
        if later and not regather:
            combine(r - 1)
        dots(r)
        if later:
            final(r - 1)

    mine = pltpu.make_async_copy(h_ref, hbuf.at[:, :, aligned(wd, depth)], own_sem)
    mine.start()
    ready()
    own(0)
    own(1)
    mine.wait()
    for one in loads:
        one.wait()
    stage1(0)
    turn(0)

    def middle(r, carry):
        turn(r)
        return carry
    lax.fori_loop(1, rounds - 3, middle, 0)
    for r in range(max(1, rounds - 3), rounds):
        turn(r)
    if not regather:
        combine(rounds - 1)
    final(rounds - 1)

    def finish():
        def drain(r, carry):
            for k in range(len(x_plan)):
                x_copy(k, r).wait_send()
            if regather:
                for step in steps:
                    sum_copy(step, r).wait_send()
                    out_copy(step, r, ring_y - step).wait_recv()
                    out_copy(step, r, 0).wait_send()
                keep_copy(r).wait()
            else:
                for k in to_opp + to_side + relayed:
                    y_copy(k, r).wait_send()
            return carry
        lax.fori_loop(0, rounds, drain, 0)
    return finish


def ring_peers():
    ring_x, ring_y, ch, wd, core, chip = where_am_i()
    return [{'wd': wd + 1 - 2 * core}] + [{'wd': lax.rem(chip + step, ring_x) * CORES + core} for step in (RIGHT, LEFT)] + [{'ch': lax.rem(ch + step, ring_y)} for step in range(1, ring_y)]


def mlp_out_kernel(rounds, bias_at, h_ref, w_in_ref, resid_ref, vec_ref, out_ref, w_ref, resid, obuf, hbuf, pbuf, side, xs, xr, ys, yr, local_sem):
    ready = greet(ring_peers())
    loads = [pltpu.make_async_copy(w_in_ref, w_ref, local_sem.at[1]), pltpu.make_async_copy(resid_ref, resid, local_sem.at[2])]
    for one in loads:
        one.start()
    ring_body(rounds, bias_at, h_ref, w_ref, resid, vec_ref, out_ref, obuf, hbuf, pbuf, side, None, xs, xr, ys, yr, local_sem.at[0], ready, loads, lambda: None)()


def ring_scratch(ring_y, share, wide, cols, rounds, regather):
    return [pltpu.VMEM((ring_y, share, wide), BF16), pltpu.VMEM((ring_y, share, cols), BF16),
            pltpu.VMEM((ring_y - 1 if regather else 2, share, cols), BF16)]


def ring_sems(rounds, ring_y):
    return [DMA((rounds, 9)), DMA((rounds, 9)), DMA((rounds, 2 * ring_y)), DMA((rounds, 2 * ring_y))]


def mlp_out(h, w, resid, vec, bias_at, ring_y, rounds, cid):
    share, cols = resid.shape
    return pl.pallas_call(
        functools.partial(mlp_out_kernel, rounds, bias_at),
        out_shape=jax.ShapeDtypeStruct((ring_y, share, cols), BF16),
        in_specs=[ANY, ANY, ANY, VMEM],
        out_specs=ANY,
        scratch_shapes=[pltpu.VMEM(w.shape, BF16), pltpu.VMEM(resid.shape, F32), pltpu.VMEM(resid.shape, BF16)]
        + ring_scratch(ring_y, share, w.shape[0], cols, rounds, True) + ring_sems(rounds, ring_y) + [DMA((3,))],
        compiler_params=pltpu.CompilerParams(collective_id=cid, has_side_effects=True, vmem_limit_bytes=GRANT),
        name='mlp_out',
    )(h, w, resid, vec).reshape(ring_y * share, cols)


def mid_kernel(rounds, offs, h_ref, w_o_ref, x_ref, vec_ref, wg_ref, wu_ref, g0_ref, u0_ref, inner_ref, resid_out, resid_ref, x_rows, hbuf, pbuf, side, opp_buf, out_ref, nbuf, w_ref, keep, send, got, sums, all_sums,
               xs, xr, ys, yr, ns, nr, ss, sr, load_sem, local_sem, ws, wr, io_sem):
    share, width = resid_ref.shape
    ring_x, ring_y, ch, wd, core, chip = where_am_i()
    wd_count = ring_x * CORES
    rr = share // rounds
    half = rr // 2
    partner = wd + 1 - 2 * core
    ff = out_ref.shape[2]

    def device(d1, d2):
        return {'ch': lax.rem(ch + d1 * (1 - core) + d2 * core, ring_y), 'wd': lax.rem(chip + d1 * core + d2 * (1 - core), ring_x) * CORES + core}

    def block(d1, d2, r, part=None):
        rows = pl.ds(r * rr, rr) if part is None else pl.ds(r * rr + part * half, half)
        at = lax.rem(chip + d1 * core + d2 * (1 - core), ring_x)
        return nbuf.at[lax.rem(ch + d1 * (1 - core) + d2 * core, ring_y), rows, aligned(at, width)]

    whole = None
    plan = [((0, 0), (RIGHT, 0), (LEFT, 0), whole), ((0, 0), (LEFT, 0), (RIGHT, 0), whole),
            ((LEFT, 0), (RIGHT, 0), (OPP, 0), 0), ((RIGHT, 0), (LEFT, 0), (OPP, 0), 1)]
    for d1 in (0, LEFT, RIGHT, OPP):
        plan += [((d1, 0), (0, RIGHT), (d1, LEFT), whole), ((d1, 0), (0, LEFT), (d1, RIGHT), whole),
                 ((d1, LEFT), (0, RIGHT), (d1, OPP), 0), ((d1, RIGHT), (0, LEFT), (d1, OPP), 1)]
    core_step = len(plan)

    def copy(k, r):
        src, to, _, part = plan[k]
        ref = block(*src, r, part)
        return remote(ref, ref, ns.at[r, k], nr.at[r, k], device(*to))

    def start(r, *ks):
        for k in ks:
            copy(k, r).start()

    def wait(r, *ks):
        for k in ks:
            ref = block(*plan[k][2], r, plan[k][3])
            remote(ref, ref, ns.at[r, k], nr.at[r, k], device(RIGHT, 0)).wait_recv()

    def own(r):
        if r < rounds:
            start(r, 0, 1, 4, 5)

    def stage1(r):
        if r < rounds:
            wait(r, 0, 1)
            start(r, 2, 3, 8, 9, 12, 13)
            wait(r, 4, 5)
            start(r, 6, 7)

    def stage2(r):
        if r < rounds:
            wait(r, 2, 3)
            start(r, 16, 17)
            wait(r, 8, 9)
            start(r, 10, 11)
            wait(r, 12, 13)
            start(r, 14, 15)

    def stage3(r):
        if r < rounds:
            wait(r, 16, 17)
            start(r, 18, 19)

    def halves(r):
        return remote(send.at[r], got.at[r], ns.at[r, core_step], nr.at[r, core_step], {'wd': partner})

    each = max(1, 256 // rr)

    def dots(r, mine):
        def one(i, carry):
            at = pl.ds(i * each, each)
            rows = nbuf[at, pl.ds(r * rr, rr), :].reshape(each * rr, nbuf.shape[2])
            if mine:
                keep[at] = jnp.dot(rows, w_ref[core], preferred_element_type=F32).reshape(each, rr, 2 * ff)
            else:
                send[r, at] = jnp.dot(rows, w_ref[1 - core], preferred_element_type=F32).astype(BF16).reshape(each, rr, 2 * ff)
            return carry
        lax.fori_loop(0, ring_y // each, one, 0)

    def inner_copy(r):
        at = pl.ds(r * rr, rr)
        return pltpu.make_async_copy(out_ref.at[:, at, :], inner_ref.at[:, at, :], io_sem.at[r])

    def finish(r):
        halves(r).wait_recv()
        b_g, b_u = (vec_ref[:, pl.ds(pl.multiple_of(offs[name] + wd * ff, LANES), ff)] for name in ('bias_g', 'bias_u'))

        def one(q, carry):
            total = keep[q] + got[r, q].astype(F32)
            out_ref[q, pl.ds(r * rr, rr), :] = (jax.nn.gelu(total[:, :ff] + b_g, approximate=True) * (total[:, ff:] + b_u)).astype(BF16)
            return carry
        lax.fori_loop(0, ring_y, one, 0)
        inner_copy(r).start()

    ready = greet([{'wd': lax.rem(wd + step, wd_count)} for step in range(1, wd_count)] + [{'ch': lax.rem(ch + step, ring_y)} for step in range(1, ring_y)])
    loads = []
    for m, (full, part) in enumerate(((wg_ref, g0_ref), (wu_ref, u0_ref))):
        for k in range(CORES):
            for step in range(1 if k else ring_x):
                rows = aligned(lax.rem(chip + step, ring_x), width)
                src = part.at[rows, :] if step else full.at[:, aligned(chip * CORES + k, ff)]
                loads.append(pltpu.make_async_copy(src, w_ref.at[k, rows, pl.ds(m * ff, ff)], load_sem.at[k, m, step]))
    moves = [one for m, full in enumerate((wg_ref, wu_ref)) for one in swaps(full, w_ref.at[1, :, pl.ds(m * ff, ff)], 1, ws.at[m], wr.at[m])]
    first_load = pltpu.make_async_copy(x_ref.at[aligned(ch, share), :], x_rows, local_sem.at[1])
    first_load.start()

    def after():
        for one in moves + loads:
            one.start()

    ring_done = ring_body(rounds, offs['bias_o'], h_ref, w_o_ref, x_rows, vec_ref, resid_ref, None, hbuf, pbuf, side, opp_buf, xs, xr, ys, yr, local_sem.at[0], ready, [first_load], after)
    keep_resid = pltpu.make_async_copy(resid_ref, resid_out, local_sem.at[2])
    keep_resid.start()
    row_sums(resid_ref, sums)
    all_sums[wd] = sums[...]
    for one in sum_copies(sums, all_sums, ss, sr):
        one.start()
    for one in sum_copies(sums, all_sums, ss, sr):
        one.wait()
    scale = lax.rsqrt(jnp.sum(all_sums[...], axis=0) / (width * wd_count) + EPS)
    gain = 1.0 + vec_ref[:, offs['gain_mlp']:offs['gain_mlp'] + width]

    def norm(r):
        for i in range(r * rr // LANES, (r + 1) * rr // LANES):
            factor = as_column(scale[i:i + 1, :])[:, 0:1]
            rows = slice(i * LANES, (i + 1) * LANES)
            nbuf[ch, rows, aligned(chip, width)] = (resid_ref[rows, :] * factor * gain).astype(BF16)

    for r in range(rounds):
        norm(r)
        if r < 3:
            own(r)
    stage1(0)
    stage2(0)
    stage1(1)
    stage3(0)
    stage2(1)
    for one in loads + moves:
        one.wait()
    for r in range(rounds):
        wait(r, 6, 7, 10, 11, 14, 15, 18, 19)
        dots(r, False)
        halves(r).start()
        own(r + 3)
        stage1(r + 2)
        stage3(r + 1)
        dots(r, True)
        stage2(r + 2)
        finish(r)
    for r in range(rounds):
        inner_copy(r).wait()
        halves(r).wait_send()
        for k in range(core_step):
            copy(k, r).wait_send()
    keep_resid.wait()
    ring_done()


def mid(offs, h, w_o, x, vec, w_g, w_u, parts, ring_x, ring_y, rounds, cid):
    tokens, width = x.shape
    share = tokens // ring_y
    depth, ff = parts[0].shape
    cols = 2 * ff
    rr = share // rounds
    return pl.pallas_call(
        functools.partial(mid_kernel, rounds, offs),
        out_shape=(jax.ShapeDtypeStruct((ring_y, share, ff), BF16), jax.ShapeDtypeStruct((share, width), F32)),
        in_specs=[ANY, VMEM, ANY, VMEM] + [ANY] * 4,
        out_specs=(ANY, ANY),
        scratch_shapes=[pltpu.VMEM((share, width), F32), pltpu.VMEM((share, width), BF16)] + ring_scratch(ring_y, share, w_o.shape[0], width, rounds, False) + [
            pltpu.VMEM((2, share, width), BF16),
            pltpu.VMEM((ring_y, share, ff), BF16),
            pltpu.VMEM((ring_y, share, depth), BF16),
            pltpu.VMEM((CORES, depth, cols), BF16),
            pltpu.VMEM((ring_y, rr, cols), F32),
            pltpu.VMEM((rounds, ring_y, rr, cols), BF16),
            pltpu.VMEM((rounds, ring_y, rr, cols), BF16),
            pltpu.VMEM((share // LANES, LANES), F32),
            pltpu.VMEM((ring_x * CORES, share // LANES, LANES), F32),
        ] + ring_sems(rounds, ring_y) + [
            DMA((rounds, 21)), DMA((rounds, 21)), DMA((ring_x * CORES,)), DMA((ring_x * CORES,)),
            DMA((CORES, 2, ring_x)), DMA((3,)), DMA((2, ring_x)), DMA((2, ring_x)), DMA((rounds,)),
        ],
        compiler_params=pltpu.CompilerParams(collective_id=cid, has_side_effects=True, vmem_limit_bytes=GRANT),
        name='mid',
    )(h.reshape(ring_y, share, h.shape[1]), w_o, x, vec, w_g, w_u, *parts)


def front_kernel(rounds, offs, x_in_ref, vec_ref, pos_ref, rg_ref, ig_ref, w_x_ref, w_y_ref, wg_ref, wu_ref, out_ref, part_g, part_u, x_ref, nbuf, wbuf, pbuf, opp_buf, side, u_ref, y_ref, u32, a_s, b_s, gate_w, sums, all_sums, local_sem, ps, pr, xs, xr, ss, sr, ws, wr, in_sem):
    tokens, width = x_ref.shape
    ring_x, _, _, wd, core, chip = where_am_i()
    wd_count = ring_x * CORES
    rr = tokens // rounds
    half = rr // 2
    mine = y_ref.shape[1]
    piece = CORES * mine
    partner = wd + 1 - 2 * core
    right, opp, left = (lax.rem(chip + step, ring_x) for step in (RIGHT, OPP, LEFT))
    first, second = 0, 1

    def span(r, part=None):
        return pl.ds(r * rr, rr) if part is None else pl.ds(r * rr + part * half, half)

    def weight(k, of):
        j, m = k // 2, k % 2
        src = (w_x_ref, w_y_ref)[m].at[:, pl.ds(pl.multiple_of((j * CORES + of) * mine, mine), mine)]
        return src, wbuf.at[aligned(core, width), pl.ds(j * piece + m * mine, mine)]

    def weight_out(k):
        src, dst = weight(k, 1 - core)
        return pltpu.make_async_remote_copy(src_ref=src, dst_ref=dst, send_sem=ps.at[rounds, k], recv_sem=pr.at[rounds, k], device_id={'wd': partner}, device_id_type=MESH)

    def weight_own(k):
        src, dst = weight(k, core)
        return pltpu.make_async_copy(src, dst, local_sem.at[k])

    def weight_in(k):
        ref = wbuf.at[aligned(1 - core, width), pl.ds((k // 2) * piece + (k % 2) * mine, mine)]
        pltpu.make_async_remote_copy(src_ref=ref, dst_ref=ref, send_sem=ps.at[rounds, k], recv_sem=pr.at[rounds, k], device_id={'wd': partner}, device_id_type=MESH).wait_recv()

    def normed(r, of):
        ref = nbuf.at[span(r), aligned(of, width)]
        return pltpu.make_async_remote_copy(src_ref=ref, dst_ref=ref, send_sem=ps.at[r, 0], recv_sem=pr.at[r, 0], device_id={'wd': partner}, device_id_type=MESH)

    def u_copy(r, of):
        ref = u_ref.at[span(r), aligned(of, mine)]
        return remote(ref, ref, ps.at[r, 1], pr.at[r, 1], {'wd': partner})

    def part_of(dest, r, part):
        return pbuf.at[span(r, part), aligned(dest, piece)]

    def x_send(k, r):
        rows = pl.ds(r * half, half)
        dest, part, dst, to = [
            (opp, first, opp_buf.at[0, rows], right), (opp, second, opp_buf.at[1, rows], left),
            (right, second, side.at[0, span(r, second)], right), (left, first, side.at[1, span(r, first)], left),
            (right, first, side.at[0, span(r, first)], right), (left, second, side.at[1, span(r, second)], left)][k]
        return remote(part_of(dest, r, part), dst, xs.at[r, k], xr.at[r, k], {'wd': to * CORES + core})

    def norm(r):
        for i in range(rr // LANES):
            tile = r * (rr // LANES) + i
            factor = as_column(scale[tile:tile + 1, :])[:, 0:1]
            rows = slice(tile * LANES, (tile + 1) * LANES)
            nbuf[rows, aligned(core, width)] = (x_ref[rows, :].astype(F32) * factor * gain).astype(BF16)
        normed(r, core).start()

    def dots(r):
        normed(r, 1 - core).wait_recv()
        step_rows = rr // 4

        def one(i, carry):
            rows = pl.ds(pl.multiple_of(r * rr + i * step_rows, step_rows), step_rows)
            pbuf[rows, :] = jnp.dot(nbuf[rows, :], wbuf[...], preferred_element_type=F32).astype(BF16)
            return carry
        lax.fori_loop(0, 4, one, 0)
        for k in range(4):
            x_send(k, r).start()

    def combine(r):
        rows = pl.ds(r * half, half)
        for k, dest, part, back in ((0, right, first, 4), (1, left, second, 5)):
            x_send(k, r).wait_recv()
            at = (span(r, part), aligned(dest, piece))
            pbuf[at] = (pbuf[at].astype(F32) + opp_buf[k, rows, :].astype(F32)).astype(BF16)
            x_send(back, r).start()

    def final(r):
        for k in range(2, 6):
            x_send(k, r).wait_recv()
        rows = span(r)
        total = pbuf[rows, aligned(chip, piece)].astype(F32) + side[0, rows, :].astype(F32) + side[1, rows, :].astype(F32)
        b_x, b_y = (vec_ref[:, pl.ds(pl.multiple_of(offs[name] + wd * mine, mine), mine)] for name in ('bias_x', 'bias_y'))
        u_ref[rows, aligned(core, mine)] = (total[:, :mine] + b_x).astype(BF16)
        u_copy(r, core).start()
        y_ref[rows, :] = jax.nn.gelu(total[:, mine:] + b_y, approximate=True).astype(BF16)

    wide = CORES * mine
    tile = tokens // SEGS
    pitch = tile + PAD
    per_seg = tile // LANES
    per_round = rr // LANES
    n_taps = offs['taps']

    def vec(name, index, size):
        return vec_ref[:, pl.ds(pl.multiple_of(offs[name] + index * size, size), size)]

    taps = [vec_ref[:, pl.ds(pl.multiple_of(offs['conv_w'] + k * offs['rnn'] + chip * wide, wide), wide)] for k in range(n_taps)]
    cbias = vec('conv_bias', chip, wide)
    gate_b = jnp.concatenate([vec('rgate_b', wd, mine), vec('igate_b', wd, mine)], axis=1)
    lam = -vec('lam_param', wd, mine)
    soft = -8.0 * (jnp.maximum(lam, 0.0) + jnp.log(1.0 + jnp.exp(-jnp.abs(lam))))

    def gates(r):
        u_copy(r, 1 - core).wait_recv()

        def widen(i, carry):
            rows = pl.multiple_of(i * LANES, LANES)
            u32[pl.ds(rows + PAD, LANES), :] = u_ref[pl.ds(rows, LANES), :].astype(F32)
            return carry
        lax.fori_loop(r * per_round, (r + 1) * per_round, widen, 0)

        def one(i, carry):
            rows = pl.multiple_of(i * LANES, LANES)
            window = u32[pl.ds(rows, LANES + PAD), :]
            pos = as_column(pos_ref[:, pl.ds(rows, LANES)].astype(F32))
            pair = jnp.concatenate([pos, pos], axis=1)
            total = cbias + window[PAD:] * taps[0]
            for k in range(1, n_taps):
                total = total + jnp.where(pair >= k, window[PAD - k:PAD - k + LANES], 0.0) * taps[k]
            conv = total.astype(BF16)
            both = jax.nn.sigmoid(jnp.dot(conv, gate_w[...], preferred_element_type=F32) + gate_b)
            log_a = both[:, :mine] * soft
            reset = pos == 0
            decay = jnp.where(reset, 0.0, jnp.exp(log_a))
            scale = jnp.where(reset, 1.0, jnp.sqrt(neg_expm1(2.0 * log_a)))
            held = conv.astype(F32)
            drive = scale * both[:, mine:] * jnp.where(core == 0, held[:, :mine], held[:, mine:])
            seg = i // per_seg
            at = pl.multiple_of(seg * pitch + (i - seg * per_seg) * LANES, PAD)
            a_s[pl.ds(at, LANES), :] = decay
            b_s[pl.ds(at, LANES), :] = drive
            return carry
        lax.fori_loop(r * per_round, (r + 1) * per_round, one, 0)

    def scan():
        def steps(i, carry):
            hid, acc = carry
            for j in range(8):
                at = pl.ds(i * 8 + j, SEGS, stride=pitch)
                a = a_s[at, :]
                hid = a * hid + b_s[at, :]
                acc = a * acc
                b_s[at, :] = hid
                a_s[at, :] = acc
            return hid, acc
        hid, acc = lax.fori_loop(0, tile // 8, steps, (jnp.zeros((SEGS, mine), F32), jnp.ones((SEGS, mine), F32)))
        entry = jnp.zeros((1, mine), F32)
        for seg in range(SEGS):
            for q in range(per_seg):
                at = seg * pitch + q * LANES
                hidden = b_s[at:at + LANES, :] + a_s[at:at + LANES, :] * entry
                rows = slice(seg * tile + q * LANES, seg * tile + (q + 1) * LANES)
                out_ref[rows, :] = (hidden * y_ref[rows, :].astype(F32)).astype(BF16)
            entry = hid[seg:seg + 1] + acc[seg:seg + 1] * entry

    x_load = pltpu.make_async_copy(x_in_ref, x_ref, in_sem.at[0])
    x_load.start()
    ready = greet([{'wd': lax.rem(wd + step, wd_count)} for step in range(1, wd_count)])
    gate_loads = [pltpu.make_async_copy(w.at[chip, :, aligned(core, mine)], gate_w.at[:, pl.ds(m * mine, mine)], in_sem.at[m + 1]) for m, w in enumerate((rg_ref, ig_ref))]
    for one in gate_loads:
        one.start()
    for k in range(2 * ring_x):
        weight_own(k).start()
    moves, later = swaps(wg_ref, part_g, 0, ws.at[0], wr.at[0]), swaps(wu_ref, part_u, 0, ws.at[1], wr.at[1])
    ready()
    moves[RIGHT - 1].start()
    moves[LEFT - 1].start()
    x_load.wait()
    row_sums(x_ref, sums)
    all_sums[wd] = sums[...]
    for one in sum_copies(sums, all_sums, ss, sr):
        one.start()
    for k in range(2 * ring_x):
        weight_out(k).start()
    moves[OPP - 1].start()
    for one in gate_loads:
        one.wait()
    u32[0:PAD, :] = jnp.zeros((PAD, wide), F32)
    for one in sum_copies(sums, all_sums, ss, sr):
        one.wait()
    scale = lax.rsqrt(jnp.sum(all_sums[...], axis=0) / (width * wd_count) + EPS)
    gain = 1.0 + vec_ref[:, offs['gain_temporal']:offs['gain_temporal'] + width]
    norm(0)
    for k in range(2 * ring_x):
        weight_own(k).wait()
        weight_in(k)
    for r in range(rounds):
        if r + 1 < rounds:
            norm(r + 1)
        dots(r)
        if r >= 1:
            combine(r - 1)
        if r >= 2:
            final(r - 2)
        if r >= 3:
            gates(r - 3)
    combine(rounds - 1)
    for one in later:
        one.start()
    final(rounds - 2)
    gates(rounds - 3)
    final(rounds - 1)
    gates(rounds - 2)
    gates(rounds - 1)
    scan()
    for k in range(2 * ring_x):
        weight_out(k).wait_send()
    for r in range(rounds):
        normed(r, core).wait_send()
        u_copy(r, core).wait_send()
        for k in range(6):
            x_send(k, r).wait_send()
    for one in moves + later:
        one.wait()


def front(offs, x, vec, pos, rgate_w, igate_w, w_x, w_y, w_g, w_u, part, ring_x, rounds, cid):
    tokens, width = x.shape
    rnn = w_x.shape[1]
    mine = rnn // (ring_x * CORES)
    wide = CORES * mine
    seg_rows = SEGS * (tokens // SEGS + PAD)
    return pl.pallas_call(
        functools.partial(front_kernel, rounds, offs),
        out_shape=(jax.ShapeDtypeStruct((tokens, mine), BF16), part, part),
        in_specs=[ANY, VMEM, VMEM] + [ANY] * 6,
        out_specs=(VMEM, ANY, ANY),
        scratch_shapes=[
            pltpu.VMEM((tokens, width), BF16),
            pltpu.VMEM((tokens, CORES * width), BF16),
            pltpu.VMEM((CORES * width, rnn), BF16),
            pltpu.VMEM((tokens, rnn), BF16),
            pltpu.VMEM((2, tokens // 2, wide), BF16),
            pltpu.VMEM((2, tokens, wide), BF16),
            pltpu.VMEM((tokens, wide), BF16),
            pltpu.VMEM((tokens, mine), BF16),
            pltpu.VMEM((tokens + PAD, wide), F32),
            pltpu.VMEM((seg_rows, mine), F32),
            pltpu.VMEM((seg_rows, mine), F32),
            pltpu.VMEM((wide, wide), BF16),
            pltpu.VMEM((tokens // LANES, LANES), F32),
            pltpu.VMEM((ring_x * CORES, tokens // LANES, LANES), F32),
            DMA((2 * ring_x,)), DMA((rounds + 1, 2 * ring_x)), DMA((rounds + 1, 2 * ring_x)), DMA((rounds, 6)), DMA((rounds, 6)),
            DMA((ring_x * CORES,)), DMA((ring_x * CORES,)), DMA((2, ring_x)), DMA((2, ring_x)), DMA((3,)),
        ],
        compiler_params=pltpu.CompilerParams(collective_id=cid, has_side_effects=True, vmem_limit_bytes=GRANT),
        name='front',
    )(x, vec, pos, rgate_w, igate_w, w_x, w_y, w_g, w_u)


def place_kernel(in_ref, out_ref, held, sems):
    parts = held.shape[0]
    ins = [pltpu.make_async_copy(in_ref.at[i], held.at[i], sems.at[0, i]) for i in range(parts)]
    outs = [pltpu.make_async_copy(held.at[i], out_ref.at[i], sems.at[1, i]) for i in range(parts)]
    for one in ins:
        one.start()
    for i in range(parts):
        ins[i].wait()
        outs[i].start()
    for one in outs:
        one.wait()


def place(val, parts):
    shape = (parts, val.shape[0] // parts, val.shape[1])
    return pl.pallas_call(
        place_kernel,
        out_shape=jax.ShapeDtypeStruct(shape, val.dtype),
        in_specs=[ANY],
        out_specs=ANY,
        scratch_shapes=[pltpu.VMEM(shape, val.dtype), DMA((2, parts))],
        compiler_params=pltpu.CompilerParams(vmem_limit_bytes=GRANT),
        name='place',
    )(val.reshape(shape)).reshape(val.shape)


def solution(mesh):
    wd_count = mesh.shape['wd']
    ch_count = mesh.shape['ch']
    chips = wd_count // CORES
    row_spec = P('dp', 'wd')
    specs = (row_spec, P('dp', None), P('wd'), P('wd', 'ch'), P('ch'), P('wd', 'ch'), P('ch'), P(None, 'ch'), P('ch'), P('ch'), P('ch', None, None), P('ch'), P('ch', None, None), P('ch'), P('ch', 'wd'), P('wd'), P('wd'), P('wd', 'ch'), P('ch'), P('wd', 'ch'), P('ch'), P('ch', 'wd'), P('wd'))

    def local_layer(resid_in, seg_pos, gain_temporal, w_x, bias_x, w_y, bias_y, conv_w, conv_bias, lam_param, rgate_w, rgate_b, igate_w, igate_b, w_o, bias_o, gain_mlp, w_g, bias_g, w_u, bias_u, w_d, bias_d):
        small = {'gain_temporal': gain_temporal, 'bias_x': bias_x, 'bias_y': bias_y, 'conv_w': conv_w, 'conv_bias': conv_bias, 'lam_param': lam_param, 'rgate_b': rgate_b,
                 'igate_b': igate_b, 'bias_o': bias_o, 'gain_mlp': gain_mlp, 'bias_g': bias_g, 'bias_u': bias_u, 'bias_d': bias_d}
        offs = {'rnn': w_x.shape[1], 'taps': conv_w.shape[0]}
        end = 0
        for name, val in sorted(small.items(), key=lambda item: -item[1].size):
            offs[name] = end
            end += val.size
        spread = [lax.pad(small[name].astype(F32).reshape(-1), jnp.zeros((), F32), [(offs[name], end - offs[name] - small[name].size, 0)]) for name in small]
        vec = functools.reduce(jnp.add, spread).reshape(1, end)
        tokens = resid_in.shape[0]
        part = jax.ShapeDtypeStruct((chips * w_g.shape[0], w_g.shape[1] // wd_count), BF16)
        mixed, g0, u0 = front(offs, resid_in, vec, seg_pos.reshape(1, tokens), rgate_w, igate_w, w_x, w_y, w_g, w_u, part, chips, 8, 1)
        inner, resid = mid(offs, mixed, w_o, resid_in, vec, w_g, w_u, (g0, u0), chips, ch_count, 4, 2)
        return place(mlp_out(inner, w_d, resid, vec, offs['bias_d'], ch_count, 16, 3), 8)

    return jax.shard_map(local_layer, mesh=mesh, in_specs=specs, out_specs=row_spec, check_vma=False)
```

```python
import functools

import jax
import jax.numpy as jnp
from jax import lax
from jax.experimental import pallas as pl
from jax.experimental.pallas import tpu as pltpu
from jax.sharding import PartitionSpec as P

EPS = 1e-6
CORES = 2
SEGS = 8
PAD = 8
LANES = 128
RIGHT, OPP, LEFT = 1, 2, 3
MESH = pl.DeviceIdType.MESH
F32 = jnp.float32
BF16 = jnp.bfloat16
VMEM = pl.BlockSpec(memory_space=pltpu.VMEM)
ANY = pl.BlockSpec(memory_space=pl.ANY)
DMA = pltpu.SemaphoreType.DMA
GRANT = 67043328


def neg_expm1(z):
    series = -z * (1.0 + z * (0.5 + z * (1.0 / 6.0 + z * (1.0 / 24.0))))
    return jnp.where(z > -0.03, series, 1.0 - jnp.exp(z))


def where_am_i():
    ring_x = lax.axis_size('wd') // CORES
    wd = lax.axis_index('wd')
    return ring_x, lax.axis_size('ch'), lax.axis_index('ch'), wd, lax.rem(wd, CORES), wd // CORES


def aligned(index, size):
    return pl.ds(pl.multiple_of(index * size, size), size)


def remote(src, dst, send, recv, device):
    return pltpu.make_async_remote_copy(src_ref=src, dst_ref=dst, send_sem=send, recv_sem=recv, device_id=device, device_id_type=MESH)


def greet(devices):
    barrier = pltpu.get_barrier_semaphore()
    for device in devices:
        pl.semaphore_signal(barrier, inc=1, device_id=device, device_id_type=MESH)
    return functools.partial(pl.semaphore_wait, barrier, len(devices))


def swaps(src, dst, k, sends, recvs):
    ring_x, _, _, _, core, chip = where_am_i()
    depth, ff = src.shape[0], dst.shape[1]
    return [remote(src.at[:, aligned(lax.rem(chip + step, ring_x) * CORES + k, ff)], dst.at[aligned(chip, depth), :],
                   sends.at[step], recvs.at[step], {'wd': lax.rem(chip + step, ring_x) * CORES + core}) for step in range(1, ring_x)]


def row_sums(x_ref, sums):
    for i in range(x_ref.shape[0] // LANES):
        sq = jnp.zeros((LANES, LANES), F32)
        for j in range(x_ref.shape[1] // LANES):
            val = x_ref[i * LANES:(i + 1) * LANES, j * LANES:(j + 1) * LANES].astype(F32)
            sq = sq + val * val
        sums[i:i + 1, :] = jnp.sum(sq.T, axis=0, keepdims=True)


def sum_copies(sums, all_sums, ss, sr):
    ring_x, _, _, wd, _, _ = where_am_i()
    count = ring_x * CORES
    return [remote(sums, all_sums.at[wd], ss.at[step], sr.at[step], {'wd': lax.rem(wd + step, count)}) for step in range(1, count)]


def as_column(row):
    return jnp.broadcast_to(row, (LANES, LANES)).T


def ring_body(rounds, bias_at, h_ref, w_ref, resid, vec_ref, out_ref, obuf, hbuf, pbuf, side, opp_buf, xs, xr, ys, yr, own_sem, ready, loads, after):
    share, depth = h_ref.shape[1:]
    cols_out = w_ref.shape[1]
    rr = share // rounds
    ring_x, ring_y, ch, wd, core, chip = where_am_i()
    regather = obuf is not None
    other = 1 - 2 * core
    partner = wd + other
    x_at = [lax.rem(chip + step, ring_x) * CORES + core for step in range(ring_x)]
    y_at = [lax.rem(ch + step, ring_y) for step in range(ring_y)]
    first, second, whole = 0, 1, None
    steps = (RIGHT, LEFT, OPP)

    def span(r, part=None):
        return aligned(r, rr) if part is None else aligned(2 * r + part, rr // 2)

    def cols(owner, r, part=None):
        return hbuf.at[:, span(r, part), aligned(owner, depth)]

    x_plan = [(wd, whole, x_at[RIGHT], x_at[LEFT]), (wd, whole, x_at[LEFT], x_at[RIGHT]),
              (x_at[LEFT], first, x_at[RIGHT], x_at[OPP]), (x_at[RIGHT], second, x_at[LEFT], x_at[OPP]),
              (wd, whole, partner, partner), (x_at[LEFT], whole, partner, x_at[LEFT] + other), (x_at[RIGHT], whole, partner, x_at[RIGHT] + other),
              (x_at[OPP], first, partner, x_at[OPP] + other), (x_at[OPP], second, partner, x_at[OPP] + other)]
    own_both, own_side, relay_both, side_both, opp_both, core_in = (0, 1), (4,), (2, 3), (5, 6), (7, 8), (4, 5, 6, 7, 8)

    def x_copy(k, r):
        owner, part, to, _ = x_plan[k]
        dst = cols(owner, r, part)
        src = h_ref.at[:, span(r), :] if k in own_both + own_side else dst
        return remote(src, dst, xs.at[r, k], xr.at[r, k], {'wd': to})

    def x_start(r, *ks):
        for k in ks:
            x_copy(k, r).start()

    def x_wait(r, *ks):
        for k in ks:
            ref = cols(x_plan[k][-1], r, x_plan[k][1])
            remote(ref, ref, xs.at[r, k], xr.at[r, k], {'wd': partner}).wait_recv()

    def sum_copy(step, r):
        return remote(pbuf.at[y_at[step], span(r), :], side.at[step - 1, span(r), :], ys.at[r, step], yr.at[r, step], {'ch': y_at[step]})

    def out_copy(step, r, owner):
        return remote(obuf.at[span(r), :], out_ref.at[y_at[owner], span(r), :], ys.at[r, ring_y + step], yr.at[r, ring_y + step], {'ch': y_at[step]})

    def keep_copy(r):
        return pltpu.make_async_copy(obuf.at[span(r), :], out_ref.at[ch, span(r), :], ys.at[r, 0])

    to_opp, to_side, relayed = (0, 1), (2, 3), (4, 5)

    def y_copy(k, r):
        piece, part, dst, to = [
            (OPP, first, opp_buf.at[0, span(r, first)], RIGHT), (OPP, second, opp_buf.at[1, span(r, second)], LEFT),
            (RIGHT, second, side.at[0, span(r, second)], RIGHT), (LEFT, first, side.at[1, span(r, first)], LEFT),
            (RIGHT, first, side.at[0, span(r, first)], RIGHT), (LEFT, second, side.at[1, span(r, second)], LEFT)][k]
        return remote(pbuf.at[y_at[piece], span(r, part)], dst, ys.at[r, k], yr.at[r, k], {'ch': y_at[to]})

    def known(r, bound):
        return not isinstance(r, int) or r < bound

    def own(r):
        if known(r, rounds):
            x_start(r, *own_both, *own_side)

    def stage1(r):
        if known(r, rounds):
            for side_in, on in zip(own_both, relay_both):
                x_wait(r, side_in)
                x_start(r, on)
            x_start(r, *side_both)
            own(r + 2)
            if isinstance(r, int) and r == rounds - 1:
                after()

    def stage2(r):
        for side_in, on in zip(relay_both, opp_both):
            x_wait(r, side_in)
            x_start(r, on)

    def dots(r):
        x_wait(r, *core_in)
        each = max(1, 256 // rr)

        def one(i, carry):
            at = pl.ds(i * each, each)
            block = hbuf[at, span(r), :].reshape(each * rr, hbuf.shape[2])
            part = jnp.dot(block, w_ref[...], preferred_element_type=F32)
            pbuf[at, span(r), :] = part.astype(BF16).reshape(each, rr, cols_out)
            return carry
        lax.fori_loop(0, ring_y // each, one, 0)
        if regather:
            for step in steps:
                sum_copy(step, r).start()
        else:
            for k in to_opp + to_side:
                y_copy(k, r).start()

    def combine(r):
        for k, piece, part in zip(to_opp, (RIGHT, LEFT), (first, second)):
            y_copy(k, r).wait_recv()
            at = y_at[piece], span(r, part)
            pbuf[at] = (pbuf[at].astype(F32) + opp_buf[k, span(r, part), :].astype(F32)).astype(BF16)
            y_copy(relayed[k], r).start()

    def final(r):
        rows = span(r)
        if regather:
            for step in steps:
                sum_copy(step, r).wait_recv()
        else:
            for k in to_side + relayed:
                y_copy(k, r).wait_recv()
        total = pbuf[ch, rows, :].astype(F32)
        for slot in range(side.shape[0]):
            total = total + side[slot, rows, :].astype(F32)
        total = resid[rows, :].astype(F32) + total + vec_ref[:, bias_at:bias_at + cols_out]
        if regather:
            obuf[rows, :] = total.astype(obuf.dtype)
            for step in steps:
                out_copy(step, r, 0).start()
            keep_copy(r).start()
        else:
            out_ref[rows, :] = total

    def turn(r):
        stage1(r + 1)
        stage2(r)
        later = not isinstance(r, int) or r >= 1
        if later and not regather:
            combine(r - 1)
        dots(r)
        if later:
            final(r - 1)

    mine = pltpu.make_async_copy(h_ref, hbuf.at[:, :, aligned(wd, depth)], own_sem)
    mine.start()
    ready()
    own(0)
    own(1)
    mine.wait()
    for one in loads:
        one.wait()
    stage1(0)
    turn(0)

    def middle(r, carry):
        turn(r)
        return carry
    lax.fori_loop(1, rounds - 3, middle, 0)
    for r in range(max(1, rounds - 3), rounds):
        turn(r)
    if not regather:
        combine(rounds - 1)
    final(rounds - 1)

    def finish():
        def drain(r, carry):
            for k in range(len(x_plan)):
                x_copy(k, r).wait_send()
            if regather:
                for step in steps:
                    sum_copy(step, r).wait_send()
                    out_copy(step, r, ring_y - step).wait_recv()
                    out_copy(step, r, 0).wait_send()
                keep_copy(r).wait()
            else:
                for k in to_opp + to_side + relayed:
                    y_copy(k, r).wait_send()
            return carry
        lax.fori_loop(0, rounds, drain, 0)
    return finish


def ring_peers():
    ring_x, ring_y, ch, wd, core, chip = where_am_i()
    return [{'wd': wd + 1 - 2 * core}] + [{'wd': lax.rem(chip + step, ring_x) * CORES + core} for step in (RIGHT, LEFT)] + [{'ch': lax.rem(ch + step, ring_y)} for step in range(1, ring_y)]


def mlp_out_kernel(rounds, bias_at, h_ref, w_in_ref, resid_ref, vec_ref, out_ref, w_ref, resid, obuf, hbuf, pbuf, side, xs, xr, ys, yr, local_sem):
    ready = greet(ring_peers())
    loads = [pltpu.make_async_copy(w_in_ref, w_ref, local_sem.at[1]), pltpu.make_async_copy(resid_ref, resid, local_sem.at[2])]
    for one in loads:
        one.start()
    ring_body(rounds, bias_at, h_ref, w_ref, resid, vec_ref, out_ref, obuf, hbuf, pbuf, side, None, xs, xr, ys, yr, local_sem.at[0], ready, loads, lambda: None)()


def ring_scratch(ring_y, share, wide, cols, rounds, regather):
    return [pltpu.VMEM((ring_y, share, wide), BF16), pltpu.VMEM((ring_y, share, cols), BF16),
            pltpu.VMEM((ring_y - 1 if regather else 2, share, cols), BF16)]


def ring_sems(rounds, ring_y):
    return [DMA((rounds, 9)), DMA((rounds, 9)), DMA((rounds, 2 * ring_y)), DMA((rounds, 2 * ring_y))]


def mlp_out(h, w, resid, vec, bias_at, ring_y, rounds, cid):
    share, cols = resid.shape
    return pl.pallas_call(
        functools.partial(mlp_out_kernel, rounds, bias_at),
        out_shape=jax.ShapeDtypeStruct((ring_y, share, cols), BF16),
        in_specs=[ANY, ANY, ANY, VMEM],
        out_specs=ANY,
        scratch_shapes=[pltpu.VMEM(w.shape, BF16), pltpu.VMEM(resid.shape, F32), pltpu.VMEM(resid.shape, BF16)]
        + ring_scratch(ring_y, share, w.shape[0], cols, rounds, True) + ring_sems(rounds, ring_y) + [DMA((3,))],
        compiler_params=pltpu.CompilerParams(collective_id=cid, has_side_effects=True, vmem_limit_bytes=GRANT),
        name='mlp_out',
    )(h, w, resid, vec).reshape(ring_y * share, cols)


def mid_kernel(rounds, offs, h_ref, w_o_ref, x_ref, vec_ref, wg_ref, wu_ref, g0_ref, u0_ref, inner_ref, resid_out, resid_ref, x_rows, hbuf, pbuf, side, opp_buf, out_ref, nbuf, w_ref, keep, send, got, sums, all_sums,
               xs, xr, ys, yr, ns, nr, ss, sr, load_sem, local_sem, ws, wr, io_sem):
    share, width = resid_ref.shape
    ring_x, ring_y, ch, wd, core, chip = where_am_i()
    wd_count = ring_x * CORES
    rr = share // rounds
    half = rr // 2
    partner = wd + 1 - 2 * core
    ff = out_ref.shape[2]

    def turned(r, d1, d2):
        flip = core if r % 2 == 0 else 1 - core
        return lax.rem(ch + d1 * (1 - flip) + d2 * flip, ring_y), lax.rem(chip + d1 * flip + d2 * (1 - flip), ring_x)

    def device(r, d1, d2):
        at_y, at_x = turned(r, d1, d2)
        return {'ch': at_y, 'wd': at_x * CORES + core}

    def block(d1, d2, r, part=None):
        rows = pl.ds(r * rr, rr) if part is None else pl.ds(r * rr + part * half, half)
        at_y, at_x = turned(r, d1, d2)
        return nbuf.at[at_y, rows, aligned(at_x, width)]

    whole = None
    plan = [((0, 0), (RIGHT, 0), (LEFT, 0), whole), ((0, 0), (LEFT, 0), (RIGHT, 0), whole),
            ((LEFT, 0), (RIGHT, 0), (OPP, 0), 0), ((RIGHT, 0), (LEFT, 0), (OPP, 0), 1)]
    for d1 in (0, LEFT, RIGHT, OPP):
        plan += [((d1, 0), (0, RIGHT), (d1, LEFT), whole), ((d1, 0), (0, LEFT), (d1, RIGHT), whole),
                 ((d1, LEFT), (0, RIGHT), (d1, OPP), 0), ((d1, RIGHT), (0, LEFT), (d1, OPP), 1)]
    core_step = len(plan)

    def copy(k, r):
        src, to, _, part = plan[k]
        ref = block(*src, r, part)
        return remote(ref, ref, ns.at[r, k], nr.at[r, k], device(r, *to))

    def start(r, *ks):
        for k in ks:
            copy(k, r).start()

    def wait(r, *ks):
        for k in ks:
            ref = block(*plan[k][2], r, plan[k][3])
            remote(ref, ref, ns.at[r, k], nr.at[r, k], device(r, RIGHT, 0)).wait_recv()

    def own(r):
        if r < rounds:
            start(r, 0, 1, 4, 5)

    def stage1(r):
        if r < rounds:
            wait(r, 0, 1)
            start(r, 2, 3, 8, 9, 12, 13)
            wait(r, 4, 5)
            start(r, 6, 7)

    def stage2(r):
        if r < rounds:
            wait(r, 2, 3)
            start(r, 16, 17)
            wait(r, 8, 9)
            start(r, 10, 11)
            wait(r, 12, 13)
            start(r, 14, 15)

    def stage3(r):
        if r < rounds:
            wait(r, 16, 17)
            start(r, 18, 19)

    def halves(r):
        return remote(send.at[r], got.at[r], ns.at[r, core_step], nr.at[r, core_step], {'wd': partner})

    each = max(1, 256 // rr)

    def dots(r, mine):
        def one(i, carry):
            at = pl.ds(i * each, each)
            rows = nbuf[at, pl.ds(r * rr, rr), :].reshape(each * rr, nbuf.shape[2])
            if mine:
                keep[at] = jnp.dot(rows, w_ref[core], preferred_element_type=F32).reshape(each, rr, 2 * ff)
            else:
                send[r, at] = jnp.dot(rows, w_ref[1 - core], preferred_element_type=F32).astype(BF16).reshape(each, rr, 2 * ff)
            return carry
        lax.fori_loop(0, ring_y // each, one, 0)

    def inner_copy(r):
        at = pl.ds(r * rr, rr)
        return pltpu.make_async_copy(out_ref.at[:, at, :], inner_ref.at[:, at, :], io_sem.at[r])

    def finish(r):
        halves(r).wait_recv()
        b_g, b_u = (vec_ref[:, pl.ds(pl.multiple_of(offs[name] + wd * ff, LANES), ff)] for name in ('bias_g', 'bias_u'))

        def one(q, carry):
            total = keep[q] + got[r, q].astype(F32)
            out_ref[q, pl.ds(r * rr, rr), :] = (jax.nn.gelu(total[:, :ff] + b_g, approximate=True) * (total[:, ff:] + b_u)).astype(BF16)
            return carry
        lax.fori_loop(0, ring_y, one, 0)
        inner_copy(r).start()

    ready = greet([{'wd': lax.rem(wd + step, wd_count)} for step in range(1, wd_count)] + [{'ch': lax.rem(ch + step, ring_y)} for step in range(1, ring_y)])
    loads = []
    for m, (full, part) in enumerate(((wg_ref, g0_ref), (wu_ref, u0_ref))):
        for k in range(CORES):
            for step in range(1 if k else ring_x):
                rows = aligned(lax.rem(chip + step, ring_x), width)
                src = part.at[rows, :] if step else full.at[:, aligned(chip * CORES + k, ff)]
                loads.append(pltpu.make_async_copy(src, w_ref.at[k, rows, pl.ds(m * ff, ff)], load_sem.at[k, m, step]))
    moves = [one for m, full in enumerate((wg_ref, wu_ref)) for one in swaps(full, w_ref.at[1, :, pl.ds(m * ff, ff)], 1, ws.at[m], wr.at[m])]
    first_load = pltpu.make_async_copy(x_ref.at[aligned(ch, share), :], x_rows, local_sem.at[1])
    first_load.start()

    def after():
        for one in moves + loads:
            one.start()

    ring_done = ring_body(rounds, offs['bias_o'], h_ref, w_o_ref, x_rows, vec_ref, resid_ref, None, hbuf, pbuf, side, opp_buf, xs, xr, ys, yr, local_sem.at[0], ready, [first_load], after)
    keep_resid = pltpu.make_async_copy(resid_ref, resid_out, local_sem.at[2])
    keep_resid.start()
    row_sums(resid_ref, sums)
    all_sums[wd] = sums[...]
    for one in sum_copies(sums, all_sums, ss, sr):
        one.start()
    for one in sum_copies(sums, all_sums, ss, sr):
        one.wait()
    scale = lax.rsqrt(jnp.sum(all_sums[...], axis=0) / (width * wd_count) + EPS)
    gain = 1.0 + vec_ref[:, offs['gain_mlp']:offs['gain_mlp'] + width]

    def norm(r):
        for i in range(r * rr // LANES, (r + 1) * rr // LANES):
            factor = as_column(scale[i:i + 1, :])[:, 0:1]
            rows = slice(i * LANES, (i + 1) * LANES)
            nbuf[ch, rows, aligned(chip, width)] = (resid_ref[rows, :] * factor * gain).astype(BF16)

    for r in range(rounds):
        norm(r)
        if r < 3:
            own(r)
    stage1(0)
    stage2(0)
    stage1(1)
    stage3(0)
    stage2(1)
    for one in loads + moves:
        one.wait()
    for r in range(rounds):
        wait(r, 6, 7, 10, 11, 14, 15, 18, 19)
        dots(r, False)
        halves(r).start()
        own(r + 3)
        stage1(r + 2)
        stage3(r + 1)
        dots(r, True)
        stage2(r + 2)
        finish(r)
    for r in range(rounds):
        inner_copy(r).wait()
        halves(r).wait_send()
        for k in range(core_step):
            copy(k, r).wait_send()
    keep_resid.wait()
    ring_done()


def mid(offs, h, w_o, x, vec, w_g, w_u, parts, ring_x, ring_y, rounds, cid):
    tokens, width = x.shape
    share = tokens // ring_y
    depth, ff = parts[0].shape
    cols = 2 * ff
    rr = share // rounds
    return pl.pallas_call(
        functools.partial(mid_kernel, rounds, offs),
        out_shape=(jax.ShapeDtypeStruct((ring_y, share, ff), BF16), jax.ShapeDtypeStruct((share, width), F32)),
        in_specs=[ANY, VMEM, ANY, VMEM] + [ANY] * 4,
        out_specs=(ANY, ANY),
        scratch_shapes=[pltpu.VMEM((share, width), F32), pltpu.VMEM((share, width), BF16)] + ring_scratch(ring_y, share, w_o.shape[0], width, rounds, False) + [
            pltpu.VMEM((2, share, width), BF16),
            pltpu.VMEM((ring_y, share, ff), BF16),
            pltpu.VMEM((ring_y, share, depth), BF16),
            pltpu.VMEM((CORES, depth, cols), BF16),
            pltpu.VMEM((ring_y, rr, cols), F32),
            pltpu.VMEM((rounds, ring_y, rr, cols), BF16),
            pltpu.VMEM((rounds, ring_y, rr, cols), BF16),
            pltpu.VMEM((share // LANES, LANES), F32),
            pltpu.VMEM((ring_x * CORES, share // LANES, LANES), F32),
        ] + ring_sems(rounds, ring_y) + [
            DMA((rounds, 21)), DMA((rounds, 21)), DMA((ring_x * CORES,)), DMA((ring_x * CORES,)),
            DMA((CORES, 2, ring_x)), DMA((3,)), DMA((2, ring_x)), DMA((2, ring_x)), DMA((rounds,)),
        ],
        compiler_params=pltpu.CompilerParams(collective_id=cid, has_side_effects=True, vmem_limit_bytes=GRANT),
        name='mid',
    )(h.reshape(ring_y, share, h.shape[1]), w_o, x, vec, w_g, w_u, *parts)


def front_kernel(rounds, offs, x_in_ref, vec_ref, pos_ref, rg_ref, ig_ref, w_x_ref, w_y_ref, wg_ref, wu_ref, out_ref, part_g, part_u, x_ref, nbuf, wbuf, pbuf, opp_buf, side, u_ref, y_ref, u32, a_s, b_s, gate_w, sums, all_sums, local_sem, ps, pr, xs, xr, ss, sr, ws, wr, in_sem):
    tokens, width = x_ref.shape
    ring_x, _, _, wd, core, chip = where_am_i()
    wd_count = ring_x * CORES
    rr = tokens // rounds
    half = rr // 2
    mine = y_ref.shape[1]
    piece = CORES * mine
    partner = wd + 1 - 2 * core
    right, opp, left = (lax.rem(chip + step, ring_x) for step in (RIGHT, OPP, LEFT))
    first, second = 0, 1

    def span(r, part=None):
        return pl.ds(r * rr, rr) if part is None else pl.ds(r * rr + part * half, half)

    def weight(k, of):
        j, m = k // 2, k % 2
        src = (w_x_ref, w_y_ref)[m].at[:, pl.ds(pl.multiple_of((j * CORES + of) * mine, mine), mine)]
        return src, wbuf.at[aligned(core, width), pl.ds(j * piece + m * mine, mine)]

    def weight_out(k):
        src, dst = weight(k, 1 - core)
        return pltpu.make_async_remote_copy(src_ref=src, dst_ref=dst, send_sem=ps.at[rounds, k], recv_sem=pr.at[rounds, k], device_id={'wd': partner}, device_id_type=MESH)

    def weight_own(k):
        src, dst = weight(k, core)
        return pltpu.make_async_copy(src, dst, local_sem.at[k])

    def weight_in(k):
        ref = wbuf.at[aligned(1 - core, width), pl.ds((k // 2) * piece + (k % 2) * mine, mine)]
        pltpu.make_async_remote_copy(src_ref=ref, dst_ref=ref, send_sem=ps.at[rounds, k], recv_sem=pr.at[rounds, k], device_id={'wd': partner}, device_id_type=MESH).wait_recv()

    def normed(r, of):
        ref = nbuf.at[span(r), aligned(of, width)]
        return pltpu.make_async_remote_copy(src_ref=ref, dst_ref=ref, send_sem=ps.at[r, 0], recv_sem=pr.at[r, 0], device_id={'wd': partner}, device_id_type=MESH)

    def u_copy(r, of):
        ref = u_ref.at[span(r), aligned(of, mine)]
        return remote(ref, ref, ps.at[r, 1], pr.at[r, 1], {'wd': partner})

    def part_of(dest, r, part):
        return pbuf.at[span(r, part), aligned(dest, piece)]

    def x_send(k, r):
        rows = pl.ds(r * half, half)
        dest, part, dst, to = [
            (opp, first, opp_buf.at[0, rows], right), (opp, second, opp_buf.at[1, rows], left),
            (right, second, side.at[0, span(r, second)], right), (left, first, side.at[1, span(r, first)], left),
            (right, first, side.at[0, span(r, first)], right), (left, second, side.at[1, span(r, second)], left)][k]
        return remote(part_of(dest, r, part), dst, xs.at[r, k], xr.at[r, k], {'wd': to * CORES + core})

    def norm(r):
        for i in range(rr // LANES):
            tile = r * (rr // LANES) + i
            factor = as_column(scale[tile:tile + 1, :])[:, 0:1]
            rows = slice(tile * LANES, (tile + 1) * LANES)
            nbuf[rows, aligned(core, width)] = (x_ref[rows, :].astype(F32) * factor * gain).astype(BF16)
        normed(r, core).start()

    def dots(r):
        normed(r, 1 - core).wait_recv()
        step_rows = rr // 4

        def one(i, carry):
            rows = pl.ds(pl.multiple_of(r * rr + i * step_rows, step_rows), step_rows)
            pbuf[rows, :] = jnp.dot(nbuf[rows, :], wbuf[...], preferred_element_type=F32).astype(BF16)
            return carry
        lax.fori_loop(0, 4, one, 0)
        for k in range(4):
            x_send(k, r).start()

    def combine(r):
        rows = pl.ds(r * half, half)
        for k, dest, part, back in ((0, right, first, 4), (1, left, second, 5)):
            x_send(k, r).wait_recv()
            at = (span(r, part), aligned(dest, piece))
            pbuf[at] = (pbuf[at].astype(F32) + opp_buf[k, rows, :].astype(F32)).astype(BF16)
            x_send(back, r).start()

    def final(r):
        for k in range(2, 6):
            x_send(k, r).wait_recv()
        rows = span(r)
        total = pbuf[rows, aligned(chip, piece)].astype(F32) + side[0, rows, :].astype(F32) + side[1, rows, :].astype(F32)
        b_x, b_y = (vec_ref[:, pl.ds(pl.multiple_of(offs[name] + wd * mine, mine), mine)] for name in ('bias_x', 'bias_y'))
        u_ref[rows, aligned(core, mine)] = (total[:, :mine] + b_x).astype(BF16)
        u_copy(r, core).start()
        y_ref[rows, :] = jax.nn.gelu(total[:, mine:] + b_y, approximate=True).astype(BF16)

    wide = CORES * mine
    tile = tokens // SEGS
    pitch = tile + PAD
    per_seg = tile // LANES
    per_round = rr // LANES
    n_taps = offs['taps']

    def vec(name, index, size):
        return vec_ref[:, pl.ds(pl.multiple_of(offs[name] + index * size, size), size)]

    taps = [vec_ref[:, pl.ds(pl.multiple_of(offs['conv_w'] + k * offs['rnn'] + chip * wide, wide), wide)] for k in range(n_taps)]
    cbias = vec('conv_bias', chip, wide)
    gate_b = jnp.concatenate([vec('rgate_b', wd, mine), vec('igate_b', wd, mine)], axis=1)
    lam = -vec('lam_param', wd, mine)
    soft = -8.0 * (jnp.maximum(lam, 0.0) + jnp.log(1.0 + jnp.exp(-jnp.abs(lam))))

    def gates(r):
        u_copy(r, 1 - core).wait_recv()

        def widen(i, carry):
            rows = pl.multiple_of(i * LANES, LANES)
            u32[pl.ds(rows + PAD, LANES), :] = u_ref[pl.ds(rows, LANES), :].astype(F32)
            return carry
        lax.fori_loop(r * per_round, (r + 1) * per_round, widen, 0)

        def one(i, carry):
            rows = pl.multiple_of(i * LANES, LANES)
            window = u32[pl.ds(rows, LANES + PAD), :]
            pos = as_column(pos_ref[:, pl.ds(rows, LANES)].astype(F32))
            pair = jnp.concatenate([pos, pos], axis=1)
            total = cbias + window[PAD:] * taps[0]
            for k in range(1, n_taps):
                total = total + jnp.where(pair >= k, window[PAD - k:PAD - k + LANES], 0.0) * taps[k]
            conv = total.astype(BF16)
            both = jax.nn.sigmoid(jnp.dot(conv, gate_w[...], preferred_element_type=F32) + gate_b)
            log_a = both[:, :mine] * soft
            reset = pos == 0
            decay = jnp.where(reset, 0.0, jnp.exp(log_a))
            scale = jnp.where(reset, 1.0, jnp.sqrt(neg_expm1(2.0 * log_a)))
            held = conv.astype(F32)
            drive = scale * both[:, mine:] * jnp.where(core == 0, held[:, :mine], held[:, mine:])
            seg = i // per_seg
            at = pl.multiple_of(seg * pitch + (i - seg * per_seg) * LANES, PAD)
            a_s[pl.ds(at, LANES), :] = decay
            b_s[pl.ds(at, LANES), :] = drive
            return carry
        lax.fori_loop(r * per_round, (r + 1) * per_round, one, 0)

    def scan():
        def steps(i, carry):
            hid, acc = carry
            for j in range(8):
                at = pl.ds(i * 8 + j, SEGS, stride=pitch)
                a = a_s[at, :]
                hid = a * hid + b_s[at, :]
                acc = a * acc
                b_s[at, :] = hid
                a_s[at, :] = acc
            return hid, acc
        hid, acc = lax.fori_loop(0, tile // 8, steps, (jnp.zeros((SEGS, mine), F32), jnp.ones((SEGS, mine), F32)))
        entry = jnp.zeros((1, mine), F32)
        for seg in range(SEGS):
            for q in range(per_seg):
                at = seg * pitch + q * LANES
                hidden = b_s[at:at + LANES, :] + a_s[at:at + LANES, :] * entry
                rows = slice(seg * tile + q * LANES, seg * tile + (q + 1) * LANES)
                out_ref[rows, :] = (hidden * y_ref[rows, :].astype(F32)).astype(BF16)
            entry = hid[seg:seg + 1] + acc[seg:seg + 1] * entry

    x_load = pltpu.make_async_copy(x_in_ref, x_ref, in_sem.at[0])
    x_load.start()
    ready = greet([{'wd': lax.rem(wd + step, wd_count)} for step in range(1, wd_count)])
    gate_loads = [pltpu.make_async_copy(w.at[chip, :, aligned(core, mine)], gate_w.at[:, pl.ds(m * mine, mine)], in_sem.at[m + 1]) for m, w in enumerate((rg_ref, ig_ref))]
    for one in gate_loads:
        one.start()
    for k in range(2 * ring_x):
        weight_own(k).start()
    moves, later = swaps(wg_ref, part_g, 0, ws.at[0], wr.at[0]), swaps(wu_ref, part_u, 0, ws.at[1], wr.at[1])
    ready()
    moves[RIGHT - 1].start()
    moves[LEFT - 1].start()
    x_load.wait()
    row_sums(x_ref, sums)
    all_sums[wd] = sums[...]
    for one in sum_copies(sums, all_sums, ss, sr):
        one.start()
    for k in range(2 * ring_x):
        weight_out(k).start()
    moves[OPP - 1].start()
    for one in gate_loads:
        one.wait()
    u32[0:PAD, :] = jnp.zeros((PAD, wide), F32)
    for one in sum_copies(sums, all_sums, ss, sr):
        one.wait()
    scale = lax.rsqrt(jnp.sum(all_sums[...], axis=0) / (width * wd_count) + EPS)
    gain = 1.0 + vec_ref[:, offs['gain_temporal']:offs['gain_temporal'] + width]
    norm(0)
    for k in range(2 * ring_x):
        weight_own(k).wait()
        weight_in(k)
    for r in range(rounds):
        if r + 1 < rounds:
            norm(r + 1)
        dots(r)
        if r >= 1:
            combine(r - 1)
        if r >= 2:
            final(r - 2)
        if r >= 3:
            gates(r - 3)
    combine(rounds - 1)
    for one in later:
        one.start()
    final(rounds - 2)
    gates(rounds - 3)
    final(rounds - 1)
    gates(rounds - 2)
    gates(rounds - 1)
    scan()
    for k in range(2 * ring_x):
        weight_out(k).wait_send()
    for r in range(rounds):
        normed(r, core).wait_send()
        u_copy(r, core).wait_send()
        for k in range(6):
            x_send(k, r).wait_send()
    for one in moves + later:
        one.wait()


def front(offs, x, vec, pos, rgate_w, igate_w, w_x, w_y, w_g, w_u, part, ring_x, rounds, cid):
    tokens, width = x.shape
    rnn = w_x.shape[1]
    mine = rnn // (ring_x * CORES)
    wide = CORES * mine
    seg_rows = SEGS * (tokens // SEGS + PAD)
    return pl.pallas_call(
        functools.partial(front_kernel, rounds, offs),
        out_shape=(jax.ShapeDtypeStruct((tokens, mine), BF16), part, part),
        in_specs=[ANY, VMEM, VMEM] + [ANY] * 6,
        out_specs=(VMEM, ANY, ANY),
        scratch_shapes=[
            pltpu.VMEM((tokens, width), BF16),
            pltpu.VMEM((tokens, CORES * width), BF16),
            pltpu.VMEM((CORES * width, rnn), BF16),
            pltpu.VMEM((tokens, rnn), BF16),
            pltpu.VMEM((2, tokens // 2, wide), BF16),
            pltpu.VMEM((2, tokens, wide), BF16),
            pltpu.VMEM((tokens, wide), BF16),
            pltpu.VMEM((tokens, mine), BF16),
            pltpu.VMEM((tokens + PAD, wide), F32),
            pltpu.VMEM((seg_rows, mine), F32),
            pltpu.VMEM((seg_rows, mine), F32),
            pltpu.VMEM((wide, wide), BF16),
            pltpu.VMEM((tokens // LANES, LANES), F32),
            pltpu.VMEM((ring_x * CORES, tokens // LANES, LANES), F32),
            DMA((2 * ring_x,)), DMA((rounds + 1, 2 * ring_x)), DMA((rounds + 1, 2 * ring_x)), DMA((rounds, 6)), DMA((rounds, 6)),
            DMA((ring_x * CORES,)), DMA((ring_x * CORES,)), DMA((2, ring_x)), DMA((2, ring_x)), DMA((3,)),
        ],
        compiler_params=pltpu.CompilerParams(collective_id=cid, has_side_effects=True, vmem_limit_bytes=GRANT),
        name='front',
    )(x, vec, pos, rgate_w, igate_w, w_x, w_y, w_g, w_u)


def place_kernel(in_ref, out_ref, held, sems):
    parts = held.shape[0]
    ins = [pltpu.make_async_copy(in_ref.at[i], held.at[i], sems.at[0, i]) for i in range(parts)]
    outs = [pltpu.make_async_copy(held.at[i], out_ref.at[i], sems.at[1, i]) for i in range(parts)]
    for one in ins:
        one.start()
    for i in range(parts):
        ins[i].wait()
        outs[i].start()
    for one in outs:
        one.wait()


def place(val, parts):
    shape = (parts, val.shape[0] // parts, val.shape[1])
    return pl.pallas_call(
        place_kernel,
        out_shape=jax.ShapeDtypeStruct(shape, val.dtype),
        in_specs=[ANY],
        out_specs=ANY,
        scratch_shapes=[pltpu.VMEM(shape, val.dtype), DMA((2, parts))],
        compiler_params=pltpu.CompilerParams(vmem_limit_bytes=GRANT),
        name='place',
    )(val.reshape(shape)).reshape(val.shape)


def solution(mesh):
    wd_count = mesh.shape['wd']
    ch_count = mesh.shape['ch']
    chips = wd_count // CORES
    row_spec = P('dp', 'wd')
    specs = (row_spec, P('dp', None), P('wd'), P('wd', 'ch'), P('ch'), P('wd', 'ch'), P('ch'), P(None, 'ch'), P('ch'), P('ch'), P('ch', None, None), P('ch'), P('ch', None, None), P('ch'), P('ch', 'wd'), P('wd'), P('wd'), P('wd', 'ch'), P('ch'), P('wd', 'ch'), P('ch'), P('ch', 'wd'), P('wd'))

    def local_layer(resid_in, seg_pos, gain_temporal, w_x, bias_x, w_y, bias_y, conv_w, conv_bias, lam_param, rgate_w, rgate_b, igate_w, igate_b, w_o, bias_o, gain_mlp, w_g, bias_g, w_u, bias_u, w_d, bias_d):
        small = {'gain_temporal': gain_temporal, 'bias_x': bias_x, 'bias_y': bias_y, 'conv_w': conv_w, 'conv_bias': conv_bias, 'lam_param': lam_param, 'rgate_b': rgate_b,
                 'igate_b': igate_b, 'bias_o': bias_o, 'gain_mlp': gain_mlp, 'bias_g': bias_g, 'bias_u': bias_u, 'bias_d': bias_d}
        offs = {'rnn': w_x.shape[1], 'taps': conv_w.shape[0]}
        end = 0
        for name, val in sorted(small.items(), key=lambda item: -item[1].size):
            offs[name] = end
            end += val.size
        spread = [lax.pad(small[name].astype(F32).reshape(-1), jnp.zeros((), F32), [(offs[name], end - offs[name] - small[name].size, 0)]) for name in small]
        vec = functools.reduce(jnp.add, spread).reshape(1, end)
        tokens = resid_in.shape[0]
        part = jax.ShapeDtypeStruct((chips * w_g.shape[0], w_g.shape[1] // wd_count), BF16)
        mixed, g0, u0 = front(offs, resid_in, vec, seg_pos.reshape(1, tokens), rgate_w, igate_w, w_x, w_y, w_g, w_u, part, chips, 8, 1)
        inner, resid = mid(offs, mixed, w_o, resid_in, vec, w_g, w_u, (g0, u0), chips, ch_count, 4, 2)
        return place(mlp_out(inner, w_d, resid, vec, offs['bias_d'], ch_count, 16, 3), 8)

    return jax.shard_map(local_layer, mesh=mesh, in_specs=specs, out_specs=row_spec, check_vma=False)
```
